32 devices in a mesh: facet: 4 (over y, core), team: 4 (over z), sub: 2 (over x).
Axes of the slice: x: 2, y: 2, z: 4, core: 2. Of those that a mesh axis runs over, the one named last changes fastest.
Arguments:
- facet_rows: bfloat16 [4, 2, 32, 4096], P('facet', None, 'team'), may hold values from -6 to 6
- sub_offsets: int32 [8, 2], replicated, may hold values from 0 to 4095
- facet_offsets: int32 [4, 2], replicated, may hold values from 0 to 4095
- aterm: bfloat16 [4, 2, 256, 256], P('facet'), may hold values from 0.29882812 to 3
- cells: int32 [4, 2, 4, 2, 256], P('facet', None, 'team'), may hold values from 0 to 1023
- observed: bfloat16 [4, 2, 4, 2, 256], P('facet', None, 'team'), may hold values from -6 to 6
- weights: bfloat16 [4, 2, 4, 256], P('facet', None, 'team'), may hold values from 0.29882812 to 3
- counts: int32 [4, 2, 4], replicated, may hold values from 1 to 256, as said below
Outputs:
- facet_update: float32 [4, 2, 32, 4096], P('facet', None, 'team', 'sub')
The draws below stay inside these ranges and needn't reach their ends.
Inputs may be any that keep to these rules, and one draw needn't show every extreme that they name: Slots 0 to counts[a, b, t] - 1 are live. For every a and t one of the two subgrids with indices [a, 0] and [a, 1] has at most 64 live slots, and which of the two it is does not change with t.
All inputs are finite; a program needn't handle non-finite values.
Results may differ from the reference program's by a relative error of at most 0.019.
Values may be sent and summed in bfloat16 or wider, within the bound.
A program may use at most 64 MiB of HBM per device.

```python
import math
import jax
import jax.numpy as jnp
from jax import lax

L = 4096
M = 128
SG = 256
VDEV = 256
R = 32
NS = 8
N_FACET = 4
N_TEAM = 4
N_SUB = 2


def draw_counts(key, part):
    key_list = jax.random.split(jax.random.fold_in(key, 7), 5)
    heavy_side = jax.random.randint(key_list[0], (N_FACET, 1), 0, 2)
    heavy_loads = jax.random.randint(key_list[1], (N_FACET, N_TEAM), VDEV // 2, VDEV + 1)
    light_loads = jax.random.randint(key_list[2], (N_FACET, N_TEAM), 1, VDEV // 4 + 1)
    flat_ids = jnp.arange(N_FACET * N_TEAM, dtype=jnp.int32).reshape(N_FACET, N_TEAM)
    top_pick = jax.random.randint(key_list[3], (), 0, N_FACET * N_TEAM)
    low_pick = jax.random.randint(key_list[4], (), 0, N_FACET * N_TEAM)
    heavy_loads = jnp.where(flat_ids == top_pick, VDEV, heavy_loads)
    light_loads = jnp.where(flat_ids == low_pick, VDEV // 4, light_loads)
    side_zero = jnp.where(heavy_side == 0, heavy_loads, light_loads)
    side_one = jnp.where(heavy_side == 0, light_loads, heavy_loads)
    return jnp.stack([side_zero, side_one], 1).astype(jnp.int32)


def place_ends(entries, rng, least, top_value):
    longest = entries.shape.index(max(entries.shape))
    spots = []
    for shift in (0, 1):
        where = [jax.random.randint(jax.random.fold_in(rng, axis), (), 0, length) for axis, length in enumerate(entries.shape)]
        where[longest] = (where[longest] + shift) % entries.shape[longest]
        spots.append(tuple(where))
    return entries.at[spots[0]].set(least).at[spots[1]].set(top_value)


def block_scale(stream_key, extent, cuts, least, largest):
    level = 1.0
    for axis_at, shards_of in cuts:
        heights = jax.random.uniform(jax.random.fold_in(jax.random.fold_in(stream_key, 6), axis_at), (shards_of,), jnp.float32, least / len(cuts), largest / len(cuts))
        level = level * jnp.repeat(jnp.exp(heights), extent[axis_at] // shards_of).reshape((-1,) + (1,) * (len(extent) - 1 - axis_at))
    return level


def noise(stream_key, extent, scale, most, cuts=(), kind=jnp.bfloat16):
    entries = scale * jax.random.normal(stream_key, extent, jnp.float32)
    if cuts:
        entries = entries * block_scale(stream_key, extent, cuts, -0.22, 0.18)
    return jnp.clip(entries, -most, most).astype(kind)


def setup_inputs(seed: int = 0) -> dict:
    splits = jax.random.split(jax.random.key(seed), 9)
    return {
        "facet_rows": noise(splits[0], (N_FACET, 2, R, L), 1.0, 6.0, ((0, 4), (2, 4))),
        "sub_offsets": place_ends(jax.random.randint(splits[1], (NS, 2), 0, L), jax.random.fold_in(splits[1], 1), 0, L - 1).astype(jnp.int32),
        "facet_offsets": place_ends(jax.random.randint(splits[2], (N_FACET, 2), 0, L), jax.random.fold_in(splits[2], 1), 0, L - 1).astype(jnp.int32),
        "aterm": jnp.clip(jnp.exp(math.log(3.0) - 2.306499 * jax.random.uniform(splits[3], (N_FACET, N_SUB, SG, SG), jnp.float32) ** block_scale(splits[3], (N_FACET, N_SUB, SG, SG), ((0, 4),), -0.2, 0.2)), 0.29882812, 3.0).astype(jnp.bfloat16),
        "cells": place_ends(jax.random.randint(splits[4], (N_FACET, N_SUB, N_TEAM, 2, VDEV), 0, 4 * SG), jax.random.fold_in(splits[4], 1), 0, (4 * SG) - 1).astype(jnp.int32),
        "observed": noise(splits[5], (N_FACET, N_SUB, N_TEAM, 2, VDEV), 1.0, 6.0, ((0, 4), (2, 4))),
        "weights": jnp.clip(jnp.exp(math.log(3.0) - 2.306499 * jax.random.uniform(splits[6], (N_FACET, N_SUB, N_TEAM, VDEV), jnp.float32) ** block_scale(splits[6], (N_FACET, N_SUB, N_TEAM, VDEV), ((0, 4), (2, 4)), -0.2, 0.2)), 0.29882812, 3.0).astype(jnp.bfloat16),
        "counts": draw_counts(jax.random.fold_in(splits[8], 71), 0),
    }


TWO_PI = 2.0 * math.pi
HIGHEST = lax.Precision.HIGHEST

def angles(left_ints, right_ints, period):
    return (left_ints * right_ints % period).astype(jnp.float32) * (TWO_PI / period)

def rounded(values_in):
    return lax.optimization_barrier(values_in.astype(jnp.bfloat16)).astype(jnp.float32)

def transform_tables():
    columns = jnp.arange(L, dtype=jnp.int32)
    frequency = jnp.arange(M, dtype=jnp.int32)
    angle_grid = angles(columns[:, None], frequency[None, :], L)
    cos_part = jnp.cos(angle_grid)
    sin_part = jnp.sin(angle_grid)
    spec_re = (cos_part / math.sqrt(L)).astype(jnp.bfloat16)
    spec_im = (-sin_part / math.sqrt(L)).astype(jnp.bfloat16)
    forward = jnp.concatenate([jnp.concatenate([spec_re, spec_im], 1), jnp.concatenate([-spec_im, spec_re], 1)], 0)
    back_re = (cos_part.T / math.sqrt(M)).astype(jnp.bfloat16)
    back_im = (sin_part.T / math.sqrt(M)).astype(jnp.bfloat16)
    backward = jnp.concatenate([jnp.concatenate([back_re, back_im], 1), jnp.concatenate([-back_im, back_re], 1)], 0)
    return (forward, backward)

def subgrid_table(size_sub):
    freq_ids = jnp.arange(M, dtype=jnp.int32)
    cell_ids = jnp.arange(size_sub, dtype=jnp.int32)
    angle_grid = angles(freq_ids[:, None], cell_ids[None, :], size_sub)
    factor = 1.0 / math.sqrt(M)
    return (jnp.cos(angle_grid) * factor, jnp.sin(angle_grid) * factor)

def facet_phase(row_ids, facet_offsets):
    col_ids = jnp.arange(M, dtype=jnp.int32)
    along_rows = row_ids[:, None] * facet_offsets[None, :, 0] % L
    along_cols = col_ids[None, :] * facet_offsets[:, 1:2] % L
    angle_grid = ((along_rows[:, :, None] + along_cols[None, :, :]) % L).astype(jnp.float32) * (TWO_PI / L)
    return (jnp.cos(angle_grid), jnp.sin(angle_grid))

def hdot(left, right):
    return jnp.dot(left, right, precision=HIGHEST, preferred_element_type=jnp.float32)

def to_image(assembled, k_re, k_im):
    grid_re = assembled[:, 0]
    grid_im = assembled[:, 1]
    temp_re = hdot(k_re.T, grid_re) - hdot(k_im.T, grid_im)
    temp_im = hdot(k_re.T, grid_im) + hdot(k_im.T, grid_re)
    image_re = hdot(temp_re, k_re) - hdot(temp_im, k_im)
    image_im = hdot(temp_re, k_im) + hdot(temp_im, k_re)
    return (image_re, image_im)

def to_return(grid, weight_map, k_re, k_im):
    size_sub = weight_map.shape[0]
    grid_re = grid[:, :size_sub] * weight_map / size_sub
    grid_im = grid[:, size_sub:] * weight_map / size_sub
    temp_re = hdot(k_re, grid_re) + hdot(k_im, grid_im)
    temp_im = hdot(k_re, grid_im) - hdot(k_im, grid_re)
    out_re = hdot(temp_re, k_re.T) + hdot(temp_im, k_im.T)
    out_im = hdot(temp_im, k_re.T) - hdot(temp_re, k_im.T)
    return jnp.stack([out_re, out_im], 1)

def degrid_block(weighted, cell_pair, observed_pair, weight, live):
    size_sub = weighted.shape[1]
    block_len = cell_pair.shape[1]
    index = jnp.arange(size_sub, dtype=jnp.int32)
    row_angle = angles(cell_pair[0][:, None], index[None, :], 4 * size_sub)
    col_angle = angles(cell_pair[1][:, None], index[None, :], 4 * size_sub)
    cos_rows = rounded(jnp.cos(row_angle))
    sin_rows = rounded(jnp.sin(row_angle))
    cos_cols = rounded(jnp.cos(col_angle))
    sin_cols = rounded(jnp.sin(col_angle))
    col_stack = jnp.concatenate([cos_cols, sin_cols], 0)
    products = jnp.einsum('jk,ik->ji', col_stack, weighted.astype(jnp.float32), precision=HIGHEST)
    part_re = products[:block_len, :size_sub] + products[block_len:, size_sub:]
    part_im = products[:block_len, size_sub:] - products[block_len:, :size_sub]
    pred_re = lax.optimization_barrier(jnp.sum(cos_rows * part_re + sin_rows * part_im, 1)) / size_sub
    pred_im = lax.optimization_barrier(jnp.sum(cos_rows * part_im - sin_rows * part_re, 1)) / size_sub
    res_re = live * weight * (observed_pair[0] - pred_re)
    res_im = live * weight * (observed_pair[1] - pred_im)
    spread_re = rounded(res_re[:, None] * cos_cols - res_im[:, None] * sin_cols)
    spread_im = rounded(res_re[:, None] * sin_cols + res_im[:, None] * cos_cols)
    right = jnp.concatenate([jnp.concatenate([spread_re, spread_im], 1), jnp.concatenate([-spread_im, spread_re], 1)], 0)
    left = jnp.concatenate([cos_rows, sin_rows], 0)
    return jnp.einsum('ji,jk->ik', left, right, precision=HIGHEST)

def reference(facet_rows, sub_offsets, facet_offsets, aterm, cells, observed, weights, counts):
    forward, backward = transform_tables()
    k_re, k_im = subgrid_table(SG)
    norm = 1.0 / math.sqrt(N_FACET)
    columns = jnp.arange(L, dtype=jnp.int32)
    row_ids = jnp.arange(R, dtype=jnp.int32)
    out_ids = jnp.arange(M, dtype=jnp.int32)
    slot_ids = jnp.arange(VDEV, dtype=jnp.int32)
    facet_re = facet_rows[:, 0].astype(jnp.float32)
    facet_im = facet_rows[:, 1].astype(jnp.float32)
    phase_cos, phase_sin = facet_phase(out_ids, facet_offsets)

    def one_subgrid(total, subgrid):
        owner = subgrid // N_SUB
        side = subgrid % N_SUB
        mod_angle = angles(sub_offsets[subgrid, 1], columns, L)
        mod_cos = jnp.cos(mod_angle)[None, None, :]
        mod_sin = jnp.sin(mod_angle)[None, None, :]
        mod_re = (facet_re * mod_cos + facet_im * mod_sin).astype(jnp.bfloat16)
        mod_im = (facet_im * mod_cos - facet_re * mod_sin).astype(jnp.bfloat16)
        stacked = jnp.concatenate([mod_re, mod_im], 2).reshape(N_FACET * R, 2 * L)
        spectrum = jnp.dot(stacked, forward, preferred_element_type=jnp.float32).reshape(N_FACET, R, 2, M)
        w_angle = angles(out_ids[:, None] + sub_offsets[subgrid, 0], row_ids[None, :], R)
        w_re = jnp.cos(w_angle) / math.sqrt(R)
        w_im = -jnp.sin(w_angle) / math.sqrt(R)
        con_re = jnp.einsum('pr,frm->pfm', w_re, spectrum[:, :, 0], precision=HIGHEST) - jnp.einsum('pr,frm->pfm', w_im, spectrum[:, :, 1], precision=HIGHEST)
        con_im = jnp.einsum('pr,frm->pfm', w_re, spectrum[:, :, 1], precision=HIGHEST) + jnp.einsum('pr,frm->pfm', w_im, spectrum[:, :, 0], precision=HIGHEST)
        grid_re = lax.optimization_barrier(jnp.sum(phase_cos * con_re - phase_sin * con_im, 1)) * norm
        grid_im = lax.optimization_barrier(jnp.sum(phase_cos * con_im + phase_sin * con_re, 1)) * norm
        image_re, image_im = to_image(jnp.stack([grid_re, grid_im], 1), k_re, k_im)
        weight_map = aterm[owner, side].astype(jnp.float32)
        weighted = jnp.concatenate([(weight_map * image_re).astype(jnp.bfloat16), (weight_map * image_im).astype(jnp.bfloat16)], 0)

        def one_team(team):
            live = (slot_ids < counts[owner, side, team]).astype(jnp.float32)
            return degrid_block(weighted, cells[owner, side, team], observed[owner, side, team].astype(jnp.float32), weights[owner, side, team].astype(jnp.float32), live)
        grid = lax.optimization_barrier(jnp.sum(lax.map(one_team, jnp.arange(N_TEAM, dtype=jnp.int32)), 0))
        returned = to_return(grid, weight_map, k_re, k_im)
        back_re = (phase_cos * returned[:, None, 0] + phase_sin * returned[:, None, 1]) * norm
        back_im = (phase_cos * returned[:, None, 1] - phase_sin * returned[:, None, 0]) * norm
        fold_re = jnp.einsum('pr,pfm->frm', w_re, back_re, precision=HIGHEST) + jnp.einsum('pr,pfm->frm', w_im, back_im, precision=HIGHEST)
        fold_im = jnp.einsum('pr,pfm->frm', w_re, back_im, precision=HIGHEST) - jnp.einsum('pr,pfm->frm', w_im, back_re, precision=HIGHEST)
        folded = jnp.stack([fold_re, fold_im], 2).astype(jnp.bfloat16).reshape(N_FACET * R, 2 * M)
        spectra_back = jnp.dot(folded, backward, preferred_element_type=jnp.float32).reshape(N_FACET, R, 2, L)
        update_re = spectra_back[:, :, 0] * mod_cos - spectra_back[:, :, 1] * mod_sin
        update_im = spectra_back[:, :, 1] * mod_cos + spectra_back[:, :, 0] * mod_sin
        return (total + jnp.stack([update_re, update_im], 1), None)
    start_total = jnp.zeros((N_FACET, 2, R, L), jnp.float32)
    total, _ = lax.scan(one_subgrid, start_total, jnp.arange(NS, dtype=jnp.int32))
    return total
```

```python
import functools
import math

import jax
import jax.numpy as jnp
import ml_dtypes
import numpy as np
from jax import lax
from jax.experimental import pallas as pl
from jax.experimental.pallas import tpu as pltpu
from jax.sharding import PartitionSpec as P

M = 128
LANES = 128
FINE = 16
TWO_PI = 2.0 * math.pi
BF = jnp.bfloat16
F32 = jnp.float32
MESH = pl.DeviceIdType.MESH


def sincos(turns, period):
    shift = period.bit_length() - 3
    quad = (turns + (1 << (shift - 1))) >> shift
    t = (turns - (quad << shift)).astype(F32) * (TWO_PI / period)
    t2 = t * t
    s = t * (1.0 + t2 * (-1.0 / 6 + t2 * (1.0 / 120 + t2 * (-1.0 / 5040))))
    c = 1.0 + t2 * (-0.5 + t2 * (1.0 / 24 + t2 * (-1.0 / 720 + t2 * (1.0 / 40320))))
    odd = (quad & 1) != 0
    cos = jnp.where(odd, s, c)
    sin = jnp.where(odd, c, s)
    cos = jnp.where(((quad + 1) & 2) != 0, -cos, cos)
    sin = jnp.where((quad & 2) != 0, -sin, sin)
    return cos, sin


def mm(left, right):
    return jnp.dot(left, right, preferred_element_type=F32)


def mm_nt(left, right):
    return lax.dot_general(left, right, (((1,), (1,)), ((), ())), preferred_element_type=F32)


def cat(parts, axis):
    return jnp.concatenate(parts, axis)


def iota(shape, dim):
    return lax.broadcasted_iota(jnp.int32, shape, dim)


def body(dims, *refs):
    (sub_hbm, fac_hbm, cnt_hbm, rows_hbm, aterm_hbm, cells_hbm, obs_hbm, wt_hbm, kk_hbm, kt_hbm, kb_hbm) = refs[:11]
    out_hbm = refs[11]
    (
        sub_off, fac_off, counts, rows, aterm, cells, observed, weights, kk, kt, kb,
        spec_out, got1, slot_out, got_x, fold_out, got2, out_buf,
        tw1, tw2, wt_near, wt_far, fine, col_w, row_c, row_s, res,
        send1, recv1, send_x, recv_x, send2, recv2, in_sem, out_sem,
    ) = refs[12:]
    nf, nt, nb, length, size, rdev = dims
    rall = rdev * nt
    n = nf * nt
    slots = cells.shape[-1]
    period = 4 * size
    tiles = length // LANES
    my_f = lax.axis_index("facet")
    my_t = lax.axis_index("team")
    my_b = lax.axis_index("sub")
    me = my_f * nt + my_t
    other = 1 - my_b

    fetches = [
        pltpu.make_async_copy(sub_hbm, sub_off, in_sem.at[0]),
        pltpu.make_async_copy(rows_hbm, rows, in_sem.at[1]),
        pltpu.make_async_copy(fac_hbm, fac_off, in_sem.at[2]),
        pltpu.make_async_copy(cnt_hbm, counts, in_sem.at[3]),
        pltpu.make_async_copy(cells_hbm.at[0, my_b, 0], cells, in_sem.at[4]),
        pltpu.make_async_copy(obs_hbm.at[0, my_b, 0], observed, in_sem.at[5]),
        pltpu.make_async_copy(wt_hbm, weights, in_sem.at[6]),
        pltpu.make_async_copy(kt_hbm, kt, in_sem.at[7]),
        pltpu.make_async_copy(kk_hbm, kk, in_sem.at[8]),
        pltpu.make_async_copy(aterm_hbm.at[0, my_b], aterm, in_sem.at[9]),
        pltpu.make_async_copy(kb_hbm, kb, in_sem.at[10]),
    ]
    for fetch in fetches:
        fetch.start()

    barrier = pltpu.get_barrier_semaphore()

    def peer_of(q):
        f = lax.rem(my_f + lax.rem(q + 1, nf), nf)
        t = lax.rem(my_t + lax.rem(q // nf + 1, nt), nt)
        return f, t

    def greet(q, carry):
        f, t = peer_of(q)
        pl.semaphore_signal(
            barrier, inc=1, device_id={"facet": f, "team": t, "sub": my_b}, device_id_type=MESH
        )
        return carry

    lax.fori_loop(0, n - 1, greet, 0)
    for f in range(nf):
        pl.semaphore_signal(
            barrier, inc=1, device_id={"facet": f, "team": my_t, "sub": other}, device_id_type=MESH
        )

    base_c, base_s = sincos(iota((M, LANES), 0) * iota((M, LANES), 1), length)
    lane_row = iota((1, LANES), 1)

    fetches[0].wait()

    def column_weights(shift_v):
        pc, ps = sincos(lane_row * shift_v, length)
        c = (base_c * pc - base_s * ps).astype(BF)
        s = (base_s * pc + base_c * ps).astype(BF)
        return cat([cat([c, s], 1), cat([-s, c], 1)], 0)

    scale = 1.0 / math.sqrt(length)
    for a in range(nf):
        shift_v = sub_off[1, a * nb + my_b]
        wt_near[a] = column_weights(shift_v)
        c, s = sincos(iota((tiles, M), 0) * (iota((tiles, M), 1) + shift_v), tiles)
        tw1[a, 0] = c * scale
        tw1[a, 1] = s * scale
    fetches[1].wait()
    x = [
        cat([rows[0, c, :, k * LANES : (k + 1) * LANES].astype(F32) for k in range(tiles)], 0)
        for c in range(2)
    ]
    x = cat(x, 1).astype(BF)
    for a in range(nf):
        y = mm_nt(x, wt_near[a])
        acc = [None] * 4
        for k in range(tiles):
            yr = y[k * rdev : (k + 1) * rdev, :M]
            yi = y[k * rdev : (k + 1) * rdev, M:]
            c = tw1[a, 0, k : k + 1, :]
            s = tw1[a, 1, k : k + 1, :]
            q = 2 * (k % 2)
            add_re = yr * c + yi * s
            add_im = yi * c - yr * s
            acc[q] = add_re if acc[q] is None else acc[q] + add_re
            acc[q + 1] = add_im if acc[q + 1] is None else acc[q + 1] + add_im
        spec_out[a] = cat([acc[0] + acc[2], acc[1] + acc[3]], 1).astype(BF)

    for i in (2, 3, 4, 5, 6):
        fetches[i].wait()
    live = iota((1, slots), 1) < counts[my_f, my_b, my_t]
    all_wt = weights[0, 0].astype(F32)
    own_wt = jnp.where(my_b == 0, all_wt[0:1, :], all_wt[1:2, :])
    own_wt = jnp.where(live, own_wt, 0.0)
    packed = cat(
        [cells[...].astype(F32), observed[...].astype(F32), own_wt, jnp.zeros((3, slots), F32)], 0
    )
    slot_out[...] = packed
    got_x[my_t] = packed

    pl.semaphore_wait(barrier, n - 1 + nf)

    def copy_x(k):
        return pltpu.make_async_remote_copy(
            src_ref=slot_out,
            dst_ref=got_x.at[my_t],
            send_sem=send_x,
            recv_sem=recv_x.at[my_t],
            device_id={"facet": my_f, "team": lax.rem(my_t + k, nt), "sub": my_b},
            device_id_type=MESH,
        )

    def copy1(q):
        f, t = peer_of(q)
        return pltpu.make_async_remote_copy(
            src_ref=spec_out.at[f],
            dst_ref=got1.at[me],
            send_sem=send1,
            recv_sem=recv1,
            device_id={"facet": f, "team": t, "sub": my_b},
            device_id_type=MESH,
        )

    for k in range(1, nt):
        copy_x(k).start()

    def start1(q, carry):
        copy1(q).start()
        return carry

    lax.fori_loop(0, n - 1, start1, 0)
    got1[me] = spec_out[my_f]

    for i in (7, 8, 9, 10):
        fetches[i].wait()
    shift_u = sub_off[0, my_f * nb + my_b]
    step = length // rall
    scale_g = 1.0 / math.sqrt(rall * nf)
    lane = iota((1, n * rdev), 1)
    col_a = jnp.zeros((1, n * rdev), jnp.int32)
    row = iota((n * rdev, 1), 0)
    row_cc = jnp.zeros((n * rdev, 1), jnp.int32)
    row2 = iota((nf * rdev, 1), 0)
    row_a = jnp.zeros((nf * rdev, 1), jnp.int32)
    for f in range(nf):
        col_a = jnp.where(lane // rall == f, fac_off[0, f], col_a)
        row_cc = jnp.where(row // rall == f, fac_off[1, f], row_cc)
        row_a = jnp.where(row2 // rdev == f, fac_off[0, f], row_a)
    p0 = iota((M, n * rdev), 0)
    gc, gs = sincos(p0 * col_a - (p0 + shift_u) * (lane % rall * step), length)
    gc = (gc * scale_g).astype(BF)
    gs = (gs * scale_g).astype(BF)
    a_mat = mm(kt[...], cat([cat([gc, gs], 1), cat([-gs, gc], 1)], 0)).astype(BF)
    p1 = iota((nf * rdev, M), 1)
    hc, hs = sincos(p1 * row_a - (p1 + shift_u) * ((row2 % rdev + my_t * rdev) * step), length)
    at = mm(cat([hc * scale_g, hs * scale_g], 1).astype(BF), kk[...])
    ah = cat([at[:, :size], -at[:, size:]], 1).astype(BF)
    ec, es = sincos(iota((n * rdev, M), 1) * row_cc, length)

    half = tiles // nb
    scale_b = 1.0 / (math.sqrt(M) * size)
    tile_no = iota((half, M), 0) + my_b * half
    for far in range(2):
        for a in range(nf):
            shift_v = sub_off[1, a * nb + (other if far else my_b)]
            if far:
                wt_far[a] = column_weights(shift_v)
            m_no = iota((half, M), 1)
            c, s = sincos((m_no + shift_v) * (tile_no * LANES) - m_no * fac_off[1, my_f], length)
            tw2[far, a, 0] = c * scale_b
            tw2[far, a, 1] = s * scale_b

    fine_no = iota((FINE, slots), 0)
    coarse = size // FINE
    coarse_no = iota((coarse, slots), 0) * FINE
    for k in range(nt):
        src = lax.rem(my_t + k, nt)
        if k:
            pltpu.make_async_copy(got_x.at[src], got_x.at[src], recv_x.at[src]).wait()
        pos = got_x[src, 0:2, :].astype(jnp.int32)
        for axis in range(2):
            lo_c, lo_s = sincos(fine_no * pos[axis : axis + 1, :], period)
            hi_c, hi_s = sincos(coarse_no * pos[axis : axis + 1, :], period)
            fine[0] = hi_c
            fine[1] = hi_s
            for q in range(coarse):
                c1 = fine[0, q : q + 1, :]
                s1 = fine[1, q : q + 1, :]
                c = c1 * lo_c - s1 * lo_s
                s = s1 * lo_c + c1 * lo_s
                rng = slice(q * FINE, (q + 1) * FINE)
                if axis == 0:
                    row_c[k, rng, :] = c
                    row_s[k, rng, :] = s
                else:
                    cb = c.astype(BF)
                    sb = s.astype(BF)
                    low = slice(size + q * FINE, size + (q + 1) * FINE)
                    col_w[k, rng, :slots] = cb
                    col_w[k, rng, slots:] = -sb
                    col_w[k, low, :slots] = sb
                    col_w[k, low, slots:] = cb
    amap = aterm[...].astype(F32)
    amap = cat([amap, amap], 1)

    done = got1.at[pl.ds(0, n - 1)]
    pltpu.make_async_copy(done, done, recv1).wait()
    sp = got1[...].astype(F32).reshape(n * rdev, 2 * M)
    sr = sp[:, :M]
    si = sp[:, M:]
    turned = cat([sr * ec - si * es, sr * es + si * ec], 1).astype(BF)
    t = mm(turned, kk[...]).astype(BF)
    tr = t[:, :size]
    ti = t[:, size:]
    image = mm(a_mat, cat([t, cat([-ti, tr], 1)], 0))
    weighted = (amap * image).astype(BF)
    grid = None
    for k in range(nt):
        src = lax.rem(my_t + k, nt)
        z = mm(weighted, col_w[k])
        zr = z[:, :slots]
        zi = z[:, slots:]
        rc = row_c[k]
        rs = row_s[k]
        pred_re = jnp.sum(rc * zr + rs * zi, 0, keepdims=True) * (1.0 / size)
        pred_im = jnp.sum(rc * zi - rs * zr, 0, keepdims=True) * (1.0 / size)
        info = got_x[src]
        res_re = info[4:5, :] * (info[2:3, :] - pred_re)
        res_im = info[4:5, :] * (info[3:4, :] - pred_im)
        res[k, 0:1, :] = res_re
        res[k, 1:2, :] = res_im
    for k in range(nt):
        rc = row_c[k]
        rs = row_s[k]
        res_re = res[k, 0:1, :]
        res_im = res[k, 1:2, :]
        left = cat([rc * res_re - rs * res_im, rc * res_im + rs * res_re], 1).astype(BF)
        part = mm_nt(left, col_w[k])
        grid = part if grid is None else grid + part
    v = (amap * grid).astype(BF)
    u = mm(v, kb[...]).astype(BF)
    ur = u[:, :M]
    ui = u[:, M:]
    part = mm(ah, cat([u, cat([-ui, ur], 1)], 0))
    fold_out[...] = part.reshape(nf, rdev, 2 * M).astype(BF)


    def copy2(k, far):
        f = lax.rem(my_f + k, nf)
        return pltpu.make_async_remote_copy(
            src_ref=fold_out.at[f],
            dst_ref=got2.at[far, my_f],
            send_sem=send2,
            recv_sem=recv2.at[far],
            device_id={"facet": f, "team": my_t, "sub": other if far else my_b},
            device_id_type=MESH,
        )

    for k in range(1, nf + 1):
        copy2(k % nf, 1).start()
    for k in range(1, nf):
        copy2(k, 0).start()
    got2[0, my_f] = fold_out[my_f]

    def update(far):
        left = []
        for a in range(nf):
            g = got2[far, a].astype(F32)
            gr = g[:, :M]
            gi = g[:, M:]
            parts = []
            for k in range(half):
                c = tw2[far, a, 0, k : k + 1, :]
                s = tw2[far, a, 1, k : k + 1, :]
                parts.append(cat([gr * c - gi * s, gr * s + gi * c], 1))
            left.append(cat(parts, 0).astype(BF))
        wts = wt_far if far else wt_near
        total = None
        for a in range(nf):
            y = mm(left[a], wts[a])
            total = y if total is None else total + y
        return total

    done = got2.at[0, pl.ds(0, nf - 1)]
    pltpu.make_async_copy(done, done, recv2.at[0]).wait()
    near = update(0)
    done = got2.at[1]
    pltpu.make_async_copy(done, done, recv2.at[1]).wait()
    total = near + update(1)
    for k in range(half):
        rng = slice(k * rdev, (k + 1) * rdev)
        lanes = slice(k * LANES, (k + 1) * LANES)
        out_buf[0, 0, :, lanes] = total[rng, :LANES]
        out_buf[0, 1, :, lanes] = total[rng, LANES:]
    write = pltpu.make_async_copy(out_buf, out_hbm, out_sem)
    write.start()
    for k in range(1, nt):
        copy_x(k).wait_send()
    sent = got1.at[pl.ds(0, n - 1)]
    pltpu.make_async_copy(sent, sent, send1).wait()
    sent = got1.at[pl.ds(0, 2 * nf - 1)]
    pltpu.make_async_copy(sent, sent, send2).wait()
    write.wait()


def tables(size):
    angle = (np.arange(M)[:, None] * np.arange(size)[None, :] % size) * (TWO_PI / size)
    kc = np.cos(angle) / math.sqrt(M)
    ks = np.sin(angle) / math.sqrt(M)
    kk = np.block([[kc, ks], [-ks, kc]])
    kt = np.concatenate([kc.T, ks.T], 1)
    kb = np.block([[kc.T, -ks.T], [ks.T, kc.T]])
    return [np.asarray(v, np.float32).astype(ml_dtypes.bfloat16) for v in (kk, kt, kb)]


def local(facet_rows, sub_offsets, facet_offsets, aterm, cells, observed, weights, counts):
    nf = lax.axis_size("facet")
    nt = lax.axis_size("team")
    nb = lax.axis_size("sub")
    rdev, length = facet_rows.shape[2:]
    size = aterm.shape[-1]
    slots = cells.shape[-1]
    n = nf * nt
    tiles = length // LANES
    dims = (nf, nt, nb, length, size, rdev)
    consts = [jnp.asarray(v) for v in tables(size)]
    hbm = pl.BlockSpec(memory_space=pltpu.HBM)
    operands = [
        sub_offsets.T, facet_offsets.T, counts, facet_rows, aterm, cells, observed,
        weights.transpose(0, 2, 1, 3), *consts,
    ]
    dma = pltpu.SemaphoreType.DMA
    vmem = pltpu.VMEM
    return pl.pallas_call(
        functools.partial(body, dims),
        out_shape=jax.ShapeDtypeStruct((1, 2, rdev, length // nb), F32),
        in_specs=[hbm] * 11,
        out_specs=hbm,
        scratch_shapes=[
            *[pltpu.SMEM(v.shape, v.dtype) for v in operands[:3]],
            vmem(facet_rows.shape, BF),
            vmem((size, size), BF),
            vmem((2, slots), jnp.int32),
            vmem((2, slots), BF),
            *[vmem(v.shape, v.dtype) for v in operands[7:]],
            vmem((nf, rdev, 2 * M), BF),
            vmem((n, rdev, 2 * M), BF),
            vmem((8, slots), F32),
            vmem((nt, 8, slots), F32),
            vmem((nf, rdev, 2 * M), BF),
            vmem((nb, nf, rdev, 2 * M), BF),
            vmem((1, 2, rdev, length // nb), F32),
            vmem((nf, 2, tiles, M), F32),
            vmem((nb, nf, 2, tiles // nb, M), F32),
            vmem((nf, 2 * M, 2 * LANES), BF),
            vmem((nf, 2 * M, 2 * LANES), BF),
            vmem((2, size // FINE, slots), F32),
            vmem((nt, 2 * size, 2 * slots), BF),
            vmem((nt, size, slots), F32),
            vmem((nt, size, slots), F32),
            vmem((nt, 8, slots), F32),
            dma, dma, dma, dma((nt,)), dma, dma((nb,)), dma((11,)), dma,
        ],
        compiler_params=pltpu.CompilerParams(
            collective_id=0, has_side_effects=True
        ),
    )(*operands)


def solution(mesh):
    placed = (
        P("facet", None, "team", None),
        P(),
        P(),
        P("facet", None, None, None),
        P("facet", None, "team", None, None),
        P("facet", None, "team", None, None),
        P("facet", None, "team", None),
        P(),
    )
    return jax.shard_map(
        local,
        mesh=mesh,
        in_specs=placed,
        out_specs=P("facet", None, "team", "sub"),
        check_vma=False,
    )
```

```python
import functools
import math

import jax
import jax.numpy as jnp
import ml_dtypes
import numpy as np
from jax import lax
from jax.experimental import pallas as pl
from jax.experimental.pallas import tpu as pltpu
from jax.sharding import PartitionSpec as P

M = 128
LANES = 128
FINE = 16
HALF_BITS = 5
TWO_PI = 2.0 * math.pi
BF = jnp.bfloat16
F32 = jnp.float32
MESH = pl.DeviceIdType.MESH


def sincos(turns, period):
    shift = period.bit_length() - 3
    quad = (turns + (1 << (shift - 1))) >> shift
    t = (turns - (quad << shift)).astype(F32) * (TWO_PI / period)
    t2 = t * t
    s = t * (1.0 + t2 * (-1.0 / 6 + t2 * (1.0 / 120 + t2 * (-1.0 / 5040))))
    c = 1.0 + t2 * (-0.5 + t2 * (1.0 / 24 + t2 * (-1.0 / 720 + t2 * (1.0 / 40320))))
    odd = (quad & 1) != 0
    cos = jnp.where(odd, s, c)
    sin = jnp.where(odd, c, s)
    cos = jnp.where(((quad + 1) & 2) != 0, -cos, cos)
    sin = jnp.where((quad & 2) != 0, -sin, sin)
    return cos, sin


def mm(left, right):
    return jnp.dot(left, right, preferred_element_type=F32)


def mm_nt(left, right):
    return lax.dot_general(left, right, (((1,), (1,)), ((), ())), preferred_element_type=F32)


def cat(parts, axis):
    return jnp.concatenate(parts, axis)


def iota(shape, dim):
    return lax.broadcasted_iota(jnp.int32, shape, dim)


def body(dims, *refs):
    (sub_hbm, fac_hbm, cnt_hbm, rows_hbm, aterm_hbm, cells_hbm, obs_hbm, wt_hbm, kk_hbm, kt_hbm, kb_hbm) = refs[:11]
    out = refs[11]
    (
        sub_off, fac_off, counts, rows, aterm, cells, observed, weights, kk, kt, kb,
        spec_out, got1, slot_out, got_x, fold_out, got2,
        tw1, tw2, wt_near, wt_far, fine, col_w, row_c, row_s, res,
        send1, recv1, send_x, recv_x, send2, recv2, in_sem,
    ) = refs[12:]
    nf, nt, nb, length, size, rdev = dims
    rall = rdev * nt
    n = nf * nt
    slots = cells.shape[-1]
    period = 4 * size
    tiles = length // LANES
    my_f = lax.axis_index("facet")
    my_t = lax.axis_index("team")
    my_b = lax.axis_index("sub")
    me = my_f * nt + my_t
    other = 1 - my_b

    fetches = [
        pltpu.make_async_copy(sub_hbm, sub_off, in_sem.at[0]),
        pltpu.make_async_copy(rows_hbm, rows, in_sem.at[1]),
        pltpu.make_async_copy(fac_hbm, fac_off, in_sem.at[2]),
        pltpu.make_async_copy(cnt_hbm, counts, in_sem.at[3]),
        pltpu.make_async_copy(cells_hbm.at[0, my_b, 0], cells, in_sem.at[4]),
        pltpu.make_async_copy(obs_hbm.at[0, my_b, 0], observed, in_sem.at[5]),
        pltpu.make_async_copy(wt_hbm, weights, in_sem.at[6]),
        pltpu.make_async_copy(kt_hbm, kt, in_sem.at[7]),
        pltpu.make_async_copy(kk_hbm, kk, in_sem.at[8]),
        pltpu.make_async_copy(aterm_hbm.at[0, my_b], aterm, in_sem.at[9]),
        pltpu.make_async_copy(kb_hbm, kb, in_sem.at[10]),
    ]
    for fetch in fetches:
        fetch.start()

    barrier = pltpu.get_barrier_semaphore()

    def peer_of(q):
        f = lax.rem(my_f + lax.rem(q + 1, nf), nf)
        t = lax.rem(my_t + lax.rem(q // nf + 1, nt), nt)
        return f, t

    def greet(q, carry):
        f, t = peer_of(q)
        pl.semaphore_signal(
            barrier, inc=1, device_id={"facet": f, "team": t, "sub": my_b}, device_id_type=MESH
        )
        return carry

    lax.fori_loop(0, n - 1, greet, 0)
    for f in range(nf):
        pl.semaphore_signal(
            barrier, inc=1, device_id={"facet": f, "team": my_t, "sub": other}, device_id_type=MESH
        )

    base_c, base_s = sincos(iota((M, LANES), 0) * iota((M, LANES), 1), length)
    lane_row = iota((1, LANES), 1)

    fetches[0].wait()

    def column_weights(shift_v):
        pc, ps = sincos(lane_row * shift_v, length)
        c = (base_c * pc - base_s * ps).astype(BF)
        s = (base_s * pc + base_c * ps).astype(BF)
        return cat([cat([c, s], 1), cat([-s, c], 1)], 0)

    scale = 1.0 / math.sqrt(length)
    for a in range(nf):
        shift_v = sub_off[1, a * nb + my_b]
        wt_near[a] = column_weights(shift_v)
        c, s = sincos(iota((tiles, M), 0) * (iota((tiles, M), 1) + shift_v), tiles)
        tw1[a, 0] = c * scale
        tw1[a, 1] = s * scale
    fetches[1].wait()
    x = [
        cat([rows[0, c, :, k * LANES : (k + 1) * LANES].astype(F32) for k in range(tiles)], 0)
        for c in range(2)
    ]
    x = cat(x, 1).astype(BF)
    for a in range(nf):
        y = mm_nt(x, wt_near[a])
        acc = [None] * 4
        for k in range(tiles):
            yr = y[k * rdev : (k + 1) * rdev, :M]
            yi = y[k * rdev : (k + 1) * rdev, M:]
            c = tw1[a, 0, k : k + 1, :]
            s = tw1[a, 1, k : k + 1, :]
            q = 2 * (k % 2)
            add_re = yr * c + yi * s
            add_im = yi * c - yr * s
            acc[q] = add_re if acc[q] is None else acc[q] + add_re
            acc[q + 1] = add_im if acc[q + 1] is None else acc[q + 1] + add_im
        spec_out[a] = cat([acc[0] + acc[2], acc[1] + acc[3]], 1).astype(BF)

    for i in (2, 3, 4, 5, 6):
        fetches[i].wait()
    live = iota((1, slots), 1) < counts[my_f, my_b, my_t]
    all_wt = weights[0, 0].astype(F32)
    own_wt = jnp.where(my_b == 0, all_wt[0:1, :], all_wt[1:2, :])
    own_wt = jnp.where(live, own_wt, 0.0)
    place = cells[...]
    packed = cat(
        [
            (place >> HALF_BITS).astype(F32), (place & ((1 << HALF_BITS) - 1)).astype(F32),
            observed[...].astype(F32), own_wt, own_wt,
        ],
        0,
    ).astype(BF)
    slot_out[...] = packed
    got_x[my_t] = packed

    pl.semaphore_wait(barrier, n - 1 + nf)

    def copy_x(k):
        return pltpu.make_async_remote_copy(
            src_ref=slot_out,
            dst_ref=got_x.at[my_t],
            send_sem=send_x,
            recv_sem=recv_x.at[my_t],
            device_id={"facet": my_f, "team": lax.rem(my_t + k, nt), "sub": my_b},
            device_id_type=MESH,
        )

    def copy1(df, dt):
        f = lax.rem(my_f + df, nf)
        t = lax.rem(my_t + dt, nt)
        return pltpu.make_async_remote_copy(
            src_ref=spec_out.at[f],
            dst_ref=got1.at[me],
            send_sem=send1,
            recv_sem=recv1,
            device_id={"facet": f, "team": t, "sub": my_b},
            device_id_type=MESH,
        )

    for dt in range(1, nt + 1):
        if dt < nt:
            copy_x(dt).start()
        for df in range(nf):
            df = (df + nf // 2) % nf
            if df or dt < nt:
                copy1(df, dt % nt).start()
    got1[me] = spec_out[my_f]

    for i in (7, 8, 9, 10):
        fetches[i].wait()
    shift_u = sub_off[0, my_f * nb + my_b]
    step = length // rall
    scale_g = 1.0 / math.sqrt(rall * nf)
    lane = iota((1, n * rdev), 1)
    col_a = jnp.zeros((1, n * rdev), jnp.int32)
    row = iota((n * rdev, 1), 0)
    row_cc = jnp.zeros((n * rdev, 1), jnp.int32)
    row2 = iota((nf * rdev, 1), 0)
    row_a = jnp.zeros((nf * rdev, 1), jnp.int32)
    for f in range(nf):
        col_a = jnp.where(lane // rall == f, fac_off[0, f], col_a)
        row_cc = jnp.where(row // rall == f, fac_off[1, f], row_cc)
        row_a = jnp.where(row2 // rdev == f, fac_off[0, f], row_a)
    p0 = iota((M, n * rdev), 0)
    gc, gs = sincos(p0 * col_a - (p0 + shift_u) * (lane % rall * step), length)
    gc = (gc * scale_g).astype(BF)
    gs = (gs * scale_g).astype(BF)
    a_mat = mm(kt[...], cat([cat([gc, gs], 1), cat([-gs, gc], 1)], 0)).astype(BF)
    p1 = iota((nf * rdev, M), 1)
    hc, hs = sincos(p1 * row_a - (p1 + shift_u) * ((row2 % rdev + my_t * rdev) * step), length)
    at = mm(cat([hc * scale_g, hs * scale_g], 1).astype(BF), kk[...])
    ah = cat([at[:, :size], -at[:, size:]], 1).astype(BF)
    ec, es = sincos(iota((n * rdev, M), 1) * row_cc, length)

    half = tiles // nb
    scale_b = 1.0 / (math.sqrt(M) * size)
    tile_no = iota((half, M), 0) + my_b * half
    for far in range(2):
        for a in range(nf):
            shift_v = sub_off[1, a * nb + (other if far else my_b)]
            if far:
                wt_far[a] = column_weights(shift_v)
            m_no = iota((half, M), 1)
            c, s = sincos((m_no + shift_v) * (tile_no * LANES) - m_no * fac_off[1, my_f], length)
            tw2[far, a, 0] = c * scale_b
            tw2[far, a, 1] = s * scale_b

    fine_no = iota((FINE, slots), 0)
    coarse = size // FINE
    coarse_no = iota((coarse, slots), 0) * FINE
    for k in range(nt):
        src = lax.rem(my_t + k, nt)
        if k:
            pltpu.make_async_copy(got_x.at[src], got_x.at[src], recv_x.at[src]).wait()
        pos = got_x[src].astype(F32)[0:4, :].astype(jnp.int32)
        pos = (pos[0:2, :] << HALF_BITS) + pos[2:4, :]
        for axis in range(2):
            lo_c, lo_s = sincos(fine_no * pos[axis : axis + 1, :], period)
            hi_c, hi_s = sincos(coarse_no * pos[axis : axis + 1, :], period)
            fine[0] = hi_c
            fine[1] = hi_s
            for q in range(coarse):
                c1 = fine[0, q : q + 1, :]
                s1 = fine[1, q : q + 1, :]
                c = c1 * lo_c - s1 * lo_s
                s = s1 * lo_c + c1 * lo_s
                rng = slice(q * FINE, (q + 1) * FINE)
                if axis == 0:
                    row_c[k, rng, :] = c
                    row_s[k, rng, :] = s
                else:
                    cb = c.astype(BF)
                    sb = s.astype(BF)
                    low = slice(size + q * FINE, size + (q + 1) * FINE)
                    col_w[k, rng, :slots] = cb
                    col_w[k, rng, slots:] = -sb
                    col_w[k, low, :slots] = sb
                    col_w[k, low, slots:] = cb
    amap = aterm[...].astype(F32)
    amap = cat([amap, amap], 1)

    done = got1.at[pl.ds(0, n - 1)]
    pltpu.make_async_copy(done, done, recv1).wait()
    sp = got1[...].astype(F32).reshape(n * rdev, 2 * M)
    sr = sp[:, :M]
    si = sp[:, M:]
    turned = cat([sr * ec - si * es, sr * es + si * ec], 1).astype(BF)
    t = mm(turned, kk[...]).astype(BF)
    tr = t[:, :size]
    ti = t[:, size:]
    image = mm(a_mat, cat([t, cat([-ti, tr], 1)], 0))
    weighted = (amap * image).astype(BF)
    grid = None
    for k in range(nt):
        src = lax.rem(my_t + k, nt)
        z = mm(weighted, col_w[k])
        zr = z[:, :slots]
        zi = z[:, slots:]
        rc = row_c[k]
        rs = row_s[k]
        pred_re = jnp.sum(rc * zr + rs * zi, 0, keepdims=True) * (1.0 / size)
        pred_im = jnp.sum(rc * zi - rs * zr, 0, keepdims=True) * (1.0 / size)
        info = got_x[src].astype(F32)
        res_re = info[6:7, :] * (info[4:5, :] - pred_re)
        res_im = info[6:7, :] * (info[5:6, :] - pred_im)
        res[k, 0:1, :] = res_re
        res[k, 1:2, :] = res_im
    for k in range(nt):
        rc = row_c[k]
        rs = row_s[k]
        res_re = res[k, 0:1, :]
        res_im = res[k, 1:2, :]
        left = cat([rc * res_re - rs * res_im, rc * res_im + rs * res_re], 1).astype(BF)
        part = mm_nt(left, col_w[k])
        grid = part if grid is None else grid + part
    v = (amap * grid).astype(BF)
    u = mm(v, kb[...]).astype(BF)
    ur = u[:, :M]
    ui = u[:, M:]
    part = mm(ah, cat([u, cat([-ui, ur], 1)], 0))
    fold_out[...] = part.reshape(nf, rdev, 2 * M).astype(BF)


    def copy2(k, far):
        f = lax.rem(my_f + k, nf)
        return pltpu.make_async_remote_copy(
            src_ref=fold_out.at[f],
            dst_ref=got2.at[far, my_f],
            send_sem=send2,
            recv_sem=recv2.at[far],
            device_id={"facet": f, "team": my_t, "sub": other if far else my_b},
            device_id_type=MESH,
        )

    for k in range(1, nf + 1):
        copy2(k % nf, 1).start()
    for k in range(1, nf):
        copy2(k, 0).start()
    got2[0, my_f] = fold_out[my_f]

    def update(far):
        left = []
        for a in range(nf):
            g = got2[far, a].astype(F32)
            gr = g[:, :M]
            gi = g[:, M:]
            parts = []
            for k in range(half):
                c = tw2[far, a, 0, k : k + 1, :]
                s = tw2[far, a, 1, k : k + 1, :]
                parts.append(cat([gr * c - gi * s, gr * s + gi * c], 1))
            left.append(cat(parts, 0).astype(BF))
        wts = wt_far if far else wt_near
        total = None
        for a in range(nf):
            y = mm(left[a], wts[a])
            total = y if total is None else total + y
        return total

    done = got2.at[0, pl.ds(0, nf - 1)]
    pltpu.make_async_copy(done, done, recv2.at[0]).wait()
    near = update(0)
    done = got2.at[1]
    pltpu.make_async_copy(done, done, recv2.at[1]).wait()
    total = near + update(1)
    for k in range(half):
        rng = slice(k * rdev, (k + 1) * rdev)
        lanes = slice(k * LANES, (k + 1) * LANES)
        out[0, 0, :, lanes] = total[rng, :LANES]
        out[0, 1, :, lanes] = total[rng, LANES:]
    for k in range(1, nt):
        copy_x(k).wait_send()
    sent = got1.at[pl.ds(0, n - 1)]
    pltpu.make_async_copy(sent, sent, send1).wait()
    sent = got1.at[pl.ds(0, 2 * nf - 1)]
    pltpu.make_async_copy(sent, sent, send2).wait()


def tables(size):
    angle = (np.arange(M)[:, None] * np.arange(size)[None, :] % size) * (TWO_PI / size)
    kc = np.cos(angle) / math.sqrt(M)
    ks = np.sin(angle) / math.sqrt(M)
    kk = np.block([[kc, ks], [-ks, kc]])
    kt = np.concatenate([kc.T, ks.T], 1)
    kb = np.block([[kc.T, -ks.T], [ks.T, kc.T]])
    return [np.asarray(v, np.float32).astype(ml_dtypes.bfloat16) for v in (kk, kt, kb)]


def local(facet_rows, sub_offsets, facet_offsets, aterm, cells, observed, weights, counts):
    nf = lax.axis_size("facet")
    nt = lax.axis_size("team")
    nb = lax.axis_size("sub")
    rdev, length = facet_rows.shape[2:]
    size = aterm.shape[-1]
    slots = cells.shape[-1]
    n = nf * nt
    tiles = length // LANES
    dims = (nf, nt, nb, length, size, rdev)
    consts = [jnp.asarray(v) for v in tables(size)]
    hbm = pl.BlockSpec(memory_space=pltpu.HBM)
    operands = [
        sub_offsets.T, facet_offsets.T, counts, facet_rows, aterm, cells, observed,
        weights.transpose(0, 2, 1, 3), *consts,
    ]
    dma = pltpu.SemaphoreType.DMA
    vmem = pltpu.VMEM
    return pl.pallas_call(
        functools.partial(body, dims),
        out_shape=pltpu.VMEM((1, 2, rdev, length // nb), F32),
        in_specs=[hbm] * 11,
        out_specs=pl.BlockSpec(memory_space=pltpu.VMEM),
        scratch_shapes=[
            *[pltpu.SMEM(v.shape, v.dtype) for v in operands[:3]],
            vmem(facet_rows.shape, BF),
            vmem((size, size), BF),
            vmem((2, slots), jnp.int32),
            vmem((2, slots), BF),
            *[vmem(v.shape, v.dtype) for v in operands[7:]],
            vmem((nf, rdev, 2 * M), BF),
            vmem((n, rdev, 2 * M), BF),
            vmem((8, slots), BF),
            vmem((nt, 8, slots), BF),
            vmem((nf, rdev, 2 * M), BF),
            vmem((nb, nf, rdev, 2 * M), BF),
            vmem((nf, 2, tiles, M), F32),
            vmem((nb, nf, 2, tiles // nb, M), F32),
            vmem((nf, 2 * M, 2 * LANES), BF),
            vmem((nf, 2 * M, 2 * LANES), BF),
            vmem((2, size // FINE, slots), F32),
            vmem((nt, 2 * size, 2 * slots), BF),
            vmem((nt, size, slots), F32),
            vmem((nt, size, slots), F32),
            vmem((nt, 8, slots), F32),
            dma, dma, dma, dma((nt,)), dma, dma((nb,)), dma((11,)),
        ],
        compiler_params=pltpu.CompilerParams(
            collective_id=0, has_side_effects=True
        ),
    )(*operands)


def solution(mesh):
    placed = (
        P("facet", None, "team", None),
        P(),
        P(),
        P("facet", None, None, None),
        P("facet", None, "team", None, None),
        P("facet", None, "team", None, None),
        P("facet", None, "team", None),
        P(),
    )
    return jax.shard_map(
        local,
        mesh=mesh,
        in_specs=placed,
        out_specs=P("facet", None, "team", "sub"),
        check_vma=False,
    )
```

```python
import functools
import math

import jax
import jax.numpy as jnp
import ml_dtypes
import numpy as np
from jax import lax
from jax.experimental import pallas as pl
from jax.experimental.pallas import tpu as pltpu
from jax.sharding import PartitionSpec as P

M = 128
LANES = 128
FINE = 16
HALF_BITS = 5
TWO_PI = 2.0 * math.pi
BF = jnp.bfloat16
F32 = jnp.float32
MESH = pl.DeviceIdType.MESH


def sincos(turns, period):
    shift = period.bit_length() - 3
    quad = (turns + (1 << (shift - 1))) >> shift
    t = (turns - (quad << shift)).astype(F32) * (TWO_PI / period)
    t2 = t * t
    s = t * (1.0 + t2 * (-1.0 / 6 + t2 * (1.0 / 120 + t2 * (-1.0 / 5040))))
    c = 1.0 + t2 * (-0.5 + t2 * (1.0 / 24 + t2 * (-1.0 / 720 + t2 * (1.0 / 40320))))
    odd = (quad & 1) != 0
    cos = jnp.where(odd, s, c)
    sin = jnp.where(odd, c, s)
    cos = jnp.where(((quad + 1) & 2) != 0, -cos, cos)
    sin = jnp.where((quad & 2) != 0, -sin, sin)
    return cos, sin


def mm(left, right):
    return jnp.dot(left, right, preferred_element_type=F32)


def mm_nt(left, right):
    return lax.dot_general(left, right, (((1,), (1,)), ((), ())), preferred_element_type=F32)


def cat(parts, axis):
    return jnp.concatenate(parts, axis)


def iota(shape, dim):
    return lax.broadcasted_iota(jnp.int32, shape, dim)


def body(dims, *refs):
    (sub_hbm, fac_hbm, cnt_hbm, rows_hbm, aterm_hbm, cells_hbm, obs_hbm, wt_hbm, kk_hbm, kt_hbm, kb_hbm) = refs[:11]
    out = refs[11]
    (
        sub_off, fac_off, counts, rows, aterm, cells, observed, weights, kk, kt, kb,
        spec_out, got1, slot_out, got_x, fold_out, got2,
        tw1, tw2, wt_near, wt_far, fine, col_w, row_c, row_s, res,
        send1, recv1, send_x, recv_x, send2, recv2, in_sem,
    ) = refs[12:]
    nf, nt, nb, length, size, rdev = dims
    rall = rdev * nt
    n = nf * nt
    slots = cells.shape[-1]
    period = 4 * size
    tiles = length // LANES
    my_f = lax.axis_index("facet")
    my_t = lax.axis_index("team")
    my_b = lax.axis_index("sub")
    me = my_f * nt + my_t
    other = 1 - my_b

    fetches = [
        pltpu.make_async_copy(sub_hbm, sub_off, in_sem.at[0]),
        pltpu.make_async_copy(rows_hbm, rows, in_sem.at[1]),
        pltpu.make_async_copy(fac_hbm, fac_off, in_sem.at[2]),
        pltpu.make_async_copy(cnt_hbm, counts, in_sem.at[3]),
        pltpu.make_async_copy(cells_hbm.at[0, my_b, 0], cells, in_sem.at[4]),
        pltpu.make_async_copy(obs_hbm.at[0, my_b, 0], observed, in_sem.at[5]),
        pltpu.make_async_copy(wt_hbm, weights, in_sem.at[6]),
        pltpu.make_async_copy(kt_hbm, kt, in_sem.at[7]),
        pltpu.make_async_copy(kk_hbm, kk, in_sem.at[8]),
        pltpu.make_async_copy(aterm_hbm.at[0, my_b], aterm, in_sem.at[9]),
        pltpu.make_async_copy(kb_hbm, kb, in_sem.at[10]),
    ]
    for fetch in fetches:
        fetch.start()

    barrier = pltpu.get_barrier_semaphore()
    nc = 2 - nf % 2
    ny = nf // nc
    order = [(k // nc + ny // 2) % ny * nc + k % nc for k in range(nf)]
    urgent = [k for k in order if k >= nc]
    local_k = [k for k in order if k < nc]

    def facet_at(k):
        row = lax.rem(my_f // nc + k // nc, ny)
        return row * nc + lax.rem(my_f + k % nc, nc)

    def greet(k, t, b):
        pl.semaphore_signal(
            barrier, inc=1, device_id={"facet": facet_at(k), "team": t, "sub": b}, device_id_type=MESH
        )

    for t in range(nt):
        for k in order:
            if k:
                greet(k, t, my_b)
            else:
                pl.when(my_t != t)(functools.partial(greet, k, t, my_b))
        if t == 0:
            greet(0, my_t, other)
    base_c, base_s = sincos(iota((M, LANES), 0) * iota((M, LANES), 1), length)
    lane_row = iota((1, LANES), 1)

    fetches[0].wait()
    fetches[1].wait()

    def column_weights(shift_v):
        pc, ps = sincos(lane_row * shift_v, length)
        c = (base_c * pc - base_s * ps).astype(BF)
        s = (base_s * pc + base_c * ps).astype(BF)
        return cat([cat([c, s], 1), cat([-s, c], 1)], 0)

    scale = 1.0 / math.sqrt(length)
    x = [
        cat([rows[0, c, :, k * LANES : (k + 1) * LANES].astype(F32) for k in range(tiles)], 0)
        for c in range(2)
    ]
    x = cat(x, 1).astype(BF)

    def spectrum(k):
        shift_v = sub_off[1, facet_at(k) * nb + my_b]
        wt_near[k] = column_weights(shift_v)
        y = mm_nt(x, wt_near[k])
        c, s = sincos(iota((tiles, M), 0) * (iota((tiles, M), 1) + shift_v), tiles)
        tw1[k, 0] = c * scale
        tw1[k, 1] = s * scale
        acc = [None] * 4
        for j in range(tiles):
            yr = y[j * rdev : (j + 1) * rdev, :M]
            yi = y[j * rdev : (j + 1) * rdev, M:]
            c = tw1[k, 0, j : j + 1, :]
            s = tw1[k, 1, j : j + 1, :]
            q = 2 * (j % 2)
            add_re = yr * c + yi * s
            add_im = yi * c - yr * s
            acc[q] = add_re if acc[q] is None else acc[q] + add_re
            acc[q + 1] = add_im if acc[q + 1] is None else acc[q + 1] + add_im
        spec_out[k] = cat([acc[0] + acc[2], acc[1] + acc[3]], 1).astype(BF)

    for k in urgent:
        spectrum(k)
    for i in (2, 3, 4, 5, 6):
        fetches[i].wait()
    live = iota((1, slots), 1) < counts[my_f, my_b, my_t]
    all_wt = weights[0, 0].astype(F32)
    own_wt = jnp.where(my_b == 0, all_wt[0:1, :], all_wt[1:2, :])
    own_wt = jnp.where(live, own_wt, 0.0)
    place = cells[...]
    packed = cat(
        [
            (place >> HALF_BITS).astype(F32), (place & ((1 << HALF_BITS) - 1)).astype(F32),
            observed[...].astype(F32), own_wt, own_wt,
        ],
        0,
    ).astype(BF)
    slot_out[...] = packed
    got_x[my_t] = packed

    pl.semaphore_wait(barrier, n)

    def copy_x(t):
        return pltpu.make_async_remote_copy(
            src_ref=slot_out,
            dst_ref=got_x.at[my_t],
            send_sem=send_x,
            recv_sem=recv_x.at[my_t],
            device_id={"facet": my_f, "team": t, "sub": my_b},
            device_id_type=MESH,
        )

    def copy1(k, t):
        return pltpu.make_async_remote_copy(
            src_ref=spec_out.at[k],
            dst_ref=got1.at[me],
            send_sem=send1,
            recv_sem=recv1.at[my_t],
            device_id={"facet": facet_at(k), "team": t, "sub": my_b},
            device_id_type=MESH,
        )

    def send_specs(ks, t):
        for k in ks:
            if k:
                copy1(k, t).start()
            else:
                pl.when(my_t != t)(lambda: copy1(0, t).start())

    def send_slots(t):
        pl.when(my_t != t)(lambda: copy_x(t).start())

    send_specs(urgent, 0)
    send_slots(0)
    for k in local_k:
        spectrum(k)
    send_specs(local_k, 0)
    got1[me] = spec_out[0]

    for i in (7, 8, 9, 10):
        fetches[i].wait()
    shift_u = sub_off[0, my_f * nb + my_b]
    step = length // rall
    scale_g = 1.0 / math.sqrt(rall * nf)
    lane = iota((1, n * rdev), 1)
    col_a = jnp.zeros((1, n * rdev), jnp.int32)
    row = iota((n * rdev, 1), 0)
    row_cc = jnp.zeros((n * rdev, 1), jnp.int32)
    row2 = iota((nf * rdev, 1), 0)
    row_a = jnp.zeros((nf * rdev, 1), jnp.int32)
    for f in range(nf):
        col_a = jnp.where(lane // rall == f, fac_off[0, f], col_a)
        row_cc = jnp.where(row // rall == f, fac_off[1, f], row_cc)
        row_a = jnp.where(row2 // rdev == f, fac_off[0, f], row_a)
    p0 = iota((M, n * rdev), 0)
    gc, gs = sincos(p0 * col_a - (p0 + shift_u) * (lane % rall * step), length)
    gc = (gc * scale_g).astype(BF)
    gs = (gs * scale_g).astype(BF)
    a_mat = mm(kt[...], cat([cat([gc, gs], 1), cat([-gs, gc], 1)], 0)).astype(BF)
    p1 = iota((nf * rdev, M), 1)
    hc, hs = sincos(p1 * row_a - (p1 + shift_u) * ((row2 % rdev + my_t * rdev) * step), length)
    at = mm(cat([hc * scale_g, hs * scale_g], 1).astype(BF), kk[...])
    ah = cat([at[:, :size], -at[:, size:]], 1).astype(BF)
    ec, es = sincos(iota((n * rdev, M), 1) * row_cc, length)

    for t in range(1, nt):
        send_specs(order, t)
        send_slots(t)
    half = tiles // nb
    scale_b = 1.0 / (math.sqrt(M) * size)
    tile_no = iota((half, M), 0) + my_b * half
    for far in range(2):
        for a in range(nf):
            shift_v = sub_off[1, facet_at(a) * nb + (other if far else my_b)]
            if far:
                wt_far[a] = column_weights(shift_v)
            m_no = iota((half, M), 1)
            c, s = sincos((m_no + shift_v) * (tile_no * LANES) - m_no * fac_off[1, my_f], length)
            tw2[far, a, 0] = c * scale_b
            tw2[far, a, 1] = s * scale_b

    fine_no = iota((FINE, slots), 0)
    coarse = size // FINE
    coarse_no = iota((coarse, slots), 0) * FINE
    for k in range(nt):
        src = lax.rem(my_t + k, nt)
        if k:
            pltpu.make_async_copy(got_x.at[src], got_x.at[src], recv_x.at[src]).wait()
        pos = got_x[src].astype(F32)[0:4, :].astype(jnp.int32)
        pos = (pos[0:2, :] << HALF_BITS) + pos[2:4, :]
        for axis in range(2):
            lo_c, lo_s = sincos(fine_no * pos[axis : axis + 1, :], period)
            hi_c, hi_s = sincos(coarse_no * pos[axis : axis + 1, :], period)
            fine[0] = hi_c
            fine[1] = hi_s
            for q in range(coarse):
                c1 = fine[0, q : q + 1, :]
                s1 = fine[1, q : q + 1, :]
                c = c1 * lo_c - s1 * lo_s
                s = s1 * lo_c + c1 * lo_s
                rng = slice(q * FINE, (q + 1) * FINE)
                if axis == 0:
                    row_c[k, rng, :] = c
                    row_s[k, rng, :] = s
                else:
                    cb = c.astype(BF)
                    sb = s.astype(BF)
                    low = slice(size + q * FINE, size + (q + 1) * FINE)
                    col_w[k, rng, :slots] = cb
                    col_w[k, rng, slots:] = -sb
                    col_w[k, low, :slots] = sb
                    col_w[k, low, slots:] = cb
    amap = aterm[...].astype(F32)
    amap = cat([amap, amap], 1)

    for k in range(nt):
        src = lax.rem(my_t + k, nt)
        done = got1.at[pl.ds(0, nf if k else nf - 1)]
        pltpu.make_async_copy(done, done, recv1.at[src]).wait()
    sp = got1[...].astype(F32).reshape(n * rdev, 2 * M)
    sr = sp[:, :M]
    si = sp[:, M:]
    turned = cat([sr * ec - si * es, sr * es + si * ec], 1).astype(BF)
    t = mm(turned, kk[...]).astype(BF)
    tr = t[:, :size]
    ti = t[:, size:]
    image = mm(a_mat, cat([t, cat([-ti, tr], 1)], 0))
    weighted = (amap * image).astype(BF)
    grid = None
    for k in range(nt):
        src = lax.rem(my_t + k, nt)
        z = mm(weighted, col_w[k])
        zr = z[:, :slots]
        zi = z[:, slots:]
        rc = row_c[k]
        rs = row_s[k]
        pred_re = jnp.sum(rc * zr + rs * zi, 0, keepdims=True) * (1.0 / size)
        pred_im = jnp.sum(rc * zi - rs * zr, 0, keepdims=True) * (1.0 / size)
        info = got_x[src].astype(F32)
        res_re = info[6:7, :] * (info[4:5, :] - pred_re)
        res_im = info[6:7, :] * (info[5:6, :] - pred_im)
        res[k, 0:1, :] = res_re
        res[k, 1:2, :] = res_im
    for k in range(nt):
        rc = row_c[k]
        rs = row_s[k]
        res_re = res[k, 0:1, :]
        res_im = res[k, 1:2, :]
        left = cat([rc * res_re - rs * res_im, rc * res_im + rs * res_re], 1).astype(BF)
        part = mm_nt(left, col_w[k])
        grid = part if grid is None else grid + part
    v = (amap * grid).astype(BF)
    u = mm(v, kb[...]).astype(BF)
    ur = u[:, :M]
    ui = u[:, M:]
    part = mm(ah, cat([u, cat([-ui, ur], 1)], 0))
    fold_out[...] = part.reshape(nf, rdev, 2 * M).astype(BF)


    def copy2(k, far):
        return pltpu.make_async_remote_copy(
            src_ref=fold_out.at[facet_at(k)],
            dst_ref=got2.at[far, my_f],
            send_sem=send2,
            recv_sem=recv2.at[min(k // nc, 1) + far],
            device_id={"facet": facet_at(k), "team": my_t, "sub": other if far else my_b},
            device_id_type=MESH,
        )

    for k in urgent:
        copy2(k, 1).start()
    for k in local_k:
        copy2(k, 1).start()
    for k in urgent + local_k:
        if k:
            copy2(k, 0).start()
    got2[0, my_f] = fold_out[my_f]

    def update(total, far, ks):
        for k in ks:
            g = got2[far, facet_at(k)].astype(F32)
            gr = g[:, :M]
            gi = g[:, M:]
            parts = []
            for j in range(half):
                c = tw2[far, k, 0, j : j + 1, :]
                s = tw2[far, k, 1, j : j + 1, :]
                parts.append(cat([gr * c - gi * s, gr * s + gi * c], 1))
            y = mm(cat(parts, 0).astype(BF), (wt_far if far else wt_near)[k])
            total = y if total is None else total + y
        return total

    def arrived(which, count):
        done = got1.at[pl.ds(0, count)]
        pltpu.make_async_copy(done, done, recv2.at[which]).wait()

    if nc > 1:
        arrived(0, nc - 1)
    total = update(None, 0, local_k)
    arrived(1, nf)
    total = update(total, 1, local_k)
    total = update(total, 0, urgent)
    if ny > 1:
        arrived(2, nf - nc)
    total = update(total, 1, urgent)
    for k in range(half):
        rng = slice(k * rdev, (k + 1) * rdev)
        lanes = slice(k * LANES, (k + 1) * LANES)
        out[0, 0, :, lanes] = total[rng, :LANES]
        out[0, 1, :, lanes] = total[rng, LANES:]
    sent = got1.at[pl.ds(0, nt - 1)]
    pltpu.make_async_copy(sent, sent, send_x).wait()
    sent = got1.at[pl.ds(0, n - 1)]
    pltpu.make_async_copy(sent, sent, send1).wait()
    sent = got1.at[pl.ds(0, 2 * nf - 1)]
    pltpu.make_async_copy(sent, sent, send2).wait()


def tables(size):
    angle = (np.arange(M)[:, None] * np.arange(size)[None, :] % size) * (TWO_PI / size)
    kc = np.cos(angle) / math.sqrt(M)
    ks = np.sin(angle) / math.sqrt(M)
    kk = np.block([[kc, ks], [-ks, kc]])
    kt = np.concatenate([kc.T, ks.T], 1)
    kb = np.block([[kc.T, -ks.T], [ks.T, kc.T]])
    return [np.asarray(v, np.float32).astype(ml_dtypes.bfloat16) for v in (kk, kt, kb)]


def local(facet_rows, sub_offsets, facet_offsets, aterm, cells, observed, weights, counts):
    nf = lax.axis_size("facet")
    nt = lax.axis_size("team")
    nb = lax.axis_size("sub")
    rdev, length = facet_rows.shape[2:]
    size = aterm.shape[-1]
    slots = cells.shape[-1]
    n = nf * nt
    tiles = length // LANES
    dims = (nf, nt, nb, length, size, rdev)
    consts = [jnp.asarray(v) for v in tables(size)]
    hbm = pl.BlockSpec(memory_space=pltpu.HBM)
    operands = [
        sub_offsets.T, facet_offsets.T, counts, facet_rows, aterm, cells, observed,
        weights.transpose(0, 2, 1, 3), *consts,
    ]
    dma = pltpu.SemaphoreType.DMA
    vmem = pltpu.VMEM
    return pl.pallas_call(
        functools.partial(body, dims),
        out_shape=pltpu.VMEM((1, 2, rdev, length // nb), F32),
        in_specs=[hbm] * 11,
        out_specs=pl.BlockSpec(memory_space=pltpu.VMEM),
        scratch_shapes=[
            *[pltpu.SMEM(v.shape, v.dtype) for v in operands[:3]],
            vmem(facet_rows.shape, BF),
            vmem((size, size), BF),
            vmem((2, slots), jnp.int32),
            vmem((2, slots), BF),
            *[vmem(v.shape, v.dtype) for v in operands[7:]],
            vmem((nf, rdev, 2 * M), BF),
            vmem((n, rdev, 2 * M), BF),
            vmem((8, slots), BF),
            vmem((nt, 8, slots), BF),
            vmem((nf, rdev, 2 * M), BF),
            vmem((nb, nf, rdev, 2 * M), BF),
            vmem((nf, 2, tiles, M), F32),
            vmem((nb, nf, 2, tiles // nb, M), F32),
            vmem((nf, 2 * M, 2 * LANES), BF),
            vmem((nf, 2 * M, 2 * LANES), BF),
            vmem((2, size // FINE, slots), F32),
            vmem((nt, 2 * size, 2 * slots), BF),
            vmem((nt, size, slots), F32),
            vmem((nt, size, slots), F32),
            vmem((nt, 8, slots), F32),
            dma, dma((nt,)), dma, dma((nt,)), dma, dma((3,)), dma((11,)),
        ],
        compiler_params=pltpu.CompilerParams(
            collective_id=0, has_side_effects=True
        ),
    )(*operands)


def solution(mesh):
    placed = (
        P("facet", None, "team", None),
        P(),
        P(),
        P("facet", None, None, None),
        P("facet", None, "team", None, None),
        P("facet", None, "team", None, None),
        P("facet", None, "team", None),
        P(),
    )
    return jax.shard_map(
        local,
        mesh=mesh,
        in_specs=placed,
        out_specs=P("facet", None, "team", "sub"),
        check_vma=False,
    )
```

```python
import functools
import math

import jax
import jax.numpy as jnp
import ml_dtypes
import numpy as np
from jax import lax
from jax.experimental import pallas as pl
from jax.experimental.pallas import tpu as pltpu
from jax.sharding import PartitionSpec as P

M = 128
LANES = 128
FINE = 16
HALF_BITS = 5
TWO_PI = 2.0 * math.pi
BF = jnp.bfloat16
F32 = jnp.float32
MESH = pl.DeviceIdType.MESH


def sincos(turns, period):
    shift = period.bit_length() - 3
    quad = (turns + (1 << (shift - 1))) >> shift
    t = (turns - (quad << shift)).astype(F32) * (TWO_PI / period)
    t2 = t * t
    s = t * (1.0 + t2 * (-1.0 / 6 + t2 * (1.0 / 120 + t2 * (-1.0 / 5040))))
    c = 1.0 + t2 * (-0.5 + t2 * (1.0 / 24 + t2 * (-1.0 / 720 + t2 * (1.0 / 40320))))
    odd = (quad & 1) != 0
    cos = jnp.where(odd, s, c)
    sin = jnp.where(odd, c, s)
    cos = jnp.where(((quad + 1) & 2) != 0, -cos, cos)
    sin = jnp.where((quad & 2) != 0, -sin, sin)
    return cos, sin


def mm(left, right):
    return jnp.dot(left, right, preferred_element_type=F32)


def mm_nt(left, right):
    return lax.dot_general(left, right, (((1,), (1,)), ((), ())), preferred_element_type=F32)


def cat(parts, axis):
    return jnp.concatenate(parts, axis)


def iota(shape, dim):
    return lax.broadcasted_iota(jnp.int32, shape, dim)


def body(dims, *refs):
    (sub_hbm, fac_hbm, cnt_hbm, rows_hbm, aterm_hbm, cells_hbm, obs_hbm, wt_hbm, kk_hbm, kt_hbm) = refs[:10]
    out = refs[10]
    (
        sub_off, fac_off, counts, rows, aterm, cells, observed, weights, kk, kt,
        spec_out, got1, slot_out, got_x, fold_out, got2,
        tw1, tw2, wt_near, wt_far, fine, col_w, row_c, row_s,
        send1, recv1, send_x, recv_x, send2, recv2, in_sem,
    ) = refs[11:]
    nf, nt, nb, length, size, rdev = dims
    rall = rdev * nt
    n = nf * nt
    slots = cells.shape[-1]
    period = 4 * size
    tiles = length // LANES
    my_f = lax.axis_index("facet")
    my_t = lax.axis_index("team")
    my_b = lax.axis_index("sub")
    me = my_f * nt + my_t
    other = 1 - my_b

    fetches = [
        pltpu.make_async_copy(sub_hbm, sub_off, in_sem.at[0]),
        pltpu.make_async_copy(rows_hbm, rows, in_sem.at[1]),
        pltpu.make_async_copy(fac_hbm, fac_off, in_sem.at[2]),
        pltpu.make_async_copy(cnt_hbm, counts, in_sem.at[3]),
        pltpu.make_async_copy(cells_hbm.at[0, my_b, 0], cells, in_sem.at[4]),
        pltpu.make_async_copy(obs_hbm.at[0, my_b, 0], observed, in_sem.at[5]),
        pltpu.make_async_copy(wt_hbm, weights, in_sem.at[6]),
        pltpu.make_async_copy(kt_hbm, kt, in_sem.at[7]),
        pltpu.make_async_copy(kk_hbm, kk, in_sem.at[8]),
        pltpu.make_async_copy(aterm_hbm.at[0, my_b], aterm, in_sem.at[9]),
    ]
    for fetch in fetches[:7]:
        fetch.start()

    barrier = pltpu.get_barrier_semaphore()
    nc = 2 - nf % 2
    ny = nf // nc
    order = [(k // nc + ny // 2) % ny * nc + k % nc for k in range(nf)]
    urgent = [k for k in order if k >= nc]
    local_k = [k for k in order if k < nc]

    def facet_at(k):
        row = lax.rem(my_f // nc + k // nc, ny)
        return row * nc + lax.rem(my_f + k % nc, nc)

    def greet(k, t, b):
        pl.semaphore_signal(
            barrier, inc=1, device_id={"facet": facet_at(k), "team": t, "sub": b}, device_id_type=MESH
        )

    for t in range(nt):
        for k in order:
            if k:
                greet(k, t, my_b)
            else:
                pl.when(my_t != t)(functools.partial(greet, k, t, my_b))
        if t == 0:
            greet(0, my_t, other)
    base_c, base_s = sincos(iota((M, LANES), 0) * iota((M, LANES), 1), length)
    lane_row = iota((1, LANES), 1)

    fetches[0].wait()
    fetches[1].wait()
    for fetch in fetches[7:]:
        fetch.start()

    def column_weights(shift_v):
        pc, ps = sincos(lane_row * shift_v, length)
        c = (base_c * pc - base_s * ps).astype(BF)
        s = (base_s * pc + base_c * ps).astype(BF)
        return cat([cat([c, s], 1), cat([-s, c], 1)], 0)

    scale = 1.0 / math.sqrt(length)
    x = [
        cat([rows[0, c, :, k * LANES : (k + 1) * LANES].astype(F32) for k in range(tiles)], 0)
        for c in range(2)
    ]
    x = cat(x, 1).astype(BF)

    def spectrum(k):
        shift_v = sub_off[1, facet_at(k) * nb + my_b]
        wt_near[k] = column_weights(shift_v)
        y = mm_nt(x, wt_near[k])
        c, s = sincos(iota((tiles, M), 0) * (iota((tiles, M), 1) + shift_v), tiles)
        tw1[k, 0] = c * scale
        tw1[k, 1] = s * scale
        acc = [None] * 4
        for j in range(tiles):
            yr = y[j * rdev : (j + 1) * rdev, :M]
            yi = y[j * rdev : (j + 1) * rdev, M:]
            c = tw1[k, 0, j : j + 1, :]
            s = tw1[k, 1, j : j + 1, :]
            q = 2 * (j % 2)
            add_re = yr * c + yi * s
            add_im = yi * c - yr * s
            acc[q] = add_re if acc[q] is None else acc[q] + add_re
            acc[q + 1] = add_im if acc[q + 1] is None else acc[q + 1] + add_im
        spec_out[k] = cat([acc[0] + acc[2], acc[1] + acc[3]], 1).astype(BF)

    for k in urgent:
        spectrum(k)
    for i in (2, 3, 4, 5, 6):
        fetches[i].wait()
    live = iota((1, slots), 1) < counts[my_f, my_b, my_t]
    all_wt = weights[0, 0].astype(F32)
    own_wt = jnp.where(my_b == 0, all_wt[0:1, :], all_wt[1:2, :])
    own_wt = jnp.where(live, own_wt, 0.0)
    place = cells[...]
    packed = cat(
        [
            (place >> HALF_BITS).astype(F32), (place & ((1 << HALF_BITS) - 1)).astype(F32),
            observed[...].astype(F32), own_wt, own_wt,
        ],
        0,
    ).astype(BF)
    slot_out[...] = packed
    got_x[my_t] = packed

    pl.semaphore_wait(barrier, n)

    def copy_x(t):
        return pltpu.make_async_remote_copy(
            src_ref=slot_out,
            dst_ref=got_x.at[my_t],
            send_sem=send_x,
            recv_sem=recv_x.at[my_t],
            device_id={"facet": my_f, "team": t, "sub": my_b},
            device_id_type=MESH,
        )

    def copy1(k, t):
        return pltpu.make_async_remote_copy(
            src_ref=spec_out.at[k],
            dst_ref=got1.at[me],
            send_sem=send1,
            recv_sem=recv1,
            device_id={"facet": facet_at(k), "team": t, "sub": my_b},
            device_id_type=MESH,
        )

    def send_specs(ks, t):
        for k in ks:
            if k:
                copy1(k, t).start()
            else:
                pl.when(my_t != t)(lambda: copy1(0, t).start())

    def send_slots(t):
        pl.when(my_t != t)(lambda: copy_x(t).start())

    send_slots(0)
    send_specs(urgent, 0)
    for k in local_k:
        spectrum(k)
    send_specs(local_k, 0)
    got1[me] = spec_out[0]

    for i in (7, 8, 9):
        fetches[i].wait()
    shift_u = sub_off[0, my_f * nb + my_b]
    step = length // rall
    scale_g = 1.0 / math.sqrt(rall * nf)
    lane = iota((1, n * rdev), 1)
    col_a = jnp.zeros((1, n * rdev), jnp.int32)
    row = iota((n * rdev, 1), 0)
    row_cc = jnp.zeros((n * rdev, 1), jnp.int32)
    row2 = iota((nf * rdev, 1), 0)
    row_a = jnp.zeros((nf * rdev, 1), jnp.int32)
    for f in range(nf):
        col_a = jnp.where(lane // rall == f, fac_off[0, f], col_a)
        row_cc = jnp.where(row // rall == f, fac_off[1, f], row_cc)
        row_a = jnp.where(row2 // rdev == f, fac_off[0, f], row_a)
    p0 = iota((M, n * rdev), 0)
    gc, gs = sincos(p0 * col_a - (p0 + shift_u) * (lane % rall * step), length)
    gc = (gc * scale_g).astype(BF)
    gs = (gs * scale_g).astype(BF)
    a_mat = mm(kt[...], cat([cat([gc, gs], 1), cat([-gs, gc], 1)], 0)).astype(BF)
    p1 = iota((nf * rdev, M), 1)
    hc, hs = sincos(p1 * row_a - (p1 + shift_u) * ((row2 % rdev + my_t * rdev) * step), length)
    at = mm(cat([hc * scale_g, hs * scale_g], 1).astype(BF), kk[...])
    ah = cat([at[:, :size], -at[:, size:]], 1).astype(BF)
    ec, es = sincos(iota((n * rdev, M), 1) * row_cc, length)

    for t in range(1, nt):
        send_slots(t)
        send_specs(order, t)
    half = tiles // nb
    scale_b = 1.0 / (math.sqrt(M) * size)
    tile_no = iota((half, M), 0) + my_b * half
    for far in range(2):
        for a in range(nf):
            shift_v = sub_off[1, facet_at(a) * nb + (other if far else my_b)]
            if far:
                wt_far[a] = column_weights(shift_v)
            m_no = iota((half, M), 1)
            c, s = sincos((m_no + shift_v) * (tile_no * LANES) - m_no * fac_off[1, my_f], length)
            tw2[far, a, 0] = c * scale_b
            tw2[far, a, 1] = s * scale_b

    fine_no = iota((FINE, slots), 0)
    coarse = size // FINE
    coarse_no = iota((coarse, slots), 0) * FINE
    for k in range(nt):
        src = lax.rem(my_t + k, nt)
        if k:
            pltpu.make_async_copy(got_x.at[src], got_x.at[src], recv_x.at[src]).wait()
        pos = got_x[src].astype(F32)[0:4, :].astype(jnp.int32)
        pos = (pos[0:2, :] << HALF_BITS) + pos[2:4, :]
        for axis in range(2):
            lo_c, lo_s = sincos(fine_no * pos[axis : axis + 1, :], period)
            hi_c, hi_s = sincos(coarse_no * pos[axis : axis + 1, :], period)
            fine[0] = hi_c
            fine[1] = hi_s
            for q in range(coarse):
                c1 = fine[0, q : q + 1, :]
                s1 = fine[1, q : q + 1, :]
                c = c1 * lo_c - s1 * lo_s
                s = s1 * lo_c + c1 * lo_s
                rng = slice(q * FINE, (q + 1) * FINE)
                if axis == 0:
                    row_c[k, rng, :] = c
                    row_s[k, rng, :] = s
                else:
                    col_w[k, 0, rng, :] = c.astype(BF)
                    col_w[k, 1, rng, :] = (c - s).astype(BF)
                    col_w[k, 2, rng, :] = (c + s).astype(BF)
    amap = aterm[...].astype(F32)
    amap = cat([amap, amap], 1)

    done = got1.at[pl.ds(0, n - 1)]
    pltpu.make_async_copy(done, done, recv1).wait()
    sp = got1[...].astype(F32).reshape(n * rdev, 2 * M)
    sr = sp[:, :M]
    si = sp[:, M:]
    turned = cat([sr * ec - si * es, sr * es + si * ec], 1).astype(BF)
    t = mm(turned, kk[...]).astype(BF)
    tr = t[:, :size]
    ti = t[:, size:]
    image = mm(a_mat, cat([t, cat([-ti, tr], 1)], 0))
    image = amap * image
    image_re = image[:, :size]
    image_im = image[:, size:]
    w_both = (image_re + image_im).astype(BF)
    w_re = image_re.astype(BF)
    w_im = image_im.astype(BF)
    left = [[], [], []]
    for k in range(nt):
        src = lax.rem(my_t + k, nt)
        z_both = mm(w_both, col_w[k, 0])
        zr = z_both - mm(w_im, col_w[k, 1])
        zi = z_both - mm(w_re, col_w[k, 2])
        rc = row_c[k]
        rs = row_s[k]
        pred_re = jnp.sum(rc * zr + rs * zi, 0, keepdims=True) * (1.0 / size)
        pred_im = jnp.sum(rc * zi - rs * zr, 0, keepdims=True) * (1.0 / size)
        info = got_x[src].astype(F32)
        res_re = info[6:7, :] * (info[4:5, :] - pred_re)
        res_im = info[6:7, :] * (info[5:6, :] - pred_im)
        left_re = rc * res_re - rs * res_im
        left_im = rc * res_im + rs * res_re
        left[0].append((left_re + left_im).astype(BF))
        left[1].append(left_re.astype(BF))
        left[2].append(left_im.astype(BF))
    prod = [
        mm_nt(cat(left[c], 1), cat([col_w[k, c] for k in range(nt)], 1)) for c in range(3)
    ]
    grid = cat([prod[0] - prod[2], prod[0] - prod[1]], 1)
    v = (amap * grid).astype(BF)
    u = mm_nt(v, kk[...]).astype(BF)
    ur = u[:, :M]
    ui = u[:, M:]
    part = mm(ah, cat([u, cat([-ui, ur], 1)], 0))
    fold_out[...] = part.reshape(nf, rdev, 2 * M).astype(BF)


    def copy2(k, far):
        return pltpu.make_async_remote_copy(
            src_ref=fold_out.at[facet_at(k)],
            dst_ref=got2.at[far, my_f],
            send_sem=send2,
            recv_sem=recv2.at[min(k // nc, 1) + far],
            device_id={"facet": facet_at(k), "team": my_t, "sub": other if far else my_b},
            device_id_type=MESH,
        )

    for k in urgent:
        copy2(k, 1).start()
    for k in local_k:
        copy2(k, 1).start()
    for k in urgent + local_k:
        if k:
            copy2(k, 0).start()
    got2[0, my_f] = fold_out[my_f]

    def update(total, far, ks):
        for k in ks:
            g = got2[far, facet_at(k)].astype(F32)
            gr = g[:, :M]
            gi = g[:, M:]
            parts = []
            for j in range(half):
                c = tw2[far, k, 0, j : j + 1, :]
                s = tw2[far, k, 1, j : j + 1, :]
                parts.append(cat([gr * c - gi * s, gr * s + gi * c], 1))
            y = mm(cat(parts, 0).astype(BF), (wt_far if far else wt_near)[k])
            total = y if total is None else total + y
        return total

    def arrived(which, count):
        done = got1.at[pl.ds(0, count)]
        pltpu.make_async_copy(done, done, recv2.at[which]).wait()

    if nc > 1:
        arrived(0, nc - 1)
    total = update(None, 0, local_k)
    arrived(1, nf)
    total = update(total, 1, local_k)
    total = update(total, 0, urgent)
    if ny > 1:
        arrived(2, nf - nc)
    total = update(total, 1, urgent)
    for k in range(half):
        rng = slice(k * rdev, (k + 1) * rdev)
        lanes = slice(k * LANES, (k + 1) * LANES)
        out[0, 0, :, lanes] = total[rng, :LANES]
        out[0, 1, :, lanes] = total[rng, LANES:]
    sent = got1.at[pl.ds(0, nt - 1)]
    pltpu.make_async_copy(sent, sent, send_x).wait()
    sent = got1.at[pl.ds(0, n - 1)]
    pltpu.make_async_copy(sent, sent, send1).wait()
    sent = got1.at[pl.ds(0, 2 * nf - 1)]
    pltpu.make_async_copy(sent, sent, send2).wait()


def tables(size):
    angle = (np.arange(M)[:, None] * np.arange(size)[None, :] % size) * (TWO_PI / size)
    kc = np.cos(angle) / math.sqrt(M)
    ks = np.sin(angle) / math.sqrt(M)
    kk = np.block([[kc, ks], [-ks, kc]])
    kt = np.concatenate([kc.T, ks.T], 1)
    return [np.asarray(v, np.float32).astype(ml_dtypes.bfloat16) for v in (kk, kt)]


def local(facet_rows, sub_offsets, facet_offsets, aterm, cells, observed, weights, counts):
    nf = lax.axis_size("facet")
    nt = lax.axis_size("team")
    nb = lax.axis_size("sub")
    rdev, length = facet_rows.shape[2:]
    size = aterm.shape[-1]
    slots = cells.shape[-1]
    n = nf * nt
    tiles = length // LANES
    dims = (nf, nt, nb, length, size, rdev)
    consts = [jnp.asarray(v) for v in tables(size)]
    hbm = pl.BlockSpec(memory_space=pltpu.HBM)
    operands = [
        sub_offsets.T, facet_offsets.T, counts, facet_rows, aterm, cells, observed,
        weights.transpose(0, 2, 1, 3), *consts,
    ]
    dma = pltpu.SemaphoreType.DMA
    vmem = pltpu.VMEM
    return pl.pallas_call(
        functools.partial(body, dims),
        out_shape=pltpu.VMEM((1, 2, rdev, length // nb), F32),
        in_specs=[hbm] * 10,
        out_specs=pl.BlockSpec(memory_space=pltpu.VMEM),
        scratch_shapes=[
            *[pltpu.SMEM(v.shape, v.dtype) for v in operands[:3]],
            vmem(facet_rows.shape, BF),
            vmem((size, size), BF),
            vmem((2, slots), jnp.int32),
            vmem((2, slots), BF),
            *[vmem(v.shape, v.dtype) for v in operands[7:]],
            vmem((nf, rdev, 2 * M), BF),
            vmem((n, rdev, 2 * M), BF),
            vmem((8, slots), BF),
            vmem((nt, 8, slots), BF),
            vmem((nf, rdev, 2 * M), BF),
            vmem((nb, nf, rdev, 2 * M), BF),
            vmem((nf, 2, tiles, M), F32),
            vmem((nb, nf, 2, tiles // nb, M), F32),
            vmem((nf, 2 * M, 2 * LANES), BF),
            vmem((nf, 2 * M, 2 * LANES), BF),
            vmem((2, size // FINE, slots), F32),
            vmem((nt, 3, size, slots), BF),
            vmem((nt, size, slots), F32),
            vmem((nt, size, slots), F32),
            dma, dma, dma, dma((nt,)), dma, dma((3,)), dma((10,)),
        ],
        compiler_params=pltpu.CompilerParams(
            collective_id=0, has_side_effects=True
        ),
    )(*operands)


def solution(mesh):
    placed = (
        P("facet", None, "team", None),
        P(),
        P(),
        P("facet", None, None, None),
        P("facet", None, "team", None, None),
        P("facet", None, "team", None, None),
        P("facet", None, "team", None),
        P(),
    )
    return jax.shard_map(
        local,
        mesh=mesh,
        in_specs=placed,
        out_specs=P("facet", None, "team", "sub"),
        check_vma=False,
    )
```

```python
import functools
import math

import jax
import jax.numpy as jnp
import ml_dtypes
import numpy as np
from jax import lax
from jax.experimental import pallas as pl
from jax.experimental.pallas import tpu as pltpu
from jax.sharding import PartitionSpec as P

M = 128
LANES = 128
FINE = 16
HALF_BITS = 5
PIECES = 4
TWO_PI = 2.0 * math.pi
BF = jnp.bfloat16
F32 = jnp.float32
MESH = pl.DeviceIdType.MESH


def sincos(turns, period):
    shift = period.bit_length() - 3
    quad = (turns + (1 << (shift - 1))) >> shift
    t = (turns - (quad << shift)).astype(F32) * (TWO_PI / period)
    t2 = t * t
    s = t * (1.0 + t2 * (-1.0 / 6 + t2 * (1.0 / 120 + t2 * (-1.0 / 5040))))
    c = 1.0 + t2 * (-0.5 + t2 * (1.0 / 24 + t2 * (-1.0 / 720 + t2 * (1.0 / 40320))))
    odd = (quad & 1) != 0
    cos = jnp.where(odd, s, c)
    sin = jnp.where(odd, c, s)
    cos = jnp.where(((quad + 1) & 2) != 0, -cos, cos)
    sin = jnp.where((quad & 2) != 0, -sin, sin)
    return cos, sin


def mm(left, right):
    return jnp.dot(left, right, preferred_element_type=F32)


def mm_nt(left, right):
    return lax.dot_general(left, right, (((1,), (1,)), ((), ())), preferred_element_type=F32)


def cat(parts, axis):
    return jnp.concatenate(parts, axis)


def iota(shape, dim):
    return lax.broadcasted_iota(jnp.int32, shape, dim)


def body(dims, *refs):
    (sub_hbm, fac_hbm, cnt_hbm, rows_hbm, aterm_hbm, cells_hbm, obs_hbm, wt_hbm, kk_hbm, kt_hbm) = refs[:10]
    out = refs[10]
    (
        sub_off, fac_off, counts, rows, aterm, cells, observed, weights, kk, kt,
        spec_out, got1, slot_out, got_x, fold_out, got2,
        tw1, tw2, wt_near, wt_far, fine, col_w, row_c, row_s,
        send1, recv1, send_x, recv_x, send2, recv2, in_sem,
    ) = refs[11:]
    nf, nt, nb, length, size, rdev = dims
    rall = rdev * nt
    n = nf * nt
    slots = cells.shape[-1]
    period = 4 * size
    tiles = length // LANES
    my_f = lax.axis_index("facet")
    my_t = lax.axis_index("team")
    my_b = lax.axis_index("sub")
    me = my_f * nt + my_t
    other = 1 - my_b

    fetches = [
        pltpu.make_async_copy(sub_hbm, sub_off, in_sem.at[0]),
        pltpu.make_async_copy(rows_hbm, rows, in_sem.at[1]),
        pltpu.make_async_copy(fac_hbm, fac_off, in_sem.at[2]),
        pltpu.make_async_copy(cnt_hbm, counts, in_sem.at[3]),
        pltpu.make_async_copy(cells_hbm.at[0, my_b, 0], cells, in_sem.at[4]),
        pltpu.make_async_copy(obs_hbm.at[0, my_b, 0], observed, in_sem.at[5]),
        pltpu.make_async_copy(wt_hbm, weights, in_sem.at[6]),
        pltpu.make_async_copy(kt_hbm, kt, in_sem.at[0]),
        pltpu.make_async_copy(kk_hbm, kk, in_sem.at[1]),
        pltpu.make_async_copy(aterm_hbm.at[0, my_b], aterm, in_sem.at[7]),
    ]
    fetches[0].start()
    piece = length // PIECES
    for c in range(2):
        for q in range(PIECES):
            lanes = pl.ds(q * piece, piece)
            pltpu.make_async_copy(
                rows_hbm.at[0, c, :, lanes], rows.at[0, c, :, lanes], in_sem.at[1]
            ).start()
    for fetch in fetches[2:7]:
        fetch.start()

    barrier = pltpu.get_barrier_semaphore()
    nc = 2 - nf % 2
    ny = nf // nc
    order = [(k // nc + ny // 2) % ny * nc + k % nc for k in range(nf)]
    urgent = [k for k in order if k >= nc]
    local_k = [k for k in order if k < nc]

    def facet_at(k):
        row = lax.rem(my_f // nc + k // nc, ny)
        return row * nc + lax.rem(my_f + k % nc, nc)

    def greet(k, t, b):
        pl.semaphore_signal(
            barrier, inc=1, device_id={"facet": facet_at(k), "team": t, "sub": b}, device_id_type=MESH
        )

    for t in range(nt):
        for k in order:
            if k:
                greet(k, t, my_b)
            else:
                pl.when(my_t != t)(functools.partial(greet, k, t, my_b))
        if t == 0:
            greet(0, my_t, other)
    base_c, base_s = sincos(iota((M, LANES), 0) * iota((M, LANES), 1), length)
    lane_row = iota((1, LANES), 1)

    fetches[0].wait()
    fetches[1].wait()
    for fetch in fetches[7:]:
        fetch.start()

    def column_weights(shift_v):
        pc, ps = sincos(lane_row * shift_v, length)
        c = (base_c * pc - base_s * ps).astype(BF)
        s = (base_s * pc + base_c * ps).astype(BF)
        return cat([cat([c, s], 1), cat([-s, c], 1)], 0)

    scale = 1.0 / math.sqrt(length)
    x = [
        cat([rows[0, c, :, k * LANES : (k + 1) * LANES].astype(F32) for k in range(tiles)], 0)
        for c in range(2)
    ]
    x = cat(x, 1).astype(BF)

    def spectrum(k):
        shift_v = sub_off[1, facet_at(k) * nb + my_b]
        wt_near[k] = column_weights(shift_v)
        y = mm_nt(x, wt_near[k])
        c, s = sincos(iota((tiles, M), 0) * (iota((tiles, M), 1) + shift_v), tiles)
        tw1[k, 0] = c * scale
        tw1[k, 1] = s * scale
        acc = [None] * 4
        for j in range(tiles):
            yr = y[j * rdev : (j + 1) * rdev, :M]
            yi = y[j * rdev : (j + 1) * rdev, M:]
            c = tw1[k, 0, j : j + 1, :]
            s = tw1[k, 1, j : j + 1, :]
            q = 2 * (j % 2)
            add_re = yr * c + yi * s
            add_im = yi * c - yr * s
            acc[q] = add_re if acc[q] is None else acc[q] + add_re
            acc[q + 1] = add_im if acc[q + 1] is None else acc[q + 1] + add_im
        spec_out[k] = cat([acc[0] + acc[2], acc[1] + acc[3]], 1).astype(BF)

    for k in urgent:
        spectrum(k)
    for i in (2, 3, 4, 5, 6):
        fetches[i].wait()
    live = iota((1, slots), 1) < counts[my_f, my_b, my_t]
    all_wt = weights[0, 0].astype(F32)
    own_wt = jnp.where(my_b == 0, all_wt[0:1, :], all_wt[1:2, :])
    own_wt = jnp.where(live, own_wt, 0.0)
    place = cells[...]
    packed = cat(
        [
            (place >> HALF_BITS).astype(F32), (place & ((1 << HALF_BITS) - 1)).astype(F32),
            observed[...].astype(F32), own_wt, own_wt,
        ],
        0,
    ).astype(BF)
    slot_out[...] = packed
    got_x[my_t] = packed

    pl.semaphore_wait(barrier, n)

    def copy_x(t):
        return pltpu.make_async_remote_copy(
            src_ref=slot_out,
            dst_ref=got_x.at[my_t],
            send_sem=send_x,
            recv_sem=recv_x.at[my_t],
            device_id={"facet": my_f, "team": t, "sub": my_b},
            device_id_type=MESH,
        )

    def copy1(k, t):
        return pltpu.make_async_remote_copy(
            src_ref=spec_out.at[k],
            dst_ref=got1.at[me],
            send_sem=send1,
            recv_sem=recv1,
            device_id={"facet": facet_at(k), "team": t, "sub": my_b},
            device_id_type=MESH,
        )

    def send_specs(ks, t):
        for k in ks:
            if k:
                copy1(k, t).start()
            else:
                pl.when(my_t != t)(lambda: copy1(0, t).start())

    def send_slots(t):
        pl.when(my_t != t)(lambda: copy_x(t).start())

    send_slots(0)
    send_specs(urgent, 0)
    for k in local_k:
        spectrum(k)
    send_specs(local_k, 0)
    got1[me] = spec_out[0]

    for i in (7, 8, 9):
        fetches[i].wait()
    shift_u = sub_off[0, my_f * nb + my_b]
    step = length // rall
    scale_g = 1.0 / math.sqrt(rall * nf)
    lane = iota((1, n * rdev), 1)
    col_a = jnp.zeros((1, n * rdev), jnp.int32)
    row = iota((n * rdev, 1), 0)
    row_cc = jnp.zeros((n * rdev, 1), jnp.int32)
    row2 = iota((nf * rdev, 1), 0)
    row_a = jnp.zeros((nf * rdev, 1), jnp.int32)
    for f in range(nf):
        col_a = jnp.where(lane // rall == f, fac_off[0, f], col_a)
        row_cc = jnp.where(row // rall == f, fac_off[1, f], row_cc)
        row_a = jnp.where(row2 // rdev == f, fac_off[0, f], row_a)
    p0 = iota((M, n * rdev), 0)
    gc, gs = sincos(p0 * col_a - (p0 + shift_u) * (lane % rall * step), length)
    gc = (gc * scale_g).astype(BF)
    gs = (gs * scale_g).astype(BF)
    a_mat = mm(kt[...], cat([cat([gc, gs], 1), cat([-gs, gc], 1)], 0)).astype(BF)
    p1 = iota((nf * rdev, M), 1)
    hc, hs = sincos(p1 * row_a - (p1 + shift_u) * ((row2 % rdev + my_t * rdev) * step), length)
    at = mm(cat([hc * scale_g, hs * scale_g], 1).astype(BF), kk[...])
    ah = cat([at[:, :size], -at[:, size:]], 1).astype(BF)
    ec, es = sincos(iota((n * rdev, M), 1) * row_cc, length)

    for t in range(1, nt):
        send_slots(t)
        send_specs(order, t)
    half = tiles // nb
    scale_b = 1.0 / (math.sqrt(M) * size)
    tile_no = iota((half, M), 0) + my_b * half
    for far in range(2):
        for a in range(nf):
            shift_v = sub_off[1, facet_at(a) * nb + (other if far else my_b)]
            if far:
                wt_far[a] = column_weights(shift_v)
            m_no = iota((half, M), 1)
            c, s = sincos((m_no + shift_v) * (tile_no * LANES) - m_no * fac_off[1, my_f], length)
            tw2[far, a, 0] = c * scale_b
            tw2[far, a, 1] = s * scale_b

    fine_no = iota((FINE, slots), 0)
    coarse = size // FINE
    coarse_no = iota((coarse, slots), 0) * FINE
    for k in range(nt):
        src = lax.rem(my_t + k, nt)
        if k:
            pltpu.make_async_copy(got_x.at[src], got_x.at[src], recv_x.at[src]).wait()
        pos = got_x[src].astype(F32)[0:4, :].astype(jnp.int32)
        pos = (pos[0:2, :] << HALF_BITS) + pos[2:4, :]
        for axis in range(2):
            lo_c, lo_s = sincos(fine_no * pos[axis : axis + 1, :], period)
            hi_c, hi_s = sincos(coarse_no * pos[axis : axis + 1, :], period)
            fine[0] = hi_c
            fine[1] = hi_s
            for q in range(coarse):
                c1 = fine[0, q : q + 1, :]
                s1 = fine[1, q : q + 1, :]
                c = c1 * lo_c - s1 * lo_s
                s = s1 * lo_c + c1 * lo_s
                rng = slice(q * FINE, (q + 1) * FINE)
                if axis == 0:
                    row_c[k, rng, :] = c
                    row_s[k, rng, :] = s
                else:
                    col_w[k, 0, rng, :] = c.astype(BF)
                    col_w[k, 1, rng, :] = (c - s).astype(BF)
                    col_w[k, 2, rng, :] = (c + s).astype(BF)
    amap = aterm[...].astype(F32)
    amap = cat([amap, amap], 1)

    done = got1.at[pl.ds(0, n - 1)]
    pltpu.make_async_copy(done, done, recv1).wait()
    sp = got1[...].astype(F32).reshape(n * rdev, 2 * M)
    sr = sp[:, :M]
    si = sp[:, M:]
    turned = cat([sr * ec - si * es, sr * es + si * ec], 1).astype(BF)
    t = mm(turned, kk[...]).astype(BF)
    tr = t[:, :size]
    ti = t[:, size:]
    image = mm(a_mat, cat([t, cat([-ti, tr], 1)], 0))
    image = amap * image
    image_re = image[:, :size]
    image_im = image[:, size:]
    w_both = (image_re + image_im).astype(BF)
    w_re = image_re.astype(BF)
    w_im = image_im.astype(BF)
    def degrid(k):
        src = lax.rem(my_t + k, nt)
        z_both = mm(w_both, col_w[k, 0])
        zr = z_both - mm(w_im, col_w[k, 1])
        zi = z_both - mm(w_re, col_w[k, 2])
        rc = row_c[k]
        rs = row_s[k]
        pred_re = jnp.sum(rc * zr + rs * zi, 0, keepdims=True) * (1.0 / size)
        pred_im = jnp.sum(rc * zi - rs * zr, 0, keepdims=True) * (1.0 / size)
        info = got_x[src].astype(F32)
        res_re = info[6:7, :] * (info[4:5, :] - pred_re)
        res_im = info[6:7, :] * (info[5:6, :] - pred_im)
        rc = rc.astype(BF)
        rs = rs.astype(BF)
        res_re = jnp.broadcast_to(res_re.astype(BF), (size, slots))
        res_im = jnp.broadcast_to(res_im.astype(BF), (size, slots))
        left_re = rc * res_re - rs * res_im
        left_im = rc * res_im + rs * res_re
        return [left_re + left_im, left_re, left_im]

    left = [None] * nt
    prod = [None] * 3
    for k in range(nt + 1):
        if k < nt:
            left[k] = degrid(k)
        if k:
            for c in range(3):
                part = mm_nt(left[k - 1][c], col_w[k - 1, c])
                prod[c] = part if prod[c] is None else prod[c] + part
    grid = cat([prod[0] - prod[2], prod[0] - prod[1]], 1)
    v = (amap * grid).astype(BF)
    u = mm_nt(v, kk[...]).astype(BF)
    ur = u[:, :M]
    ui = u[:, M:]
    part = mm(ah, cat([u, cat([-ui, ur], 1)], 0))
    fold_out[...] = part.reshape(nf, rdev, 2 * M).astype(BF)


    def copy2(k, far):
        return pltpu.make_async_remote_copy(
            src_ref=fold_out.at[facet_at(k)],
            dst_ref=got2.at[far, my_f],
            send_sem=send2,
            recv_sem=recv2.at[min(k // nc, 1) + far],
            device_id={"facet": facet_at(k), "team": my_t, "sub": other if far else my_b},
            device_id_type=MESH,
        )

    for k in urgent:
        copy2(k, 1).start()
    for k in local_k:
        copy2(k, 1).start()
    for k in urgent + local_k:
        if k:
            copy2(k, 0).start()
    got2[0, my_f] = fold_out[my_f]

    def update(total, far, ks):
        for k in ks:
            g = got2[far, facet_at(k)].astype(F32)
            gr = g[:, :M]
            gi = g[:, M:]
            parts = []
            for j in range(half):
                c = tw2[far, k, 0, j : j + 1, :]
                s = tw2[far, k, 1, j : j + 1, :]
                parts.append(cat([gr * c - gi * s, gr * s + gi * c], 1))
            y = mm(cat(parts, 0).astype(BF), (wt_far if far else wt_near)[k])
            total = y if total is None else total + y
        return total

    def arrived(which, count):
        done = got1.at[pl.ds(0, count)]
        pltpu.make_async_copy(done, done, recv2.at[which]).wait()

    if nc > 1:
        arrived(0, nc - 1)
    total = update(None, 0, local_k)
    arrived(1, nf)
    total = update(total, 1, local_k)
    total = update(total, 0, urgent)
    if ny > 1:
        arrived(2, nf - nc)
    total = update(total, 1, urgent)
    for k in range(half):
        rng = slice(k * rdev, (k + 1) * rdev)
        lanes = slice(k * LANES, (k + 1) * LANES)
        out[0, 0, :, lanes] = total[rng, :LANES]
        out[0, 1, :, lanes] = total[rng, LANES:]
    sent = got1.at[pl.ds(0, nt - 1)]
    pltpu.make_async_copy(sent, sent, send_x).wait()
    sent = got1.at[pl.ds(0, n - 1)]
    pltpu.make_async_copy(sent, sent, send1).wait()
    sent = got1.at[pl.ds(0, 2 * nf - 1)]
    pltpu.make_async_copy(sent, sent, send2).wait()


def tables(size):
    angle = (np.arange(M)[:, None] * np.arange(size)[None, :] % size) * (TWO_PI / size)
    kc = np.cos(angle) / math.sqrt(M)
    ks = np.sin(angle) / math.sqrt(M)
    kk = np.block([[kc, ks], [-ks, kc]])
    kt = np.concatenate([kc.T, ks.T], 1)
    return [np.asarray(v, np.float32).astype(ml_dtypes.bfloat16) for v in (kk, kt)]


def local(facet_rows, sub_offsets, facet_offsets, aterm, cells, observed, weights, counts):
    nf = lax.axis_size("facet")
    nt = lax.axis_size("team")
    nb = lax.axis_size("sub")
    rdev, length = facet_rows.shape[2:]
    size = aterm.shape[-1]
    slots = cells.shape[-1]
    n = nf * nt
    tiles = length // LANES
    dims = (nf, nt, nb, length, size, rdev)
    consts = [jnp.asarray(v) for v in tables(size)]
    hbm = pl.BlockSpec(memory_space=pltpu.HBM)
    operands = [
        sub_offsets.T, facet_offsets.T, counts, facet_rows, aterm, cells, observed,
        weights.transpose(0, 2, 1, 3), *consts,
    ]
    dma = pltpu.SemaphoreType.DMA
    vmem = pltpu.VMEM
    return pl.pallas_call(
        functools.partial(body, dims),
        out_shape=pltpu.VMEM((1, 2, rdev, length // nb), F32),
        in_specs=[hbm] * 10,
        out_specs=pl.BlockSpec(memory_space=pltpu.VMEM),
        scratch_shapes=[
            *[pltpu.SMEM(v.shape, v.dtype) for v in operands[:3]],
            vmem(facet_rows.shape, BF),
            vmem((size, size), BF),
            vmem((2, slots), jnp.int32),
            vmem((2, slots), BF),
            *[vmem(v.shape, v.dtype) for v in operands[7:]],
            vmem((nf, rdev, 2 * M), BF),
            vmem((n, rdev, 2 * M), BF),
            vmem((8, slots), BF),
            vmem((nt, 8, slots), BF),
            vmem((nf, rdev, 2 * M), BF),
            vmem((nb, nf, rdev, 2 * M), BF),
            vmem((nf, 2, tiles, M), F32),
            vmem((nb, nf, 2, tiles // nb, M), F32),
            vmem((nf, 2 * M, 2 * LANES), BF),
            vmem((nf, 2 * M, 2 * LANES), BF),
            vmem((2, size // FINE, slots), F32),
            vmem((nt, 3, size, slots), BF),
            vmem((nt, size, slots), F32),
            vmem((nt, size, slots), F32),
            dma, dma, dma, dma((nt,)), dma, dma((3,)), dma((8,)),
        ],
        compiler_params=pltpu.CompilerParams(
            collective_id=0, has_side_effects=True
        ),
    )(*operands)


def solution(mesh):
    placed = (
        P("facet", None, "team", None),
        P(),
        P(),
        P("facet", None, None, None),
        P("facet", None, "team", None, None),
        P("facet", None, "team", None, None),
        P("facet", None, "team", None),
        P(),
    )
    return jax.shard_map(
        local,
        mesh=mesh,
        in_specs=placed,
        out_specs=P("facet", None, "team", "sub"),
        check_vma=False,
    )
```

```python
import functools
import math

import jax
import jax.numpy as jnp
import ml_dtypes
import numpy as np
from jax import lax
from jax.experimental import pallas as pl
from jax.experimental.pallas import tpu as pltpu
from jax.sharding import PartitionSpec as P

M = 128
LANES = 128
FINE = 16
HALF_BITS = 5
PIECES = 4
TWO_PI = 2.0 * math.pi
BF = jnp.bfloat16
F32 = jnp.float32
MESH = pl.DeviceIdType.MESH


def sincos(turns, period):
    shift = period.bit_length() - 3
    quad = (turns + (1 << (shift - 1))) >> shift
    t = (turns - (quad << shift)).astype(F32) * (TWO_PI / period)
    t2 = t * t
    s = t * (1.0 + t2 * (-1.0 / 6 + t2 * (1.0 / 120 + t2 * (-1.0 / 5040))))
    c = 1.0 + t2 * (-0.5 + t2 * (1.0 / 24 + t2 * (-1.0 / 720 + t2 * (1.0 / 40320))))
    odd = (quad & 1) != 0
    cos = jnp.where(odd, s, c)
    sin = jnp.where(odd, c, s)
    cos = jnp.where(((quad + 1) & 2) != 0, -cos, cos)
    sin = jnp.where((quad & 2) != 0, -sin, sin)
    return cos, sin


def mm(left, right):
    return jnp.dot(left, right, preferred_element_type=F32)


def mm_nt(left, right):
    return lax.dot_general(left, right, (((1,), (1,)), ((), ())), preferred_element_type=F32)


def cat(parts, axis):
    return jnp.concatenate(parts, axis)


def iota(shape, dim):
    return lax.broadcasted_iota(jnp.int32, shape, dim)


def body(dims, *refs):
    (sub_hbm, fac_hbm, cnt_hbm, rows_hbm, aterm_hbm, cells_hbm, obs_hbm, wt_hbm, kk_hbm, kt_hbm) = refs[:10]
    out = refs[10]
    (
        sub_off, fac_off, counts, rows, aterm, cells, observed, weights, kk, kt,
        spec_out, got1, slot_out, got_x, fold_out, got2,
        tw1, tw2, wt_near, wt_far, fine, col_w, row_c, row_s,
        send1, recv1, send_x, recv_x, send2, recv2, in_sem, ready,
    ) = refs[11:]
    nf, nt, nb, length, size, rdev = dims
    rall = rdev * nt
    n = nf * nt
    slots = cells.shape[-1]
    period = 4 * size
    tiles = length // LANES
    my_f = lax.axis_index("facet")
    my_t = lax.axis_index("team")
    my_b = lax.axis_index("sub")
    me = my_f * nt + my_t
    other = 1 - my_b

    fetches = [
        pltpu.make_async_copy(sub_hbm, sub_off, in_sem.at[0]),
        pltpu.make_async_copy(rows_hbm, rows, in_sem.at[1]),
        pltpu.make_async_copy(fac_hbm, fac_off, in_sem.at[2]),
        pltpu.make_async_copy(cnt_hbm, counts, in_sem.at[3]),
        pltpu.make_async_copy(cells_hbm.at[0, my_b, 0], cells, in_sem.at[4]),
        pltpu.make_async_copy(obs_hbm.at[0, my_b, 0], observed, in_sem.at[5]),
        pltpu.make_async_copy(wt_hbm, weights, in_sem.at[6]),
        pltpu.make_async_copy(kt_hbm, kt, in_sem.at[0]),
        pltpu.make_async_copy(kk_hbm, kk, in_sem.at[1]),
        pltpu.make_async_copy(aterm_hbm.at[0, my_b], aterm, in_sem.at[7]),
    ]
    fetches[0].start()
    piece = length // PIECES
    for c in range(2):
        for q in range(PIECES):
            lanes = pl.ds(q * piece, piece)
            pltpu.make_async_copy(
                rows_hbm.at[0, c, :, lanes], rows.at[0, c, :, lanes], in_sem.at[1]
            ).start()
    for fetch in fetches[2:7]:
        fetch.start()

    barrier = pltpu.get_barrier_semaphore()
    nc = 2 - nf % 2
    ny = nf // nc
    order = [(k // nc + ny // 2) % ny * nc + k % nc for k in range(nf)]
    urgent = [k for k in order if k >= nc]
    local_k = [k for k in order if k < nc]

    def facet_at(k):
        row = lax.rem(my_f // nc + k // nc, ny)
        return row * nc + lax.rem(my_f + k % nc, nc)

    def greet(k, t, b):
        pl.semaphore_signal(
            barrier, inc=1, device_id={"facet": facet_at(k), "team": t, "sub": b}, device_id_type=MESH
        )

    def greet_team(t):
        for k in order:
            greet(k, t, my_b)

    for t in reversed(range(1, nt)):
        pl.when(my_t < t)(functools.partial(greet_team, t))
    greet(0, my_t, other)
    for k in order:
        if k:
            greet(k, my_t, my_b)

    base_c, base_s = sincos(iota((M, LANES), 0) * iota((M, LANES), 1), length)
    lane_row = iota((1, LANES), 1)

    fetches[0].wait()
    fetches[1].wait()
    for fetch in fetches[7:]:
        fetch.start()

    def column_weights(shift_v):
        pc, ps = sincos(lane_row * shift_v, length)
        c = (base_c * pc - base_s * ps).astype(BF)
        s = (base_s * pc + base_c * ps).astype(BF)
        return cat([cat([c, s], 1), cat([-s, c], 1)], 0)

    scale = 1.0 / math.sqrt(length)
    x = [
        cat([rows[0, c, :, k * LANES : (k + 1) * LANES].astype(F32) for k in range(tiles)], 0)
        for c in range(2)
    ]
    x = cat(x, 1).astype(BF)

    def spectrum(k):
        shift_v = sub_off[1, facet_at(k) * nb + my_b]
        wt_near[k] = column_weights(shift_v)
        y = mm_nt(x, wt_near[k])
        c, s = sincos(iota((tiles, M), 0) * (iota((tiles, M), 1) + shift_v), tiles)
        tw1[k, 0] = c * scale
        tw1[k, 1] = s * scale
        acc = [None] * 4
        for j in range(tiles):
            yr = y[j * rdev : (j + 1) * rdev, :M]
            yi = y[j * rdev : (j + 1) * rdev, M:]
            c = tw1[k, 0, j : j + 1, :]
            s = tw1[k, 1, j : j + 1, :]
            q = 2 * (j % 2)
            add_re = yr * c + yi * s
            add_im = yi * c - yr * s
            acc[q] = add_re if acc[q] is None else acc[q] + add_re
            acc[q + 1] = add_im if acc[q + 1] is None else acc[q + 1] + add_im
        spec_out[k] = cat([acc[0] + acc[2], acc[1] + acc[3]], 1).astype(BF)

    for k in urgent:
        spectrum(k)
    for i in (2, 3, 4, 5, 6):
        fetches[i].wait()
    live = iota((1, slots), 1) < counts[my_f, my_b, my_t]
    all_wt = weights[0, 0].astype(F32)
    own_wt = jnp.where(my_b == 0, all_wt[0:1, :], all_wt[1:2, :])
    own_wt = jnp.where(live, own_wt, 0.0)
    place = cells[...]
    packed = cat(
        [
            (place >> HALF_BITS).astype(F32), (place & ((1 << HALF_BITS) - 1)).astype(F32),
            observed[...].astype(F32), own_wt, own_wt,
        ],
        0,
    ).astype(BF)
    slot_out[...] = packed
    got_x[my_t] = packed

    pl.semaphore_wait(barrier, nf * (my_t + 1))

    def report(t):
        for k in order:
            pl.semaphore_signal(
                ready.at[my_t], inc=1,
                device_id={"facet": facet_at(k), "team": t, "sub": my_b}, device_id_type=MESH,
            )


    def copy_x(t):
        return pltpu.make_async_remote_copy(
            src_ref=slot_out,
            dst_ref=got_x.at[my_t],
            send_sem=send_x,
            recv_sem=recv_x.at[my_t],
            device_id={"facet": my_f, "team": t, "sub": my_b},
            device_id_type=MESH,
        )

    def copy1(k, t):
        return pltpu.make_async_remote_copy(
            src_ref=spec_out.at[k],
            dst_ref=got1.at[me],
            send_sem=send1,
            recv_sem=recv1,
            device_id={"facet": facet_at(k), "team": t, "sub": my_b},
            device_id_type=MESH,
        )

    def send_specs(ks, t):
        for k in ks:
            if k:
                copy1(k, t).start()
            else:
                pl.when(my_t != t)(lambda: copy1(0, t).start())

    def send_slots(t):
        pl.when(my_t != t)(lambda: copy_x(t).start())

    send_slots(0)
    send_specs(urgent, 0)
    for t in range(nt - 1):
        pl.when(my_t > t)(functools.partial(report, t))
    for k in local_k:
        spectrum(k)
    send_specs(local_k, 0)
    got1[me] = spec_out[0]

    for i in (7, 8, 9):
        fetches[i].wait()
    shift_u = sub_off[0, my_f * nb + my_b]
    step = length // rall
    scale_g = 1.0 / math.sqrt(rall * nf)
    lane = iota((1, n * rdev), 1)
    col_a = jnp.zeros((1, n * rdev), jnp.int32)
    row = iota((n * rdev, 1), 0)
    row_cc = jnp.zeros((n * rdev, 1), jnp.int32)
    row2 = iota((nf * rdev, 1), 0)
    row_a = jnp.zeros((nf * rdev, 1), jnp.int32)
    for f in range(nf):
        col_a = jnp.where(lane // rall == f, fac_off[0, f], col_a)
        row_cc = jnp.where(row // rall == f, fac_off[1, f], row_cc)
        row_a = jnp.where(row2 // rdev == f, fac_off[0, f], row_a)
    p0 = iota((M, n * rdev), 0)
    gc, gs = sincos(p0 * col_a - (p0 + shift_u) * (lane % rall * step), length)
    gc = (gc * scale_g).astype(BF)
    gs = (gs * scale_g).astype(BF)
    a_mat = mm(kt[...], cat([cat([gc, gs], 1), cat([-gs, gc], 1)], 0)).astype(BF)
    p1 = iota((nf * rdev, M), 1)
    hc, hs = sincos(p1 * row_a - (p1 + shift_u) * ((row2 % rdev + my_t * rdev) * step), length)
    at = mm(cat([hc * scale_g, hs * scale_g], 1).astype(BF), kk[...])
    ah = cat([at[:, :size], -at[:, size:]], 1).astype(BF)
    ec, es = sincos(iota((n * rdev, M), 1) * row_cc, length)

    for t in range(1, nt):
        pl.when(my_t < t)(lambda: pl.semaphore_wait(ready.at[t], nf))
        send_slots(t)
        send_specs(order, t)
    half = tiles // nb
    scale_b = 1.0 / (math.sqrt(M) * size)
    tile_no = iota((half, M), 0) + my_b * half
    for far in range(2):
        for a in range(nf):
            shift_v = sub_off[1, facet_at(a) * nb + (other if far else my_b)]
            if far:
                wt_far[a] = column_weights(shift_v)
            m_no = iota((half, M), 1)
            c, s = sincos((m_no + shift_v) * (tile_no * LANES) - m_no * fac_off[1, my_f], length)
            tw2[far, a, 0] = c * scale_b
            tw2[far, a, 1] = s * scale_b

    fine_no = iota((FINE, slots), 0)
    coarse = size // FINE
    coarse_no = iota((coarse, slots), 0) * FINE
    for k in range(nt):
        src = lax.rem(my_t + k, nt)
        if k:
            pltpu.make_async_copy(got_x.at[src], got_x.at[src], recv_x.at[src]).wait()
        pos = got_x[src].astype(F32)[0:4, :].astype(jnp.int32)
        pos = (pos[0:2, :] << HALF_BITS) + pos[2:4, :]
        for axis in range(2):
            lo_c, lo_s = sincos(fine_no * pos[axis : axis + 1, :], period)
            hi_c, hi_s = sincos(coarse_no * pos[axis : axis + 1, :], period)
            fine[0] = hi_c
            fine[1] = hi_s
            for q in range(coarse):
                c1 = fine[0, q : q + 1, :]
                s1 = fine[1, q : q + 1, :]
                c = c1 * lo_c - s1 * lo_s
                s = s1 * lo_c + c1 * lo_s
                rng = slice(q * FINE, (q + 1) * FINE)
                if axis == 0:
                    row_c[k, rng, :] = c
                    row_s[k, rng, :] = s
                else:
                    col_w[k, 0, rng, :] = c.astype(BF)
                    col_w[k, 1, rng, :] = (c - s).astype(BF)
                    col_w[k, 2, rng, :] = (c + s).astype(BF)
    amap = aterm[...].astype(F32)
    amap = cat([amap, amap], 1)

    done = got1.at[pl.ds(0, n - 1)]
    pltpu.make_async_copy(done, done, recv1).wait()
    sp = got1[...].astype(F32).reshape(n * rdev, 2 * M)
    sr = sp[:, :M]
    si = sp[:, M:]
    turned = cat([sr * ec - si * es, sr * es + si * ec], 1).astype(BF)
    t = mm(turned, kk[...]).astype(BF)
    tr = t[:, :size]
    ti = t[:, size:]
    image = mm(a_mat, cat([t, cat([-ti, tr], 1)], 0))
    image = amap * image
    image_re = image[:, :size]
    image_im = image[:, size:]
    w_both = (image_re + image_im).astype(BF)
    w_re = image_re.astype(BF)
    w_im = image_im.astype(BF)
    def degrid(k):
        src = lax.rem(my_t + k, nt)
        z_both = mm(w_both, col_w[k, 0])
        zr = z_both - mm(w_im, col_w[k, 1])
        zi = z_both - mm(w_re, col_w[k, 2])
        rc = row_c[k]
        rs = row_s[k]
        pred_re = jnp.sum(rc * zr + rs * zi, 0, keepdims=True) * (1.0 / size)
        pred_im = jnp.sum(rc * zi - rs * zr, 0, keepdims=True) * (1.0 / size)
        info = got_x[src].astype(F32)
        res_re = info[6:7, :] * (info[4:5, :] - pred_re)
        res_im = info[6:7, :] * (info[5:6, :] - pred_im)
        rc = rc.astype(BF)
        rs = rs.astype(BF)
        res_re = jnp.broadcast_to(res_re.astype(BF), (size, slots))
        res_im = jnp.broadcast_to(res_im.astype(BF), (size, slots))
        left_re = rc * res_re - rs * res_im
        left_im = rc * res_im + rs * res_re
        return [left_re + left_im, left_re, left_im]

    left = [None] * nt
    prod = [None] * 3
    for k in range(nt + 1):
        if k < nt:
            left[k] = degrid(k)
        if k:
            for c in range(3):
                part = mm_nt(left[k - 1][c], col_w[k - 1, c])
                prod[c] = part if prod[c] is None else prod[c] + part
    grid = cat([prod[0] - prod[2], prod[0] - prod[1]], 1)
    v = (amap * grid).astype(BF)
    u = mm_nt(v, kk[...]).astype(BF)
    ur = u[:, :M]
    ui = u[:, M:]
    part = mm(ah, cat([u, cat([-ui, ur], 1)], 0))
    fold_out[...] = part.reshape(nf, rdev, 2 * M).astype(BF)


    def copy2(k, far):
        return pltpu.make_async_remote_copy(
            src_ref=fold_out.at[facet_at(k)],
            dst_ref=got2.at[far, my_f],
            send_sem=send2,
            recv_sem=recv2.at[min(k // nc, 1) + far],
            device_id={"facet": facet_at(k), "team": my_t, "sub": other if far else my_b},
            device_id_type=MESH,
        )

    for k in urgent:
        copy2(k, 1).start()
    for k in local_k:
        copy2(k, 1).start()
    for k in urgent + local_k:
        if k:
            copy2(k, 0).start()
    got2[0, my_f] = fold_out[my_f]

    def update(total, far, ks):
        for k in ks:
            g = got2[far, facet_at(k)].astype(F32)
            gr = g[:, :M]
            gi = g[:, M:]
            parts = []
            for j in range(half):
                c = tw2[far, k, 0, j : j + 1, :]
                s = tw2[far, k, 1, j : j + 1, :]
                parts.append(cat([gr * c - gi * s, gr * s + gi * c], 1))
            y = mm(cat(parts, 0).astype(BF), (wt_far if far else wt_near)[k])
            total = y if total is None else total + y
        return total

    def arrived(which, count):
        done = got1.at[pl.ds(0, count)]
        pltpu.make_async_copy(done, done, recv2.at[which]).wait()

    if nc > 1:
        arrived(0, nc - 1)
    total = update(None, 0, local_k)
    arrived(1, nf)
    total = update(total, 1, local_k)
    total = update(total, 0, urgent)
    if ny > 1:
        arrived(2, nf - nc)
    total = update(total, 1, urgent)
    for k in range(half):
        rng = slice(k * rdev, (k + 1) * rdev)
        lanes = slice(k * LANES, (k + 1) * LANES)
        out[0, 0, :, lanes] = total[rng, :LANES]
        out[0, 1, :, lanes] = total[rng, LANES:]
    sent = got1.at[pl.ds(0, nt - 1)]
    pltpu.make_async_copy(sent, sent, send_x).wait()
    sent = got1.at[pl.ds(0, n - 1)]
    pltpu.make_async_copy(sent, sent, send1).wait()
    sent = got1.at[pl.ds(0, 2 * nf - 1)]
    pltpu.make_async_copy(sent, sent, send2).wait()


def tables(size):
    angle = (np.arange(M)[:, None] * np.arange(size)[None, :] % size) * (TWO_PI / size)
    kc = np.cos(angle) / math.sqrt(M)
    ks = np.sin(angle) / math.sqrt(M)
    kk = np.block([[kc, ks], [-ks, kc]])
    kt = np.concatenate([kc.T, ks.T], 1)
    return [np.asarray(v, np.float32).astype(ml_dtypes.bfloat16) for v in (kk, kt)]


def local(facet_rows, sub_offsets, facet_offsets, aterm, cells, observed, weights, counts):
    nf = lax.axis_size("facet")
    nt = lax.axis_size("team")
    nb = lax.axis_size("sub")
    rdev, length = facet_rows.shape[2:]
    size = aterm.shape[-1]
    slots = cells.shape[-1]
    n = nf * nt
    tiles = length // LANES
    dims = (nf, nt, nb, length, size, rdev)
    consts = [jnp.asarray(v) for v in tables(size)]
    hbm = pl.BlockSpec(memory_space=pltpu.HBM)
    operands = [
        sub_offsets.T, facet_offsets.T, counts, facet_rows, aterm, cells, observed,
        weights.transpose(0, 2, 1, 3), *consts,
    ]
    dma = pltpu.SemaphoreType.DMA
    vmem = pltpu.VMEM
    return pl.pallas_call(
        functools.partial(body, dims),
        out_shape=pltpu.VMEM((1, 2, rdev, length // nb), F32),
        in_specs=[hbm] * 10,
        out_specs=pl.BlockSpec(memory_space=pltpu.VMEM),
        scratch_shapes=[
            *[pltpu.SMEM(v.shape, v.dtype) for v in operands[:3]],
            vmem(facet_rows.shape, BF),
            vmem((size, size), BF),
            vmem((2, slots), jnp.int32),
            vmem((2, slots), BF),
            *[vmem(v.shape, v.dtype) for v in operands[7:]],
            vmem((nf, rdev, 2 * M), BF),
            vmem((n, rdev, 2 * M), BF),
            vmem((8, slots), BF),
            vmem((nt, 8, slots), BF),
            vmem((nf, rdev, 2 * M), BF),
            vmem((nb, nf, rdev, 2 * M), BF),
            vmem((nf, 2, tiles, M), F32),
            vmem((nb, nf, 2, tiles // nb, M), F32),
            vmem((nf, 2 * M, 2 * LANES), BF),
            vmem((nf, 2 * M, 2 * LANES), BF),
            vmem((2, size // FINE, slots), F32),
            vmem((nt, 3, size, slots), BF),
            vmem((nt, size, slots), F32),
            vmem((nt, size, slots), F32),
            dma, dma, dma, dma((nt,)), dma, dma((3,)), dma((8,)), pltpu.SemaphoreType.REGULAR((nt,)),
        ],
        compiler_params=pltpu.CompilerParams(
            collective_id=0, has_side_effects=True
        ),
    )(*operands)


def solution(mesh):
    placed = (
        P("facet", None, "team", None),
        P(),
        P(),
        P("facet", None, None, None),
        P("facet", None, "team", None, None),
        P("facet", None, "team", None, None),
        P("facet", None, "team", None),
        P(),
    )
    return jax.shard_map(
        local,
        mesh=mesh,
        in_specs=placed,
        out_specs=P("facet", None, "team", "sub"),
        check_vma=False,
    )
```

```python
import functools
import math

import jax
import jax.numpy as jnp
import ml_dtypes
import numpy as np
from jax import lax
from jax.experimental import pallas as pl
from jax.experimental.pallas import tpu as pltpu
from jax.sharding import PartitionSpec as P

M = 128
LANES = 128
FINE = 16
HALF_BITS = 5
PIECES = 4
TWO_PI = 2.0 * math.pi
BF = jnp.bfloat16
F32 = jnp.float32
MESH = pl.DeviceIdType.MESH


def sincos(turns, period):
    shift = period.bit_length() - 3
    quad = (turns + (1 << (shift - 1))) >> shift
    t = (turns - (quad << shift)).astype(F32) * (TWO_PI / period)
    t2 = t * t
    s = t * (1.0 + t2 * (-1.0 / 6 + t2 * (1.0 / 120 + t2 * (-1.0 / 5040))))
    c = 1.0 + t2 * (-0.5 + t2 * (1.0 / 24 + t2 * (-1.0 / 720 + t2 * (1.0 / 40320))))
    odd = (quad & 1) != 0
    cos = jnp.where(odd, s, c)
    sin = jnp.where(odd, c, s)
    cos = jnp.where(((quad + 1) & 2) != 0, -cos, cos)
    sin = jnp.where((quad & 2) != 0, -sin, sin)
    return cos, sin


def mm(left, right):
    return jnp.dot(left, right, preferred_element_type=F32)


def mm_nt(left, right):
    return lax.dot_general(left, right, (((1,), (1,)), ((), ())), preferred_element_type=F32)


def cat(parts, axis):
    return jnp.concatenate(parts, axis)


def iota(shape, dim):
    return lax.broadcasted_iota(jnp.int32, shape, dim)


def body(dims, *refs):
    (sub_hbm, fac_hbm, cnt_hbm, rows_hbm, aterm_hbm, cells_hbm, obs_hbm, wt_hbm, kk_hbm, kt_hbm) = refs[:10]
    out = refs[10]
    (
        sub_off, fac_off, counts, rows, aterm, cells, observed, weights, kk, kt,
        spec_out, got1, slot_out, got_x, fold_out, got2,
        tw1, tw2, wt_near, wt_far, coarse, col_w, row_c, row_s,
        send1, recv1, send_x, recv_x, send2, recv2, in_sem, ready,
    ) = refs[11:]
    nf, nt, nb, length, size, rdev = dims
    rall = rdev * nt
    n = nf * nt
    slots = cells.shape[-1]
    period = 4 * size
    tiles = length // LANES
    my_f = lax.axis_index("facet")
    my_t = lax.axis_index("team")
    my_b = lax.axis_index("sub")
    me = my_f * nt + my_t
    other = 1 - my_b

    fetches = [
        pltpu.make_async_copy(sub_hbm, sub_off, in_sem.at[0]),
        pltpu.make_async_copy(rows_hbm, rows, in_sem.at[1]),
        pltpu.make_async_copy(fac_hbm, fac_off, in_sem.at[2]),
        pltpu.make_async_copy(cnt_hbm, counts, in_sem.at[3]),
        pltpu.make_async_copy(cells_hbm.at[0, my_b, 0], cells, in_sem.at[4]),
        pltpu.make_async_copy(obs_hbm.at[0, my_b, 0], observed, in_sem.at[5]),
        pltpu.make_async_copy(wt_hbm, weights, in_sem.at[6]),
        pltpu.make_async_copy(kt_hbm, kt, in_sem.at[0]),
        pltpu.make_async_copy(kk_hbm, kk, in_sem.at[1]),
        pltpu.make_async_copy(aterm_hbm.at[0, my_b], aterm, in_sem.at[7]),
    ]
    fetches[0].start()
    piece = length // PIECES
    for c in range(2):
        for q in range(PIECES):
            lanes = pl.ds(q * piece, piece)
            pltpu.make_async_copy(
                rows_hbm.at[0, c, :, lanes], rows.at[0, c, :, lanes], in_sem.at[1]
            ).start()
    for fetch in fetches[2:7]:
        fetch.start()

    barrier = pltpu.get_barrier_semaphore()
    nc = 2 - nf % 2
    ny = nf // nc
    order = [(k // nc + ny // 2) % ny * nc + k % nc for k in range(nf)]
    urgent = [k for k in order if k >= nc]
    local_k = [k for k in order if k < nc]

    def facet_at(k):
        row = lax.rem(my_f // nc + k // nc, ny)
        return row * nc + lax.rem(my_f + k % nc, nc)

    def greet(k, t, b):
        pl.semaphore_signal(
            barrier, inc=1, device_id={"facet": facet_at(k), "team": t, "sub": b}, device_id_type=MESH
        )

    def greet_team(t):
        for k in order:
            greet(k, t, my_b)

    for t in reversed(range(1, nt)):
        pl.when(my_t < t)(functools.partial(greet_team, t))
    greet(0, my_t, other)
    for k in order:
        if k:
            greet(k, my_t, my_b)

    base_c, base_s = sincos(iota((M, LANES), 0) * iota((M, LANES), 1), length)
    lane_row = iota((1, LANES), 1)

    fetches[0].wait()
    fetches[1].wait()
    for fetch in fetches[7:]:
        fetch.start()

    def column_weights(shift_v):
        pc, ps = sincos(lane_row * shift_v, length)
        c = (base_c * pc - base_s * ps).astype(BF)
        s = (base_s * pc + base_c * ps).astype(BF)
        return cat([cat([c, s], 1), cat([-s, c], 1)], 0)

    scale = 1.0 / math.sqrt(length)
    x = [
        cat([rows[0, c, :, k * LANES : (k + 1) * LANES].astype(F32) for k in range(tiles)], 0)
        for c in range(2)
    ]
    x = cat(x, 1).astype(BF)

    def spectrum(k):
        shift_v = sub_off[1, facet_at(k) * nb + my_b]
        wt_near[k] = column_weights(shift_v)
        y = mm_nt(x, wt_near[k])
        c, s = sincos(iota((tiles, M), 0) * (iota((tiles, M), 1) + shift_v), tiles)
        tw1[k, 0] = c * scale
        tw1[k, 1] = s * scale
        acc = [None] * 4
        for j in range(tiles):
            yr = y[j * rdev : (j + 1) * rdev, :M]
            yi = y[j * rdev : (j + 1) * rdev, M:]
            c = tw1[k, 0, j : j + 1, :]
            s = tw1[k, 1, j : j + 1, :]
            q = 2 * (j % 2)
            add_re = yr * c + yi * s
            add_im = yi * c - yr * s
            acc[q] = add_re if acc[q] is None else acc[q] + add_re
            acc[q + 1] = add_im if acc[q + 1] is None else acc[q + 1] + add_im
        spec_out[k] = cat([acc[0] + acc[2], acc[1] + acc[3]], 1).astype(BF)

    for k in urgent:
        spectrum(k)
    for i in (2, 3, 4, 5, 6):
        fetches[i].wait()
    live = iota((1, slots), 1) < counts[my_f, my_b, my_t]
    all_wt = weights[0, 0].astype(F32)
    own_wt = jnp.where(my_b == 0, all_wt[0:1, :], all_wt[1:2, :])
    own_wt = jnp.where(live, own_wt, 0.0)
    place = cells[...]
    packed = cat(
        [
            (place >> HALF_BITS).astype(F32), (place & ((1 << HALF_BITS) - 1)).astype(F32),
            observed[...].astype(F32), own_wt, own_wt,
        ],
        0,
    ).astype(BF)
    slot_out[...] = packed
    got_x[my_t] = packed

    pl.semaphore_wait(barrier, nf * (my_t + 1))

    def report(t):
        for k in order:
            pl.semaphore_signal(
                ready.at[my_t], inc=1,
                device_id={"facet": facet_at(k), "team": t, "sub": my_b}, device_id_type=MESH,
            )


    def copy_x(t):
        return pltpu.make_async_remote_copy(
            src_ref=slot_out,
            dst_ref=got_x.at[my_t],
            send_sem=send_x,
            recv_sem=recv_x.at[my_t],
            device_id={"facet": my_f, "team": t, "sub": my_b},
            device_id_type=MESH,
        )

    def copy1(k, t):
        return pltpu.make_async_remote_copy(
            src_ref=spec_out.at[k],
            dst_ref=got1.at[me],
            send_sem=send1,
            recv_sem=recv1,
            device_id={"facet": facet_at(k), "team": t, "sub": my_b},
            device_id_type=MESH,
        )

    def send_specs(ks, t):
        for k in ks:
            if k:
                copy1(k, t).start()
            else:
                pl.when(my_t != t)(lambda: copy1(0, t).start())

    def send_slots(t):
        pl.when(my_t != t)(lambda: copy_x(t).start())

    send_slots(0)
    send_specs(urgent, 0)
    for t in range(nt - 1):
        pl.when(my_t > t)(functools.partial(report, t))
    for k in local_k:
        spectrum(k)
    send_specs(local_k, 0)
    got1[me] = spec_out[0]

    for i in (7, 8, 9):
        fetches[i].wait()
    mirror = size // 2
    shift_u = sub_off[0, my_f * nb + my_b]
    step = length // rall
    scale_g = 1.0 / math.sqrt(rall * nf)
    lane = iota((1, n * rdev), 1)
    col_a = jnp.zeros((1, n * rdev), jnp.int32)
    row = iota((n * rdev, 1), 0)
    row_cc = jnp.zeros((n * rdev, 1), jnp.int32)
    row2 = iota((nf * rdev, 1), 0)
    row_a = jnp.zeros((nf * rdev, 1), jnp.int32)
    for f in range(nf):
        col_a = jnp.where(lane // rall == f, fac_off[0, f], col_a)
        row_cc = jnp.where(row // rall == f, fac_off[1, f], row_cc)
        row_a = jnp.where(row2 // rdev == f, fac_off[0, f], row_a)
    p0 = iota((M, n * rdev), 0)
    gc, gs = sincos(p0 * col_a - (p0 + shift_u) * (lane % rall * step), length)
    gc = (gc * scale_g).astype(BF)
    gs = (gs * scale_g).astype(BF)
    a_mat = mm(kt[...], cat([cat([gc, gs], 1), cat([-gs, gc], 1)], 0)).astype(BF)
    p1 = iota((nf * rdev, M), 1)
    hc, hs = sincos(p1 * row_a - (p1 + shift_u) * ((row2 % rdev + my_t * rdev) * step), length)
    hc = (hc * scale_g).astype(BF)
    hs = (hs * scale_g).astype(BF)
    at = mm_nt(cat([cat([hc, -hs], 1), cat([hs, hc], 1)], 0), kt[...])
    ah = cat([at[: nf * rdev], -at[nf * rdev :]], 1).astype(BF)
    ec, es = sincos(iota((n * rdev, M), 1) * row_cc, length)

    for t in range(1, nt):
        pl.when(my_t < t)(lambda: pl.semaphore_wait(ready.at[t], nf))
        send_slots(t)
        send_specs(order, t)
    flip = (iota((mirror, mirror), 0) + iota((mirror, mirror), 1) == mirror - 1).astype(F32).astype(BF)
    left_half = mm(aterm[:, :mirror], flip)
    amap = cat([aterm[:, mirror:].astype(F32), left_half], 1)
    amap = cat([amap, amap], 1)
    half = tiles // nb
    scale_b = 1.0 / (math.sqrt(M) * size)
    tile_no = iota((half, M), 0) + my_b * half
    for far in range(2):
        for a in range(nf):
            shift_v = sub_off[1, facet_at(a) * nb + (other if far else my_b)]
            if far:
                wt_far[a] = column_weights(shift_v)
            m_no = iota((half, M), 1)
            c, s = sincos((m_no + shift_v) * (tile_no * LANES) - m_no * fac_off[1, my_f], length)
            tw2[far, a, 0] = c * scale_b
            tw2[far, a, 1] = s * scale_b

    fine_no = iota((FINE, slots), 0)
    row_no = iota((size // FINE, slots), 0)
    col_no = iota((mirror // FINE, slots), 0)
    for k in range(nt):
        src = lax.rem(my_t + k, nt)
        if k:
            pltpu.make_async_copy(got_x.at[src], got_x.at[src], recv_x.at[src]).wait()
        pos = got_x[src].astype(F32)[0:4, :].astype(jnp.int32)
        pos = (pos[0:2, :] << HALF_BITS) + pos[2:4, :]
        pos_x = pos[0:1, :]
        pos_y = pos[1:2, :]
        lo_c, lo_s = sincos(2 * fine_no * pos_x, 2 * period)
        hi_c, hi_s = sincos(2 * FINE * row_no * pos_x + (size - 1) * pos_y, 2 * period)
        coarse[0] = hi_c
        coarse[1] = hi_s
        for q in range(size // FINE):
            c1 = coarse[0, q : q + 1, :]
            s1 = coarse[1, q : q + 1, :]
            rng = slice(q * FINE, (q + 1) * FINE)
            row_c[k, rng, :] = c1 * lo_c - s1 * lo_s
            row_s[k, rng, :] = s1 * lo_c + c1 * lo_s
        lo_c, lo_s = sincos((2 * fine_no + 1) * pos_y, 2 * period)
        hi_c, hi_s = sincos(2 * FINE * col_no * pos_y, 2 * period)
        coarse[0, : mirror // FINE, :] = hi_c
        coarse[1, : mirror // FINE, :] = hi_s
        for q in range(mirror // FINE):
            c1 = coarse[0, q : q + 1, :]
            s1 = coarse[1, q : q + 1, :]
            rng = slice(q * FINE, (q + 1) * FINE)
            col_w[k, rng, :] = (c1 * lo_c - s1 * lo_s).astype(BF)
            rng = slice(mirror + q * FINE, mirror + (q + 1) * FINE)
            col_w[k, rng, :] = (s1 * lo_c + c1 * lo_s).astype(BF)

    done = got1.at[pl.ds(0, n - 1)]
    pltpu.make_async_copy(done, done, recv1).wait()
    sp = got1[...].astype(F32).reshape(n * rdev, 2 * M)
    sr = sp[:, :M]
    si = sp[:, M:]
    turn_re = (sr * ec - si * es).astype(BF)
    turn_im = (sr * es + si * ec).astype(BF)
    full = mm(a_mat, cat([cat([turn_re, turn_im], 1), cat([-turn_im, turn_re], 1)], 0))
    image = mm(full.astype(BF), kk[...])
    image = amap * image
    re_p, re_n, im_p, im_n = (image[:, c * mirror : (c + 1) * mirror] for c in range(4))
    folded = cat(
        [cat([re_p + re_n, im_p - im_n], 1), cat([im_p + im_n, re_n - re_p], 1)], 0
    ).astype(BF)
    def degrid(k):
        src = lax.rem(my_t + k, nt)
        z = mm(folded, col_w[k])
        zr = z[:size]
        zi = z[size:]
        rc = row_c[k]
        rs = row_s[k]
        pred_re = jnp.sum(rc * zr + rs * zi, 0, keepdims=True) * (1.0 / size)
        pred_im = jnp.sum(rc * zi - rs * zr, 0, keepdims=True) * (1.0 / size)
        info = got_x[src].astype(F32)
        res_re = info[6:7, :] * (info[4:5, :] - pred_re)
        res_im = info[6:7, :] * (info[5:6, :] - pred_im)
        rc = rc.astype(BF)
        rs = rs.astype(BF)
        res_re = jnp.broadcast_to(res_re.astype(BF), (size, slots))
        res_im = jnp.broadcast_to(res_im.astype(BF), (size, slots))
        left_re = rc * res_re - rs * res_im
        left_im = rc * res_im + rs * res_re
        return cat([left_re, left_im], 0)

    left = [None] * nt
    prod = None
    for k in range(nt + 1):
        if k < nt:
            left[k] = degrid(k)
        if k:
            part = mm_nt(left[k - 1], col_w[k - 1])
            prod = part if prod is None else prod + part
    cr, sr = prod[:size, :mirror], prod[:size, mirror:]
    ci, si = prod[size:, :mirror], prod[size:, mirror:]
    grid = cat([cr - si, cr + si, ci + sr, ci - sr], 1)
    v = (amap * grid).astype(BF)
    u = mm_nt(v, kk[...]).astype(BF)
    ur = u[:, :M]
    ui = u[:, M:]
    part = mm(ah, cat([u, cat([-ui, ur], 1)], 0))
    fold_out[...] = part.reshape(nf, rdev, 2 * M).astype(BF)


    def copy2(k, far):
        return pltpu.make_async_remote_copy(
            src_ref=fold_out.at[facet_at(k)],
            dst_ref=got2.at[far, my_f],
            send_sem=send2,
            recv_sem=recv2.at[min(k // nc, 1) + far],
            device_id={"facet": facet_at(k), "team": my_t, "sub": other if far else my_b},
            device_id_type=MESH,
        )

    for k in urgent:
        copy2(k, 1).start()
    for k in local_k:
        copy2(k, 1).start()
    for k in urgent + local_k:
        if k:
            copy2(k, 0).start()
    got2[0, my_f] = fold_out[my_f]

    def update(total, far, ks):
        for k in ks:
            g = got2[far, facet_at(k)].astype(F32)
            gr = g[:, :M]
            gi = g[:, M:]
            parts = []
            for j in range(half):
                c = tw2[far, k, 0, j : j + 1, :]
                s = tw2[far, k, 1, j : j + 1, :]
                parts.append(cat([gr * c - gi * s, gr * s + gi * c], 1))
            y = mm(cat(parts, 0).astype(BF), (wt_far if far else wt_near)[k])
            total = y if total is None else total + y
        return total

    def arrived(which, count):
        done = got1.at[pl.ds(0, count)]
        pltpu.make_async_copy(done, done, recv2.at[which]).wait()

    if nc > 1:
        arrived(0, nc - 1)
    total = update(None, 0, local_k)
    arrived(1, nf)
    total = update(total, 1, local_k)
    total = update(total, 0, urgent)
    if ny > 1:
        arrived(2, nf - nc)
    total = update(total, 1, urgent)
    for k in range(half):
        rng = slice(k * rdev, (k + 1) * rdev)
        lanes = slice(k * LANES, (k + 1) * LANES)
        out[0, 0, :, lanes] = total[rng, :LANES]
        out[0, 1, :, lanes] = total[rng, LANES:]
    sent = got1.at[pl.ds(0, nt - 1)]
    pltpu.make_async_copy(sent, sent, send_x).wait()
    sent = got1.at[pl.ds(0, n - 1)]
    pltpu.make_async_copy(sent, sent, send1).wait()
    sent = got1.at[pl.ds(0, 2 * nf - 1)]
    pltpu.make_async_copy(sent, sent, send2).wait()


def tables(size):
    angle = (np.arange(M)[:, None] * np.arange(size)[None, :] % size) * (TWO_PI / size)
    kc = np.cos(angle) / math.sqrt(M)
    ks = np.sin(angle) / math.sqrt(M)
    kt = np.concatenate([kc.T, ks.T], 1)
    half = size // 2
    order = np.concatenate([np.arange(half, size), np.arange(half - 1, -1, -1)])
    kc, ks = kc[:, order], ks[:, order]
    kk = np.block([[kc, ks], [-ks, kc]])
    return [np.asarray(v, np.float32).astype(ml_dtypes.bfloat16) for v in (kk, kt)]


def local(facet_rows, sub_offsets, facet_offsets, aterm, cells, observed, weights, counts):
    nf = lax.axis_size("facet")
    nt = lax.axis_size("team")
    nb = lax.axis_size("sub")
    rdev, length = facet_rows.shape[2:]
    size = aterm.shape[-1]
    slots = cells.shape[-1]
    n = nf * nt
    tiles = length // LANES
    dims = (nf, nt, nb, length, size, rdev)
    consts = [jnp.asarray(v) for v in tables(size)]
    hbm = pl.BlockSpec(memory_space=pltpu.HBM)
    operands = [
        sub_offsets.T, facet_offsets.T, counts, facet_rows, aterm, cells, observed,
        weights.transpose(0, 2, 1, 3), *consts,
    ]
    dma = pltpu.SemaphoreType.DMA
    vmem = pltpu.VMEM
    return pl.pallas_call(
        functools.partial(body, dims),
        out_shape=pltpu.VMEM((1, 2, rdev, length // nb), F32),
        in_specs=[hbm] * 10,
        out_specs=pl.BlockSpec(memory_space=pltpu.VMEM),
        scratch_shapes=[
            *[pltpu.SMEM(v.shape, v.dtype) for v in operands[:3]],
            vmem(facet_rows.shape, BF),
            vmem((size, size), BF),
            vmem((2, slots), jnp.int32),
            vmem((2, slots), BF),
            *[vmem(v.shape, v.dtype) for v in operands[7:]],
            vmem((nf, rdev, 2 * M), BF),
            vmem((n, rdev, 2 * M), BF),
            vmem((8, slots), BF),
            vmem((nt, 8, slots), BF),
            vmem((nf, rdev, 2 * M), BF),
            vmem((nb, nf, rdev, 2 * M), BF),
            vmem((nf, 2, tiles, M), F32),
            vmem((nb, nf, 2, tiles // nb, M), F32),
            vmem((nf, 2 * M, 2 * LANES), BF),
            vmem((nf, 2 * M, 2 * LANES), BF),
            vmem((2, size // FINE, slots), F32),
            vmem((nt, size, slots), BF),
            vmem((nt, size, slots), F32),
            vmem((nt, size, slots), F32),
            dma, dma, dma, dma((nt,)), dma, dma((3,)), dma((8,)), pltpu.SemaphoreType.REGULAR((nt,)),
        ],
        compiler_params=pltpu.CompilerParams(
            collective_id=0, has_side_effects=True
        ),
    )(*operands)


def solution(mesh):
    placed = (
        P("facet", None, "team", None),
        P(),
        P(),
        P("facet", None, None, None),
        P("facet", None, "team", None, None),
        P("facet", None, "team", None, None),
        P("facet", None, "team", None),
        P(),
    )
    return jax.shard_map(
        local,
        mesh=mesh,
        in_specs=placed,
        out_specs=P("facet", None, "team", "sub"),
        check_vma=False,
    )
```

```python
import functools
import math

import jax
import jax.numpy as jnp
import ml_dtypes
import numpy as np
from jax import lax
from jax.experimental import pallas as pl
from jax.experimental.pallas import tpu as pltpu
from jax.sharding import PartitionSpec as P

M = 128
LANES = 128
FINE = 16
HALF_BITS = 5
PIECES = 4
TWO_PI = 2.0 * math.pi
BF = jnp.bfloat16
F32 = jnp.float32
MESH = pl.DeviceIdType.MESH


def sincos(turns, period):
    shift = period.bit_length() - 3
    quad = (turns + (1 << (shift - 1))) >> shift
    t = (turns - (quad << shift)).astype(F32) * (TWO_PI / period)
    t2 = t * t
    s = t * (1.0 + t2 * (-1.0 / 6 + t2 * (1.0 / 120 + t2 * (-1.0 / 5040))))
    c = 1.0 + t2 * (-0.5 + t2 * (1.0 / 24 + t2 * (-1.0 / 720 + t2 * (1.0 / 40320))))
    odd = (quad & 1) != 0
    cos = jnp.where(odd, s, c)
    sin = jnp.where(odd, c, s)
    cos = jnp.where(((quad + 1) & 2) != 0, -cos, cos)
    sin = jnp.where((quad & 2) != 0, -sin, sin)
    return cos, sin


def mm(left, right):
    return jnp.dot(left, right, preferred_element_type=F32)


def mm_nt(left, right):
    return lax.dot_general(left, right, (((1,), (1,)), ((), ())), preferred_element_type=F32)


def cat(parts, axis):
    return jnp.concatenate(parts, axis)


def iota(shape, dim):
    return lax.broadcasted_iota(jnp.int32, shape, dim)


def body(dims, *refs):
    (sub_hbm, fac_hbm, cnt_hbm, rows_hbm, aterm_hbm, cells_hbm, obs_hbm, wt_hbm, kk_hbm, kt_hbm) = refs[:10]
    out = refs[10]
    (
        sub_off, fac_off, counts, rows, aterm, cells, observed, weights, kk, kt,
        spec_out, got1, slot_out, got_x, fold_out, got2,
        tw1, tw2, wt_near, wt_far, coarse, col_w, row_w, row_c, row_s,
        send1, recv1, send_x, recv_x, send2, recv2, in_sem, ready,
    ) = refs[11:]
    nf, nt, nb, length, size, rdev = dims
    rall = rdev * nt
    n = nf * nt
    slots = cells.shape[-1]
    period = 4 * size
    tiles = length // LANES
    my_f = lax.axis_index("facet")
    my_t = lax.axis_index("team")
    my_b = lax.axis_index("sub")
    me = my_f * nt + my_t
    other = 1 - my_b

    fetches = [
        pltpu.make_async_copy(sub_hbm, sub_off, in_sem.at[0]),
        pltpu.make_async_copy(rows_hbm, rows, in_sem.at[1]),
        pltpu.make_async_copy(fac_hbm, fac_off, in_sem.at[2]),
        pltpu.make_async_copy(cnt_hbm, counts, in_sem.at[2]),
        pltpu.make_async_copy(cells_hbm.at[0, my_b, 0], cells, in_sem.at[2]),
        pltpu.make_async_copy(obs_hbm.at[0, my_b, 0], observed, in_sem.at[2]),
        pltpu.make_async_copy(wt_hbm, weights, in_sem.at[2]),
        pltpu.make_async_copy(kt_hbm, kt, in_sem.at[0]),
        pltpu.make_async_copy(kk_hbm, kk, in_sem.at[1]),
        pltpu.make_async_copy(aterm_hbm.at[0, my_b], aterm, in_sem.at[3]),
    ]
    fetches[0].start()
    piece = length // PIECES
    for c in range(2):
        for q in range(PIECES):
            lanes = pl.ds(q * piece, piece)
            pltpu.make_async_copy(
                rows_hbm.at[0, c, :, lanes], rows.at[0, c, :, lanes], in_sem.at[1]
            ).start()
    for fetch in fetches[2:7]:
        fetch.start()

    barrier = pltpu.get_barrier_semaphore()
    nc = 2 - nf % 2
    ny = nf // nc
    order = [(k // nc + ny // 2) % ny * nc + k % nc for k in range(nf)]
    urgent = [k for k in order if k >= nc]
    local_k = [k for k in order if k < nc]

    def facet_at(k):
        row = lax.rem(my_f // nc + k // nc, ny)
        return row * nc + lax.rem(my_f + k % nc, nc)

    def greet(k, t, b):
        pl.semaphore_signal(
            barrier, inc=1, device_id={"facet": facet_at(k), "team": t, "sub": b}, device_id_type=MESH
        )

    def greet_team(t):
        for k in order:
            greet(k, t, my_b)

    for t in reversed(range(1, nt)):
        pl.when(my_t < t)(functools.partial(greet_team, t))
    greet(0, my_t, other)
    for k in order:
        if k:
            greet(k, my_t, my_b)

    base_c, base_s = sincos(iota((M, LANES), 0) * iota((M, LANES), 1), length)
    lane_row = iota((1, LANES), 1)

    fetches[0].wait()
    fetches[1].wait()
    for fetch in fetches[7:]:
        fetch.start()

    def column_weights(shift_v):
        pc, ps = sincos(lane_row * shift_v, length)
        c = (base_c * pc - base_s * ps).astype(BF)
        s = (base_s * pc + base_c * ps).astype(BF)
        return cat([cat([c, s], 1), cat([-s, c], 1)], 0)

    scale = 1.0 / math.sqrt(length)
    x = [
        cat([rows[0, c, :, k * LANES : (k + 1) * LANES].astype(F32) for k in range(tiles)], 0)
        for c in range(2)
    ]
    x = cat(x, 1).astype(BF)

    def spectrum(k):
        shift_v = sub_off[1, facet_at(k) * nb + my_b]
        wt_near[k] = column_weights(shift_v)
        y = mm_nt(x, wt_near[k])
        c, s = sincos(iota((tiles, M), 0) * (iota((tiles, M), 1) + shift_v), tiles)
        tw1[k, 0] = c * scale
        tw1[k, 1] = s * scale
        acc = [None] * 4
        for j in range(tiles):
            yr = y[j * rdev : (j + 1) * rdev, :M]
            yi = y[j * rdev : (j + 1) * rdev, M:]
            c = tw1[k, 0, j : j + 1, :]
            s = tw1[k, 1, j : j + 1, :]
            q = 2 * (j % 2)
            add_re = yr * c + yi * s
            add_im = yi * c - yr * s
            acc[q] = add_re if acc[q] is None else acc[q] + add_re
            acc[q + 1] = add_im if acc[q + 1] is None else acc[q + 1] + add_im
        spec_out[k] = cat([acc[0] + acc[2], acc[1] + acc[3]], 1).astype(BF)

    for k in urgent:
        spectrum(k)
    for i in (2, 3, 4, 5, 6):
        fetches[i].wait()
    live = iota((1, slots), 1) < counts[my_f, my_b, my_t]
    all_wt = weights[0, 0].astype(F32)
    own_wt = jnp.where(my_b == 0, all_wt[0:1, :], all_wt[1:2, :])
    own_wt = jnp.where(live, own_wt, 0.0)
    place = cells[...]
    packed = cat(
        [
            (place >> HALF_BITS).astype(F32), (place & ((1 << HALF_BITS) - 1)).astype(F32),
            observed[...].astype(F32), own_wt, own_wt,
        ],
        0,
    ).astype(BF)
    slot_out[...] = packed
    got_x[my_t] = packed

    pl.semaphore_wait(barrier, nf * (my_t + 1))

    def report(t):
        for k in order:
            pl.semaphore_signal(
                ready.at[my_t - 1], inc=1,
                device_id={"facet": facet_at(k), "team": t, "sub": my_b}, device_id_type=MESH,
            )


    def copy_x(t):
        return pltpu.make_async_remote_copy(
            src_ref=slot_out,
            dst_ref=got_x.at[my_t],
            send_sem=send_x,
            recv_sem=recv_x.at[my_t],
            device_id={"facet": my_f, "team": t, "sub": my_b},
            device_id_type=MESH,
        )

    def copy1(k, t):
        return pltpu.make_async_remote_copy(
            src_ref=spec_out.at[k],
            dst_ref=got1.at[me],
            send_sem=send1,
            recv_sem=recv1,
            device_id={"facet": facet_at(k), "team": t, "sub": my_b},
            device_id_type=MESH,
        )

    def send_specs(ks, t):
        for k in ks:
            if k:
                copy1(k, t).start()
            else:
                pl.when(my_t != t)(lambda: copy1(0, t).start())

    def send_slots(t):
        pl.when(my_t != t)(lambda: copy_x(t).start())

    send_specs(urgent, 0)
    send_slots(0)
    for t in range(nt - 1):
        pl.when(my_t > t)(functools.partial(report, t))
    for k in local_k:
        spectrum(k)
    send_specs(local_k, 0)
    got1[me] = spec_out[0]

    for i in (7, 8, 9):
        fetches[i].wait()
    mirror = size // 2
    shift_u = sub_off[0, my_f * nb + my_b]
    step = length // rall
    scale_g = 1.0 / math.sqrt(rall * nf)
    lane = iota((1, n * rdev), 1)
    col_a = jnp.zeros((1, n * rdev), jnp.int32)
    row = iota((n * rdev, 1), 0)
    row_cc = jnp.zeros((n * rdev, 1), jnp.int32)
    row2 = iota((nf * rdev, 1), 0)
    row_a = jnp.zeros((nf * rdev, 1), jnp.int32)
    for f in range(nf):
        col_a = jnp.where(lane // rall == f, fac_off[0, f], col_a)
        row_cc = jnp.where(row // rall == f, fac_off[1, f], row_cc)
        row_a = jnp.where(row2 // rdev == f, fac_off[0, f], row_a)
    p0 = iota((M, n * rdev), 0)
    gc, gs = sincos(p0 * col_a - (p0 + shift_u) * (lane % rall * step), length)
    gc = (gc * scale_g).astype(BF)
    gs = (gs * scale_g).astype(BF)
    a_mat = mm(kt[...], cat([cat([gc, gs], 1), cat([-gs, gc], 1)], 0)).astype(BF)
    p1 = iota((nf * rdev, M), 1)
    hc, hs = sincos(p1 * row_a - (p1 + shift_u) * ((row2 % rdev + my_t * rdev) * step), length)
    hc = (hc * scale_g).astype(BF)
    hs = (hs * scale_g).astype(BF)
    at = mm_nt(cat([cat([hc, -hs], 1), cat([hs, hc], 1)], 0), kt[...])
    ah = cat([at[: nf * rdev], -at[nf * rdev :]], 1).astype(BF)
    ec, es = sincos(iota((n * rdev, M), 1) * row_cc, length)

    for t in range(1, nt):
        pl.when(my_t < t)(lambda: pl.semaphore_wait(ready.at[t - 1], nf))
        send_slots(t)
        send_specs(order, t)
    flip = (iota((mirror, mirror), 0) + iota((mirror, mirror), 1) == mirror - 1).astype(F32).astype(BF)
    left_half = mm(aterm[:, :mirror], flip)
    amap = cat([aterm[:, mirror:].astype(F32), left_half], 1)
    amap = cat([amap, amap], 1)
    half = tiles // nb
    scale_b = 1.0 / (math.sqrt(M) * size)
    tile_no = iota((half, M), 0) + my_b * half
    for far in range(2):
        for a in range(nf):
            shift_v = sub_off[1, facet_at(a) * nb + (other if far else my_b)]
            if far:
                wt_far[a] = column_weights(shift_v)
            m_no = iota((half, M), 1)
            c, s = sincos((m_no + shift_v) * (tile_no * LANES) - m_no * fac_off[1, my_f], length)
            tw2[far, a, 0] = c * scale_b
            tw2[far, a, 1] = s * scale_b

    fine_no = iota((FINE, slots), 0)
    row_no = iota((size // FINE, slots), 0)
    col_no = iota((mirror // FINE, slots), 0)
    for k in range(nt):
        src = lax.rem(my_t + k, nt)
        if k:
            pltpu.make_async_copy(got_x.at[src], got_x.at[src], recv_x.at[src]).wait()
        pos = got_x[src].astype(F32)[0:4, :].astype(jnp.int32)
        pos = (pos[0:2, :] << HALF_BITS) + pos[2:4, :]
        pos_x = pos[0:1, :]
        pos_y = pos[1:2, :]
        lo_c, lo_s = sincos(2 * fine_no * pos_x, 2 * period)
        hi_c, hi_s = sincos(2 * FINE * row_no * pos_x + (size - 1) * pos_y, 2 * period)
        coarse[0] = hi_c
        coarse[1] = hi_s
        for q in range(size // FINE):
            c1 = coarse[0, q : q + 1, :]
            s1 = coarse[1, q : q + 1, :]
            rng = slice(q * FINE, (q + 1) * FINE)
            c = c1 * lo_c - s1 * lo_s
            s = s1 * lo_c + c1 * lo_s
            row_c[k, rng, :] = c
            row_s[k, rng, :] = s
            row_w[k, 0, rng, :] = c.astype(BF)
            row_w[k, 1, rng, :] = s.astype(BF)
        lo_c, lo_s = sincos((2 * fine_no + 1) * pos_y, 2 * period)
        hi_c, hi_s = sincos(2 * FINE * col_no * pos_y, 2 * period)
        coarse[0, : mirror // FINE, :] = hi_c
        coarse[1, : mirror // FINE, :] = hi_s
        for q in range(mirror // FINE):
            c1 = coarse[0, q : q + 1, :]
            s1 = coarse[1, q : q + 1, :]
            rng = slice(q * FINE, (q + 1) * FINE)
            col_w[k, rng, :] = (c1 * lo_c - s1 * lo_s).astype(BF)
            rng = slice(mirror + q * FINE, mirror + (q + 1) * FINE)
            col_w[k, rng, :] = (s1 * lo_c + c1 * lo_s).astype(BF)

    done = got1.at[pl.ds(0, n - 1)]
    pltpu.make_async_copy(done, done, recv1).wait()
    sp = got1[...].astype(F32).reshape(n * rdev, 2 * M)
    sr = sp[:, :M]
    si = sp[:, M:]
    turn_re = (sr * ec - si * es).astype(BF)
    turn_im = (sr * es + si * ec).astype(BF)
    full = mm(a_mat, cat([cat([turn_re, turn_im], 1), cat([-turn_im, turn_re], 1)], 0))
    image = mm(full.astype(BF), kk[...])
    image = amap * image
    re_p, re_n, im_p, im_n = (image[:, c * mirror : (c + 1) * mirror] for c in range(4))
    folded = cat(
        [cat([re_p + re_n, im_p - im_n], 1), cat([im_p + im_n, re_n - re_p], 1)], 0
    ).astype(BF)
    def degrid(k):
        src = lax.rem(my_t + k, nt)
        z = mm(folded, col_w[k])
        zr = z[:size]
        zi = z[size:]
        rc = row_c[k]
        rs = row_s[k]
        pred_re = jnp.sum(rc * zr + rs * zi, 0, keepdims=True) * (1.0 / size)
        pred_im = jnp.sum(rc * zi - rs * zr, 0, keepdims=True) * (1.0 / size)
        info = got_x[src].astype(F32)
        res_re = info[6:7, :] * (info[4:5, :] - pred_re)
        res_im = info[6:7, :] * (info[5:6, :] - pred_im)
        rc = row_w[k, 0]
        rs = row_w[k, 1]
        res_re = jnp.broadcast_to(res_re.astype(BF), (size, slots))
        res_im = jnp.broadcast_to(res_im.astype(BF), (size, slots))
        left_re = rc * res_re - rs * res_im
        left_im = rc * res_im + rs * res_re
        return cat([left_re, left_im], 0)

    left = [None] * nt
    prod = None
    for k in range(nt + 1):
        if k < nt:
            left[k] = degrid(k)
        if k:
            part = mm_nt(left[k - 1], col_w[k - 1])
            prod = part if prod is None else prod + part
    cr, sr = prod[:size, :mirror], prod[:size, mirror:]
    ci, si = prod[size:, :mirror], prod[size:, mirror:]
    grid = cat([cr - si, cr + si, ci + sr, ci - sr], 1)
    v = (amap * grid).astype(BF)
    u = mm_nt(v, kk[...]).astype(BF)
    ur = u[:, :M]
    ui = u[:, M:]
    part = mm(ah, cat([u, cat([-ui, ur], 1)], 0))
    fold_out[...] = part.reshape(nf, rdev, 2 * M).astype(BF)


    def copy2(k, far):
        return pltpu.make_async_remote_copy(
            src_ref=fold_out.at[facet_at(k)],
            dst_ref=got2.at[far, my_f],
            send_sem=send2,
            recv_sem=recv2.at[min(k // nc, 1) + far],
            device_id={"facet": facet_at(k), "team": my_t, "sub": other if far else my_b},
            device_id_type=MESH,
        )

    for k in urgent:
        copy2(k, 1).start()
    for k in local_k:
        copy2(k, 1).start()
    for k in urgent + local_k:
        if k:
            copy2(k, 0).start()
    got2[0, my_f] = fold_out[my_f]

    def update(total, far, ks):
        for k in ks:
            g = got2[far, facet_at(k)].astype(F32)
            gr = g[:, :M]
            gi = g[:, M:]
            parts = []
            for j in range(half):
                c = tw2[far, k, 0, j : j + 1, :]
                s = tw2[far, k, 1, j : j + 1, :]
                parts.append(cat([gr * c - gi * s, gr * s + gi * c], 1))
            y = mm(cat(parts, 0).astype(BF), (wt_far if far else wt_near)[k])
            total = y if total is None else total + y
        return total

    def arrived(which, count):
        done = got1.at[pl.ds(0, count)]
        pltpu.make_async_copy(done, done, recv2.at[which]).wait()

    if nc > 1:
        arrived(0, nc - 1)
    total = update(None, 0, local_k)
    arrived(1, nf)
    total = update(total, 1, local_k)
    total = update(total, 0, urgent)
    if ny > 1:
        arrived(2, nf - nc)
    total = update(total, 1, urgent)
    for k in range(half):
        rng = slice(k * rdev, (k + 1) * rdev)
        lanes = slice(k * LANES, (k + 1) * LANES)
        out[0, 0, :, lanes] = total[rng, :LANES]
        out[0, 1, :, lanes] = total[rng, LANES:]
    sent = got1.at[pl.ds(0, nt - 1)]
    pltpu.make_async_copy(sent, sent, send_x).wait()
    sent = got1.at[pl.ds(0, n - 1)]
    pltpu.make_async_copy(sent, sent, send1).wait()
    sent = got1.at[pl.ds(0, 2 * nf - 1)]
    pltpu.make_async_copy(sent, sent, send2).wait()


def tables(size):
    angle = (np.arange(M)[:, None] * np.arange(size)[None, :] % size) * (TWO_PI / size)
    kc = np.cos(angle) / math.sqrt(M)
    ks = np.sin(angle) / math.sqrt(M)
    kt = np.concatenate([kc.T, ks.T], 1)
    half = size // 2
    order = np.concatenate([np.arange(half, size), np.arange(half - 1, -1, -1)])
    kc, ks = kc[:, order], ks[:, order]
    kk = np.block([[kc, ks], [-ks, kc]])
    return [np.asarray(v, np.float32).astype(ml_dtypes.bfloat16) for v in (kk, kt)]


def local(facet_rows, sub_offsets, facet_offsets, aterm, cells, observed, weights, counts):
    nf = lax.axis_size("facet")
    nt = lax.axis_size("team")
    nb = lax.axis_size("sub")
    rdev, length = facet_rows.shape[2:]
    size = aterm.shape[-1]
    slots = cells.shape[-1]
    n = nf * nt
    tiles = length // LANES
    dims = (nf, nt, nb, length, size, rdev)
    consts = [jnp.asarray(v) for v in tables(size)]
    hbm = pl.BlockSpec(memory_space=pltpu.HBM)
    operands = [
        sub_offsets.T, facet_offsets.T, counts, facet_rows, aterm, cells, observed,
        weights.transpose(0, 2, 1, 3), *consts,
    ]
    dma = pltpu.SemaphoreType.DMA
    vmem = pltpu.VMEM
    return pl.pallas_call(
        functools.partial(body, dims),
        out_shape=pltpu.VMEM((1, 2, rdev, length // nb), F32),
        in_specs=[hbm] * 10,
        out_specs=pl.BlockSpec(memory_space=pltpu.VMEM),
        scratch_shapes=[
            *[pltpu.SMEM(v.shape, v.dtype) for v in operands[:3]],
            vmem(facet_rows.shape, BF),
            vmem((size, size), BF),
            vmem((2, slots), jnp.int32),
            vmem((2, slots), BF),
            *[vmem(v.shape, v.dtype) for v in operands[7:]],
            vmem((nf, rdev, 2 * M), BF),
            vmem((n, rdev, 2 * M), BF),
            vmem((8, slots), BF),
            vmem((nt, 8, slots), BF),
            vmem((nf, rdev, 2 * M), BF),
            vmem((nb, nf, rdev, 2 * M), BF),
            vmem((nf, 2, tiles, M), F32),
            vmem((nb, nf, 2, tiles // nb, M), F32),
            vmem((nf, 2 * M, 2 * LANES), BF),
            vmem((nf, 2 * M, 2 * LANES), BF),
            vmem((2, size // FINE, slots), F32),
            vmem((nt, size, slots), BF),
            vmem((nt, 2, size, slots), BF),
            vmem((nt, size, slots), F32),
            vmem((nt, size, slots), F32),
            dma, dma, dma, dma((nt,)), dma, dma((3,)), dma((4,)), pltpu.SemaphoreType.REGULAR((max(nt - 1, 1),)),
        ],
        compiler_params=pltpu.CompilerParams(
            collective_id=0, has_side_effects=True
        ),
    )(*operands)


def solution(mesh):
    placed = (
        P("facet", None, "team", None),
        P(),
        P(),
        P("facet", None, None, None),
        P("facet", None, "team", None, None),
        P("facet", None, "team", None, None),
        P("facet", None, "team", None),
        P(),
    )
    return jax.shard_map(
        local,
        mesh=mesh,
        in_specs=placed,
        out_specs=P("facet", None, "team", "sub"),
        check_vma=False,
    )
```

```python
import functools
import math

import jax
import jax.numpy as jnp
import ml_dtypes
import numpy as np
from jax import lax
from jax.experimental import pallas as pl
from jax.experimental.pallas import tpu as pltpu
from jax.sharding import PartitionSpec as P

M = 128
LANES = 128
FINE = 16
HALF_BITS = 5
PIECES = 2
TWO_PI = 2.0 * math.pi
BF = jnp.bfloat16
F32 = jnp.float32
MESH = pl.DeviceIdType.MESH


def sincos(turns, period):
    shift = period.bit_length() - 3
    quad = (turns + (1 << (shift - 1))) >> shift
    t = (turns - (quad << shift)).astype(F32) * (TWO_PI / period)
    t2 = t * t
    s = t * (1.0 + t2 * (-1.0 / 6 + t2 * (1.0 / 120 + t2 * (-1.0 / 5040))))
    c = 1.0 + t2 * (-0.5 + t2 * (1.0 / 24 + t2 * (-1.0 / 720 + t2 * (1.0 / 40320))))
    odd = (quad & 1) != 0
    cos = jnp.where(odd, s, c)
    sin = jnp.where(odd, c, s)
    cos = jnp.where(((quad + 1) & 2) != 0, -cos, cos)
    sin = jnp.where((quad & 2) != 0, -sin, sin)
    return cos, sin


def mm(left, right):
    return jnp.dot(left, right, preferred_element_type=F32)


def mm_nt(left, right):
    return lax.dot_general(left, right, (((1,), (1,)), ((), ())), preferred_element_type=F32)


def cat(parts, axis):
    return jnp.concatenate(parts, axis)


def iota(shape, dim):
    return lax.broadcasted_iota(jnp.int32, shape, dim)


def body(dims, *refs):
    (sub_hbm, fac_hbm, cnt_hbm, rows_hbm, aterm_hbm, cells_hbm, obs_hbm, wt_hbm, kk_hbm, kt_hbm) = refs[:10]
    out = refs[10]
    (
        sub_off, fac_off, counts, rows, aterm, cells, observed, weights, kk, kt,
        spec_out, got1, slot_out, got_x, fold_out, got2,
        tw1, tw2, wt_near, wt_far, coarse, col_w, row_w, row_c, row_s,
        sent, recv1, recv_x, recv2, in_sem, ready,
    ) = refs[11:]
    nf, nt, nb, length, size, rdev = dims
    rall = rdev * nt
    n = nf * nt
    slots = cells.shape[-1]
    period = 4 * size
    tiles = length // LANES
    my_f = lax.axis_index("facet")
    my_t = lax.axis_index("team")
    my_b = lax.axis_index("sub")
    me = my_f * nt + my_t
    other = 1 - my_b

    fetches = [
        pltpu.make_async_copy(sub_hbm, sub_off, in_sem.at[0]),
        pltpu.make_async_copy(rows_hbm, rows, in_sem.at[1]),
        pltpu.make_async_copy(fac_hbm, fac_off, in_sem.at[2]),
        pltpu.make_async_copy(cnt_hbm, counts, in_sem.at[2]),
        pltpu.make_async_copy(cells_hbm.at[0, my_b, 0], cells, in_sem.at[2]),
        pltpu.make_async_copy(obs_hbm.at[0, my_b, 0], observed, in_sem.at[2]),
        pltpu.make_async_copy(wt_hbm, weights, in_sem.at[2]),
        pltpu.make_async_copy(kt_hbm, kt, in_sem.at[0]),
        pltpu.make_async_copy(kk_hbm, kk, in_sem.at[1]),
        pltpu.make_async_copy(aterm_hbm.at[0, my_b], aterm, in_sem.at[3]),
    ]
    fetches[0].start()
    piece = length // PIECES
    for c in range(2):
        for q in range(PIECES):
            lanes = pl.ds(q * piece, piece)
            pltpu.make_async_copy(
                rows_hbm.at[0, c, :, lanes], rows.at[0, c, :, lanes], in_sem.at[1]
            ).start()
    for fetch in fetches[2:7]:
        fetch.start()

    barrier = pltpu.get_barrier_semaphore()
    nc = 2 - nf % 2
    ny = nf // nc
    rows_far = [(y + ny // 2) % ny for y in range(ny)]
    order = [y * nc + c for c in range(nc) for y in rows_far]
    first = order[:ny]
    second = order[ny:]
    local_k = list(range(nc))
    urgent = [k for k in order if k >= nc]
    my_c = lax.rem(my_f, nc)

    def facet_at(k):
        return lax.rem(my_f // nc + k // nc, ny) * nc + k % nc

    def greet(k, t, b):
        pl.semaphore_signal(
            barrier, inc=1, device_id={"facet": facet_at(k), "team": t, "sub": b}, device_id_type=MESH
        )

    def unless_self(k, act):
        if k < nc:
            pl.when(my_c != k)(act)
        else:
            act()

    def greet_team(t):
        for k in order:
            greet(k, t, my_b)

    for t in reversed(range(1, nt)):
        pl.when(my_t < t)(functools.partial(greet_team, t))
    pl.semaphore_signal(
        barrier, inc=1, device_id={"facet": my_f, "team": my_t, "sub": other}, device_id_type=MESH
    )
    for k in order:
        unless_self(k, functools.partial(greet, k, my_t, my_b))

    base_c, base_s = sincos(iota((M, LANES), 0) * iota((M, LANES), 1), length)
    lane_row = iota((1, LANES), 1)

    fetches[0].wait()

    def column_weights(shift_v):
        pc, ps = sincos(lane_row * shift_v, length)
        c = (base_c * pc - base_s * ps).astype(BF)
        s = (base_s * pc + base_c * ps).astype(BF)
        return cat([cat([c, s], 1), cat([-s, c], 1)], 0)

    scale = 1.0 / math.sqrt(length)

    def prepare(k):
        shift_v = sub_off[1, facet_at(k) * nb + my_b]
        wt_near[k] = column_weights(shift_v)
        c, s = sincos(iota((tiles, M), 0) * (iota((tiles, M), 1) + shift_v), tiles)
        tw1[k, 0] = c * scale
        tw1[k, 1] = s * scale

    for k in first:
        prepare(k)
    fetches[1].wait()
    for fetch in fetches[7:]:
        fetch.start()
    x = [
        cat([rows[0, c, :, k * LANES : (k + 1) * LANES].astype(F32) for k in range(tiles)], 0)
        for c in range(2)
    ]
    x = cat(x, 1).astype(BF)

    def spectrum(k):
        y = mm_nt(x, wt_near[k])
        acc = [None] * 4
        for j in range(tiles):
            yr = y[j * rdev : (j + 1) * rdev, :M]
            yi = y[j * rdev : (j + 1) * rdev, M:]
            c = tw1[k, 0, j : j + 1, :]
            s = tw1[k, 1, j : j + 1, :]
            q = 2 * (j % 2)
            add_re = yr * c + yi * s
            add_im = yi * c - yr * s
            acc[q] = add_re if acc[q] is None else acc[q] + add_re
            acc[q + 1] = add_im if acc[q + 1] is None else acc[q + 1] + add_im
        spec_out[k] = cat([acc[0] + acc[2], acc[1] + acc[3]], 1).astype(BF)

    for k in first:
        spectrum(k)
    for i in (2, 3, 4, 5, 6):
        fetches[i].wait()
    live = iota((1, slots), 1) < counts[my_f, my_b, my_t]
    all_wt = weights[0, 0].astype(F32)
    own_wt = jnp.where(my_b == 0, all_wt[0:1, :], all_wt[1:2, :])
    own_wt = jnp.where(live, own_wt, 0.0)
    place = cells[...]
    packed = cat(
        [
            (place >> HALF_BITS).astype(F32), (place & ((1 << HALF_BITS) - 1)).astype(F32),
            observed[...].astype(F32), own_wt, own_wt,
        ],
        0,
    ).astype(BF)
    slot_out[...] = packed
    got_x[my_t] = packed

    pl.semaphore_wait(barrier, nf * (my_t + 1))

    def report(t):
        for k in order:
            pl.semaphore_signal(
                ready.at[my_t - 1], inc=1,
                device_id={"facet": facet_at(k), "team": t, "sub": my_b}, device_id_type=MESH,
            )


    def copy_x(t):
        return pltpu.make_async_remote_copy(
            src_ref=slot_out,
            dst_ref=got_x.at[my_t],
            send_sem=sent,
            recv_sem=recv_x.at[my_t],
            device_id={"facet": my_f, "team": t, "sub": my_b},
            device_id_type=MESH,
        )

    def copy1(k, t):
        return pltpu.make_async_remote_copy(
            src_ref=spec_out.at[k],
            dst_ref=got1.at[me],
            send_sem=sent,
            recv_sem=recv1,
            device_id={"facet": facet_at(k), "team": t, "sub": my_b},
            device_id_type=MESH,
        )

    def send_specs(ks, t):
        for k in ks:
            if k >= nc:
                copy1(k, t).start()
            else:
                there = jnp.logical_or(my_t != t, my_c != k)
                pl.when(there)(lambda: copy1(k, t).start())

    def send_slots(t):
        pl.when(my_t != t)(lambda: copy_x(t).start())

    send_specs(first, 0)
    send_slots(0)
    for t in range(nt - 1):
        pl.when(my_t > t)(functools.partial(report, t))
    for k in second:
        prepare(k)
        spectrum(k)
    send_specs(second, 0)
    got1[me] = spec_out[my_c]

    for i in (7, 8, 9):
        fetches[i].wait()
    mirror = size // 2
    shift_u = sub_off[0, my_f * nb + my_b]
    step = length // rall
    scale_g = 1.0 / math.sqrt(rall * nf)
    lane = iota((1, n * rdev), 1)
    col_a = jnp.zeros((1, n * rdev), jnp.int32)
    row = iota((n * rdev, 1), 0)
    row_cc = jnp.zeros((n * rdev, 1), jnp.int32)
    row2 = iota((nf * rdev, 1), 0)
    row_a = jnp.zeros((nf * rdev, 1), jnp.int32)
    for f in range(nf):
        col_a = jnp.where(lane // rall == f, fac_off[0, f], col_a)
        row_cc = jnp.where(row // rall == f, fac_off[1, f], row_cc)
        row_a = jnp.where(row2 // rdev == f, fac_off[0, f], row_a)
    p0 = iota((M, n * rdev), 0)
    gc, gs = sincos(p0 * col_a - (p0 + shift_u) * (lane % rall * step), length)
    gc = (gc * scale_g).astype(BF)
    gs = (gs * scale_g).astype(BF)
    a_mat = mm(kt[...], cat([cat([gc, gs], 1), cat([-gs, gc], 1)], 0)).astype(BF)
    p1 = iota((nf * rdev, M), 1)
    hc, hs = sincos(p1 * row_a - (p1 + shift_u) * ((row2 % rdev + my_t * rdev) * step), length)
    hc = (hc * scale_g).astype(BF)
    hs = (hs * scale_g).astype(BF)
    at = mm_nt(cat([cat([hc, -hs], 1), cat([hs, hc], 1)], 0), kt[...])
    ah = cat([at[: nf * rdev], -at[nf * rdev :]], 1).astype(BF)
    ec, es = sincos(iota((n * rdev, M), 1) * row_cc, length)

    for t in range(1, nt):
        pl.when(my_t < t)(lambda: pl.semaphore_wait(ready.at[t - 1], nf))
        send_slots(t)
        send_specs(order, t)
    flip = (iota((mirror, mirror), 0) + iota((mirror, mirror), 1) == mirror - 1).astype(F32).astype(BF)
    left_half = mm(aterm[:, :mirror], flip)
    amap = cat([aterm[:, mirror:].astype(F32), left_half], 1)
    amap = cat([amap, amap], 1)
    half = tiles // nb
    scale_b = 1.0 / (math.sqrt(M) * size)
    tile_no = iota((half, M), 0) + my_b * half
    for far in range(2):
        for a in range(nf):
            shift_v = sub_off[1, facet_at(a) * nb + (other if far else my_b)]
            if far:
                wt_far[a] = column_weights(shift_v)
            m_no = iota((half, M), 1)
            c, s = sincos((m_no + shift_v) * (tile_no * LANES) - m_no * fac_off[1, my_f], length)
            tw2[far, a, 0] = c * scale_b
            tw2[far, a, 1] = s * scale_b

    fine_no = iota((FINE, slots), 0)
    row_no = iota((size // FINE, slots), 0)
    col_no = iota((mirror // FINE, slots), 0)
    for k in range(nt):
        src = lax.rem(my_t + k, nt)
        if k:
            pltpu.make_async_copy(got_x.at[src], got_x.at[src], recv_x.at[src]).wait()
        pos = got_x[src].astype(F32)[0:4, :].astype(jnp.int32)
        pos = (pos[0:2, :] << HALF_BITS) + pos[2:4, :]
        pos_x = pos[0:1, :]
        pos_y = pos[1:2, :]
        lo_c, lo_s = sincos(2 * fine_no * pos_x, 2 * period)
        hi_c, hi_s = sincos(2 * FINE * row_no * pos_x + (size - 1) * pos_y, 2 * period)
        coarse[0] = hi_c
        coarse[1] = hi_s
        for q in range(size // FINE):
            c1 = coarse[0, q : q + 1, :]
            s1 = coarse[1, q : q + 1, :]
            rng = slice(q * FINE, (q + 1) * FINE)
            c = c1 * lo_c - s1 * lo_s
            s = s1 * lo_c + c1 * lo_s
            row_c[k, rng, :] = c
            row_s[k, rng, :] = s
            row_w[k, 0, rng, :] = c.astype(BF)
            row_w[k, 1, rng, :] = s.astype(BF)
        lo_c, lo_s = sincos((2 * fine_no + 1) * pos_y, 2 * period)
        hi_c, hi_s = sincos(2 * FINE * col_no * pos_y, 2 * period)
        coarse[0, : mirror // FINE, :] = hi_c
        coarse[1, : mirror // FINE, :] = hi_s
        for q in range(mirror // FINE):
            c1 = coarse[0, q : q + 1, :]
            s1 = coarse[1, q : q + 1, :]
            rng = slice(q * FINE, (q + 1) * FINE)
            col_w[k, rng, :] = (c1 * lo_c - s1 * lo_s).astype(BF)
            rng = slice(mirror + q * FINE, mirror + (q + 1) * FINE)
            col_w[k, rng, :] = (s1 * lo_c + c1 * lo_s).astype(BF)

    done = got1.at[pl.ds(0, n - 1)]
    pltpu.make_async_copy(done, done, recv1).wait()
    sp = got1[...].astype(F32).reshape(n * rdev, 2 * M)
    sr = sp[:, :M]
    si = sp[:, M:]
    turn_re = (sr * ec - si * es).astype(BF)
    turn_im = (sr * es + si * ec).astype(BF)
    full = mm(a_mat, cat([cat([turn_re, turn_im], 1), cat([-turn_im, turn_re], 1)], 0))
    image = mm(full.astype(BF), kk[...])
    image = amap * image
    re_p, re_n, im_p, im_n = (image[:, c * mirror : (c + 1) * mirror] for c in range(4))
    folded = cat(
        [cat([re_p + re_n, im_p - im_n], 1), cat([im_p + im_n, re_n - re_p], 1)], 0
    ).astype(BF)
    def degrid(k):
        src = lax.rem(my_t + k, nt)
        z = mm(folded, col_w[k])
        zr = z[:size]
        zi = z[size:]
        rc = row_c[k]
        rs = row_s[k]
        pred_re = jnp.sum(rc * zr + rs * zi, 0, keepdims=True) * (1.0 / size)
        pred_im = jnp.sum(rc * zi - rs * zr, 0, keepdims=True) * (1.0 / size)
        info = got_x[src].astype(F32)
        res_re = info[6:7, :] * (info[4:5, :] - pred_re)
        res_im = info[6:7, :] * (info[5:6, :] - pred_im)
        rc = row_w[k, 0]
        rs = row_w[k, 1]
        res_re = jnp.broadcast_to(res_re.astype(BF), (size, slots))
        res_im = jnp.broadcast_to(res_im.astype(BF), (size, slots))
        left_re = rc * res_re - rs * res_im
        left_im = rc * res_im + rs * res_re
        return cat([left_re, left_im], 0)

    left = [None] * nt
    prod = None
    for k in range(nt + 1):
        if k < nt:
            left[k] = degrid(k)
        if k:
            part = mm_nt(left[k - 1], col_w[k - 1])
            prod = part if prod is None else prod + part
    cr, sr = prod[:size, :mirror], prod[:size, mirror:]
    ci, si = prod[size:, :mirror], prod[size:, mirror:]
    grid = cat([cr - si, cr + si, ci + sr, ci - sr], 1)
    v = (amap * grid).astype(BF)
    u = mm_nt(v, kk[...]).astype(BF)
    ur = u[:, :M]
    ui = u[:, M:]
    part = mm(ah, cat([u, cat([-ui, ur], 1)], 0))
    fold_out[...] = part.reshape(nf, rdev, 2 * M).astype(BF)


    def copy2(k, far):
        return pltpu.make_async_remote_copy(
            src_ref=fold_out.at[facet_at(k)],
            dst_ref=got2.at[far, my_f],
            send_sem=sent,
            recv_sem=recv2.at[min(k // nc, 1) + far],
            device_id={"facet": facet_at(k), "team": my_t, "sub": other if far else my_b},
            device_id_type=MESH,
        )

    for k in order:
        copy2(k, 1).start()
    for k in order:
        unless_self(k, lambda: copy2(k, 0).start())
    got2[0, my_f] = fold_out[my_f]

    def update(total, far, ks):
        for k in ks:
            g = got2[far, facet_at(k)].astype(F32)
            gr = g[:, :M]
            gi = g[:, M:]
            parts = []
            for j in range(half):
                c = tw2[far, k, 0, j : j + 1, :]
                s = tw2[far, k, 1, j : j + 1, :]
                parts.append(cat([gr * c - gi * s, gr * s + gi * c], 1))
            y = mm(cat(parts, 0).astype(BF), (wt_far if far else wt_near)[k])
            total = y if total is None else total + y
        return total

    def arrived(which, count):
        done = got1.at[pl.ds(0, count)]
        pltpu.make_async_copy(done, done, recv2.at[which]).wait()

    if nc > 1:
        arrived(0, nc - 1)
    total = update(None, 0, local_k)
    arrived(1, nf)
    total = update(total, 1, local_k)
    total = update(total, 0, urgent)
    if ny > 1:
        arrived(2, nf - nc)
    total = update(total, 1, urgent)
    for k in range(half):
        rng = slice(k * rdev, (k + 1) * rdev)
        lanes = slice(k * LANES, (k + 1) * LANES)
        out[0, 0, :, lanes] = total[rng, :LANES]
        out[0, 1, :, lanes] = total[rng, LANES:]
    for count in (n - 1, nt - 1, 2 * nf - 1):
        gone = got1.at[pl.ds(0, count)]
        pltpu.make_async_copy(gone, gone, sent).wait()


def tables(size):
    angle = (np.arange(M)[:, None] * np.arange(size)[None, :] % size) * (TWO_PI / size)
    kc = np.cos(angle) / math.sqrt(M)
    ks = np.sin(angle) / math.sqrt(M)
    kt = np.concatenate([kc.T, ks.T], 1)
    half = size // 2
    order = np.concatenate([np.arange(half, size), np.arange(half - 1, -1, -1)])
    kc, ks = kc[:, order], ks[:, order]
    kk = np.block([[kc, ks], [-ks, kc]])
    return [np.asarray(v, np.float32).astype(ml_dtypes.bfloat16) for v in (kk, kt)]


def local(facet_rows, sub_offsets, facet_offsets, aterm, cells, observed, weights, counts):
    nf = lax.axis_size("facet")
    nt = lax.axis_size("team")
    nb = lax.axis_size("sub")
    rdev, length = facet_rows.shape[2:]
    size = aterm.shape[-1]
    slots = cells.shape[-1]
    n = nf * nt
    tiles = length // LANES
    dims = (nf, nt, nb, length, size, rdev)
    consts = [jnp.asarray(v) for v in tables(size)]
    hbm = pl.BlockSpec(memory_space=pltpu.HBM)
    operands = [
        sub_offsets.T, facet_offsets.T, counts, facet_rows, aterm, cells, observed,
        weights.transpose(0, 2, 1, 3), *consts,
    ]
    dma = pltpu.SemaphoreType.DMA
    vmem = pltpu.VMEM
    return pl.pallas_call(
        functools.partial(body, dims),
        out_shape=pltpu.VMEM((1, 2, rdev, length // nb), F32),
        in_specs=[hbm] * 10,
        out_specs=pl.BlockSpec(memory_space=pltpu.VMEM),
        scratch_shapes=[
            *[pltpu.SMEM(v.shape, v.dtype) for v in operands[:3]],
            vmem(facet_rows.shape, BF),
            vmem((size, size), BF),
            vmem((2, slots), jnp.int32),
            vmem((2, slots), BF),
            *[vmem(v.shape, v.dtype) for v in operands[7:]],
            vmem((nf, rdev, 2 * M), BF),
            vmem((n, rdev, 2 * M), BF),
            vmem((8, slots), BF),
            vmem((nt, 8, slots), BF),
            vmem((nf, rdev, 2 * M), BF),
            vmem((nb, nf, rdev, 2 * M), BF),
            vmem((nf, 2, tiles, M), F32),
            vmem((nb, nf, 2, tiles // nb, M), F32),
            vmem((nf, 2 * M, 2 * LANES), BF),
            vmem((nf, 2 * M, 2 * LANES), BF),
            vmem((2, size // FINE, slots), F32),
            vmem((nt, size, slots), BF),
            vmem((nt, 2, size, slots), BF),
            vmem((nt, size, slots), F32),
            vmem((nt, size, slots), F32),
            dma, dma, dma((nt,)), dma((3,)), dma((4,)), pltpu.SemaphoreType.REGULAR((max(nt - 1, 1),)),
        ],
        compiler_params=pltpu.CompilerParams(
            collective_id=0, has_side_effects=True
        ),
    )(*operands)


def solution(mesh):
    placed = (
        P("facet", None, "team", None),
        P(),
        P(),
        P("facet", None, None, None),
        P("facet", None, "team", None, None),
        P("facet", None, "team", None, None),
        P("facet", None, "team", None),
        P(),
    )
    return jax.shard_map(
        local,
        mesh=mesh,
        in_specs=placed,
        out_specs=P("facet", None, "team", "sub"),
        check_vma=False,
    )
```

```python
import functools
import math

import jax
import jax.numpy as jnp
import ml_dtypes
import numpy as np
from jax import lax
from jax.experimental import pallas as pl
from jax.experimental.pallas import tpu as pltpu
from jax.sharding import PartitionSpec as P

M = 128
LANES = 128
FINE = 16
HALF_BITS = 5
PIECES = 2
TWO_PI = 2.0 * math.pi
BF = jnp.bfloat16
F32 = jnp.float32
MESH = pl.DeviceIdType.MESH


def sincos(turns, period):
    shift = period.bit_length() - 3
    quad = (turns + (1 << (shift - 1))) >> shift
    t = (turns - (quad << shift)).astype(F32) * (TWO_PI / period)
    t2 = t * t
    s = t * (1.0 + t2 * (-1.0 / 6 + t2 * (1.0 / 120 + t2 * (-1.0 / 5040))))
    c = 1.0 + t2 * (-0.5 + t2 * (1.0 / 24 + t2 * (-1.0 / 720 + t2 * (1.0 / 40320))))
    odd = (quad & 1) != 0
    cos = jnp.where(odd, s, c)
    sin = jnp.where(odd, c, s)
    cos = jnp.where(((quad + 1) & 2) != 0, -cos, cos)
    sin = jnp.where((quad & 2) != 0, -sin, sin)
    return cos, sin


def mm(left, right):
    return jnp.dot(left, right, preferred_element_type=F32)


def mm_nt(left, right):
    return lax.dot_general(left, right, (((1,), (1,)), ((), ())), preferred_element_type=F32)


def cat(parts, axis):
    return jnp.concatenate(parts, axis)


def iota(shape, dim):
    return lax.broadcasted_iota(jnp.int32, shape, dim)


def body(dims, *refs):
    (sub_hbm, fac_hbm, cnt_hbm, rows_hbm, aterm_hbm, cells_hbm, obs_hbm, wt_hbm, kk_hbm, kt_hbm) = refs[:10]
    out = refs[10]
    (
        sub_off, fac_off, counts, rows, aterm, cells, observed, weights, kk, kt,
        spec_out, got1, slot_out, got_x, fold_out, got2,
        tw1, tw2, wt_near, wt_far, coarse, col_w, row_w, row_c, row_s,
        sent, recv1, recv_x, recv2, in_sem, ready,
    ) = refs[11:]
    nf, nt, nb, length, size, rdev = dims
    rall = rdev * nt
    n = nf * nt
    slots = cells.shape[-1]
    period = 4 * size
    tiles = length // LANES
    my_f = lax.axis_index("facet")
    my_t = lax.axis_index("team")
    my_b = lax.axis_index("sub")
    me = my_f * nt + my_t
    other = 1 - my_b

    fetches = [
        pltpu.make_async_copy(sub_hbm, sub_off, in_sem.at[0]),
        pltpu.make_async_copy(rows_hbm, rows, in_sem.at[1]),
        pltpu.make_async_copy(fac_hbm, fac_off, in_sem.at[4]),
        pltpu.make_async_copy(cnt_hbm, counts, in_sem.at[2]),
        pltpu.make_async_copy(cells_hbm.at[0, my_b, 0], cells, in_sem.at[2]),
        pltpu.make_async_copy(obs_hbm.at[0, my_b, 0], observed, in_sem.at[2]),
        pltpu.make_async_copy(wt_hbm, weights, in_sem.at[2]),
        pltpu.make_async_copy(kt_hbm, kt, in_sem.at[0]),
        pltpu.make_async_copy(kk_hbm, kk, in_sem.at[1]),
        pltpu.make_async_copy(aterm_hbm.at[0, my_b], aterm, in_sem.at[3]),
    ]
    fetches[0].start()
    fetches[2].start()
    piece = length // PIECES
    for c in range(2):
        for q in range(PIECES):
            lanes = pl.ds(q * piece, piece)
            pltpu.make_async_copy(
                rows_hbm.at[0, c, :, lanes], rows.at[0, c, :, lanes], in_sem.at[1]
            ).start()
    for fetch in fetches[3:7]:
        fetch.start()

    barrier = pltpu.get_barrier_semaphore()
    nc = 2 - nf % 2
    ny = nf // nc
    rows_far = [(y + ny // 2) % ny for y in range(ny)]
    order = [y * nc + c for c in range(nc) for y in rows_far]
    first = order[:ny]
    second = order[ny:]
    local_k = list(range(nc))
    urgent = [k for k in order if k >= nc]
    my_c = lax.rem(my_f, nc)

    def facet_at(k):
        return lax.rem(my_f // nc + k // nc, ny) * nc + k % nc

    def greet(k, t, b):
        pl.semaphore_signal(
            barrier, inc=1, device_id={"facet": facet_at(k), "team": t, "sub": b}, device_id_type=MESH
        )

    def unless_self(k, act):
        if k < nc:
            pl.when(my_c != k)(act)
        else:
            act()

    def greet_team(t):
        for k in order:
            greet(k, t, my_b)

    for t in reversed(range(1, nt)):
        pl.when(my_t < t)(functools.partial(greet_team, t))
    pl.semaphore_signal(
        barrier, inc=1, device_id={"facet": my_f, "team": my_t, "sub": other}, device_id_type=MESH
    )
    for k in order:
        unless_self(k, functools.partial(greet, k, my_t, my_b))

    base_c, base_s = sincos(iota((M, LANES), 0) * iota((M, LANES), 1), length)
    lane_row = iota((1, LANES), 1)

    fetches[0].wait()
    fetches[2].wait()

    def column_weights(shift_v):
        pc, ps = sincos(lane_row * shift_v, length)
        c = (base_c * pc - base_s * ps).astype(BF)
        s = (base_s * pc + base_c * ps).astype(BF)
        return cat([cat([c, s], 1), cat([-s, c], 1)], 0)

    scale = 1.0 / math.sqrt(length)

    def prepare(k):
        shift_v = sub_off[1, facet_at(k) * nb + my_b]
        wt_near[k] = column_weights(shift_v)
        m_no = iota((tiles, M), 1)
        turns = iota((tiles, M), 0) * LANES * (m_no + shift_v) - m_no * fac_off[1, my_f]
        c, s = sincos(turns, length)
        tw1[k, 0] = c * scale
        tw1[k, 1] = s * scale

    for k in first:
        prepare(k)
    fetches[1].wait()
    for fetch in fetches[7:]:
        fetch.start()
    x = [
        cat([rows[0, c, :, k * LANES : (k + 1) * LANES].astype(F32) for k in range(tiles)], 0)
        for c in range(2)
    ]
    x = cat(x, 1).astype(BF)

    def spectrum(k):
        y = mm_nt(x, wt_near[k])
        acc = [None] * 4
        for j in range(tiles):
            yr = y[j * rdev : (j + 1) * rdev, :M]
            yi = y[j * rdev : (j + 1) * rdev, M:]
            c = tw1[k, 0, j : j + 1, :]
            s = tw1[k, 1, j : j + 1, :]
            q = 2 * (j % 2)
            add_re = yr * c + yi * s
            add_im = yi * c - yr * s
            acc[q] = add_re if acc[q] is None else acc[q] + add_re
            acc[q + 1] = add_im if acc[q + 1] is None else acc[q + 1] + add_im
        spec_out[k] = cat([acc[0] + acc[2], acc[1] + acc[3]], 1).astype(BF)

    for k in first:
        spectrum(k)
    for i in (3, 4, 5, 6):
        fetches[i].wait()
    live = iota((1, slots), 1) < counts[my_f, my_b, my_t]
    all_wt = weights[0, 0].astype(F32)
    own_wt = jnp.where(my_b == 0, all_wt[0:1, :], all_wt[1:2, :])
    own_wt = jnp.where(live, own_wt, 0.0)
    place = cells[...]
    packed = cat(
        [
            (place >> HALF_BITS).astype(F32), (place & ((1 << HALF_BITS) - 1)).astype(F32),
            observed[...].astype(F32), own_wt, own_wt,
        ],
        0,
    ).astype(BF)
    slot_out[...] = packed
    got_x[my_t] = packed

    pl.semaphore_wait(barrier, nf * (my_t + 1))

    def report(t):
        for k in order:
            pl.semaphore_signal(
                ready.at[my_t - 1], inc=1,
                device_id={"facet": facet_at(k), "team": t, "sub": my_b}, device_id_type=MESH,
            )


    def copy_x(t):
        return pltpu.make_async_remote_copy(
            src_ref=slot_out,
            dst_ref=got_x.at[my_t],
            send_sem=sent,
            recv_sem=recv_x.at[my_t],
            device_id={"facet": my_f, "team": t, "sub": my_b},
            device_id_type=MESH,
        )

    def copy1(k, t):
        return pltpu.make_async_remote_copy(
            src_ref=spec_out.at[k],
            dst_ref=got1.at[me],
            send_sem=sent,
            recv_sem=recv1,
            device_id={"facet": facet_at(k), "team": t, "sub": my_b},
            device_id_type=MESH,
        )

    def send_specs(ks, t):
        for k in ks:
            if k >= nc:
                copy1(k, t).start()
            else:
                there = jnp.logical_or(my_t != t, my_c != k)
                pl.when(there)(lambda: copy1(k, t).start())

    def send_slots(t):
        pl.when(my_t != t)(lambda: copy_x(t).start())

    send_specs(first, 0)
    send_slots(0)
    for t in range(nt - 1):
        pl.when(my_t > t)(functools.partial(report, t))
    for k in second:
        prepare(k)
        spectrum(k)
    send_specs(second, 0)
    got1[me] = spec_out[my_c]

    for i in (7, 8, 9):
        fetches[i].wait()
    mirror = size // 2
    shift_u = sub_off[0, my_f * nb + my_b]
    step = length // rall
    scale_g = 1.0 / math.sqrt(rall * nf)
    lane = iota((1, n * rdev), 1)
    col_a = jnp.zeros((1, n * rdev), jnp.int32)
    row2 = iota((nf * rdev, 1), 0)
    row_a = jnp.zeros((nf * rdev, 1), jnp.int32)
    for f in range(nf):
        col_a = jnp.where(lane // rall == f, fac_off[0, f], col_a)
        row_a = jnp.where(row2 // rdev == f, fac_off[0, f], row_a)
    p0 = iota((M, n * rdev), 0)
    gc, gs = sincos(p0 * col_a - (p0 + shift_u) * (lane % rall * step), length)
    gc = (gc * scale_g).astype(BF)
    gs = (gs * scale_g).astype(BF)
    a_mat = mm(kt[...], cat([cat([gc, gs], 1), cat([-gs, gc], 1)], 0)).astype(BF)
    p1 = iota((nf * rdev, M), 1)
    hc, hs = sincos(p1 * row_a - (p1 + shift_u) * ((row2 % rdev + my_t * rdev) * step), length)
    hc = (hc * scale_g).astype(BF)
    hs = (hs * scale_g).astype(BF)
    at = mm_nt(cat([cat([hc, -hs], 1), cat([hs, hc], 1)], 0), kt[...])
    ah = cat([at[: nf * rdev], -at[nf * rdev :]], 1).astype(BF)

    for t in range(1, nt):
        pl.when(my_t < t)(lambda: pl.semaphore_wait(ready.at[t - 1], nf))
        send_slots(t)
        send_specs(order, t)
    flip = (iota((mirror, mirror), 0) + iota((mirror, mirror), 1) == mirror - 1).astype(F32).astype(BF)
    left_half = mm(aterm[:, :mirror], flip)
    amap = cat([aterm[:, mirror:].astype(F32), left_half], 1)
    amap = cat([amap, amap], 1)
    half = tiles // nb
    scale_b = 1.0 / (math.sqrt(M) * size)
    tile_no = iota((half, M), 0) + my_b * half
    for far in range(2):
        for a in range(nf):
            shift_v = sub_off[1, facet_at(a) * nb + (other if far else my_b)]
            if far:
                wt_far[a] = column_weights(shift_v)
            m_no = iota((half, M), 1)
            c, s = sincos((m_no + shift_v) * (tile_no * LANES) - m_no * fac_off[1, my_f], length)
            tw2[far, a, 0] = c * scale_b
            tw2[far, a, 1] = s * scale_b

    fine_no = iota((FINE, slots), 0)
    row_no = iota((size // FINE, slots), 0)
    col_no = iota((mirror // FINE, slots), 0)
    for k in range(nt):
        src = lax.rem(my_t + k, nt)
        if k:
            pltpu.make_async_copy(got_x.at[src], got_x.at[src], recv_x.at[src]).wait()
        pos = got_x[src].astype(F32)[0:4, :].astype(jnp.int32)
        pos = (pos[0:2, :] << HALF_BITS) + pos[2:4, :]
        pos_x = pos[0:1, :]
        pos_y = pos[1:2, :]
        lo_c, lo_s = sincos(2 * fine_no * pos_x, 2 * period)
        hi_c, hi_s = sincos(2 * FINE * row_no * pos_x + (size - 1) * pos_y, 2 * period)
        coarse[0] = hi_c
        coarse[1] = hi_s
        for q in range(size // FINE):
            c1 = coarse[0, q : q + 1, :]
            s1 = coarse[1, q : q + 1, :]
            rng = slice(q * FINE, (q + 1) * FINE)
            c = c1 * lo_c - s1 * lo_s
            s = s1 * lo_c + c1 * lo_s
            row_c[k, rng, :] = c
            row_s[k, rng, :] = s
            row_w[k, 0, rng, :] = c.astype(BF)
            row_w[k, 1, rng, :] = s.astype(BF)
        lo_c, lo_s = sincos((2 * fine_no + 1) * pos_y, 2 * period)
        hi_c, hi_s = sincos(2 * FINE * col_no * pos_y, 2 * period)
        coarse[0, : mirror // FINE, :] = hi_c
        coarse[1, : mirror // FINE, :] = hi_s
        for q in range(mirror // FINE):
            c1 = coarse[0, q : q + 1, :]
            s1 = coarse[1, q : q + 1, :]
            rng = slice(q * FINE, (q + 1) * FINE)
            col_w[k, rng, :] = (c1 * lo_c - s1 * lo_s).astype(BF)
            rng = slice(mirror + q * FINE, mirror + (q + 1) * FINE)
            col_w[k, rng, :] = (s1 * lo_c + c1 * lo_s).astype(BF)

    done = got1.at[pl.ds(0, n - 1)]
    pltpu.make_async_copy(done, done, recv1).wait()
    got = got1[...].astype(F32).reshape(n * rdev, 2 * M)
    got = cat([got, cat([-got[:, M:], got[:, :M]], 1)], 0).astype(BF)
    full = mm(a_mat, got)
    image = mm(full.astype(BF), kk[...])
    image = amap * image
    re_p, re_n, im_p, im_n = (image[:, c * mirror : (c + 1) * mirror] for c in range(4))
    folded = cat(
        [cat([re_p + re_n, im_p - im_n], 1), cat([im_p + im_n, re_n - re_p], 1)], 0
    ).astype(BF)
    def degrid(k):
        src = lax.rem(my_t + k, nt)
        z = mm(folded, col_w[k])
        zr = z[:size]
        zi = z[size:]
        rc = row_c[k]
        rs = row_s[k]
        pred_re = jnp.sum(rc * zr + rs * zi, 0, keepdims=True) * (1.0 / size)
        pred_im = jnp.sum(rc * zi - rs * zr, 0, keepdims=True) * (1.0 / size)
        info = got_x[src].astype(F32)
        res_re = info[6:7, :] * (info[4:5, :] - pred_re)
        res_im = info[6:7, :] * (info[5:6, :] - pred_im)
        rc = row_w[k, 0]
        rs = row_w[k, 1]
        res_re = jnp.broadcast_to(res_re.astype(BF), (size, slots))
        res_im = jnp.broadcast_to(res_im.astype(BF), (size, slots))
        left_re = rc * res_re - rs * res_im
        left_im = rc * res_im + rs * res_re
        return cat([left_re, left_im], 0)

    left = [None] * nt
    prod = None
    for k in range(nt + 1):
        if k < nt:
            left[k] = degrid(k)
        if k:
            part = mm_nt(left[k - 1], col_w[k - 1])
            prod = part if prod is None else prod + part
    cr, sr = prod[:size, :mirror], prod[:size, mirror:]
    ci, si = prod[size:, :mirror], prod[size:, mirror:]
    grid = cat([cr - si, cr + si, ci + sr, ci - sr], 1)
    v = (amap * grid).astype(BF)
    u = mm_nt(v, kk[...]).astype(BF)
    ur = u[:, :M]
    ui = u[:, M:]
    part = mm(ah, cat([u, cat([-ui, ur], 1)], 0))
    fold_out[...] = part.reshape(nf, rdev, 2 * M).astype(BF)


    def copy2(k, far):
        return pltpu.make_async_remote_copy(
            src_ref=fold_out.at[facet_at(k)],
            dst_ref=got2.at[far, my_f],
            send_sem=sent,
            recv_sem=recv2.at[min(k // nc, 1) + far],
            device_id={"facet": facet_at(k), "team": my_t, "sub": other if far else my_b},
            device_id_type=MESH,
        )

    for k in order:
        copy2(k, 1).start()
    for k in order:
        unless_self(k, lambda: copy2(k, 0).start())
    got2[0, my_f] = fold_out[my_f]

    def update(total, far, ks):
        for k in ks:
            g = got2[far, facet_at(k)].astype(F32)
            gr = g[:, :M]
            gi = g[:, M:]
            parts = []
            for j in range(half):
                c = tw2[far, k, 0, j : j + 1, :]
                s = tw2[far, k, 1, j : j + 1, :]
                parts.append(cat([gr * c - gi * s, gr * s + gi * c], 1))
            y = mm(cat(parts, 0).astype(BF), (wt_far if far else wt_near)[k])
            total = y if total is None else total + y
        return total

    def arrived(which, count):
        done = got1.at[pl.ds(0, count)]
        pltpu.make_async_copy(done, done, recv2.at[which]).wait()

    if nc > 1:
        arrived(0, nc - 1)
    total = update(None, 0, local_k)
    arrived(1, nf)
    total = update(total, 1, local_k)
    total = update(total, 0, urgent)
    if ny > 1:
        arrived(2, nf - nc)
    total = update(total, 1, urgent)
    for k in range(half):
        rng = slice(k * rdev, (k + 1) * rdev)
        lanes = slice(k * LANES, (k + 1) * LANES)
        out[0, 0, :, lanes] = total[rng, :LANES]
        out[0, 1, :, lanes] = total[rng, LANES:]
    for count in (n - 1, nt - 1, 2 * nf - 1):
        gone = got1.at[pl.ds(0, count)]
        pltpu.make_async_copy(gone, gone, sent).wait()


def tables(size):
    angle = (np.arange(M)[:, None] * np.arange(size)[None, :] % size) * (TWO_PI / size)
    kc = np.cos(angle) / math.sqrt(M)
    ks = np.sin(angle) / math.sqrt(M)
    kt = np.concatenate([kc.T, ks.T], 1)
    half = size // 2
    order = np.concatenate([np.arange(half, size), np.arange(half - 1, -1, -1)])
    kc, ks = kc[:, order], ks[:, order]
    kk = np.block([[kc, ks], [-ks, kc]])
    return [np.asarray(v, np.float32).astype(ml_dtypes.bfloat16) for v in (kk, kt)]


def local(facet_rows, sub_offsets, facet_offsets, aterm, cells, observed, weights, counts):
    nf = lax.axis_size("facet")
    nt = lax.axis_size("team")
    nb = lax.axis_size("sub")
    rdev, length = facet_rows.shape[2:]
    size = aterm.shape[-1]
    slots = cells.shape[-1]
    n = nf * nt
    tiles = length // LANES
    dims = (nf, nt, nb, length, size, rdev)
    consts = [jnp.asarray(v) for v in tables(size)]
    hbm = pl.BlockSpec(memory_space=pltpu.HBM)
    operands = [
        sub_offsets.T, facet_offsets.T, counts, facet_rows, aterm, cells, observed,
        weights.transpose(0, 2, 1, 3), *consts,
    ]
    dma = pltpu.SemaphoreType.DMA
    vmem = pltpu.VMEM
    return pl.pallas_call(
        functools.partial(body, dims),
        out_shape=pltpu.VMEM((1, 2, rdev, length // nb), F32),
        in_specs=[hbm] * 10,
        out_specs=pl.BlockSpec(memory_space=pltpu.VMEM),
        scratch_shapes=[
            *[pltpu.SMEM(v.shape, v.dtype) for v in operands[:3]],
            vmem(facet_rows.shape, BF),
            vmem((size, size), BF),
            vmem((2, slots), jnp.int32),
            vmem((2, slots), BF),
            *[vmem(v.shape, v.dtype) for v in operands[7:]],
            vmem((nf, rdev, 2 * M), BF),
            vmem((n, rdev, 2 * M), BF),
            vmem((8, slots), BF),
            vmem((nt, 8, slots), BF),
            vmem((nf, rdev, 2 * M), BF),
            vmem((nb, nf, rdev, 2 * M), BF),
            vmem((nf, 2, tiles, M), F32),
            vmem((nb, nf, 2, tiles // nb, M), F32),
            vmem((nf, 2 * M, 2 * LANES), BF),
            vmem((nf, 2 * M, 2 * LANES), BF),
            vmem((2, size // FINE, slots), F32),
            vmem((nt, size, slots), BF),
            vmem((nt, 2, size, slots), BF),
            vmem((nt, size, slots), F32),
            vmem((nt, size, slots), F32),
            dma, dma, dma((nt,)), dma((3,)), dma((5,)), pltpu.SemaphoreType.REGULAR((max(nt - 1, 1),)),
        ],
        compiler_params=pltpu.CompilerParams(
            collective_id=0, has_side_effects=True
        ),
    )(*operands)


def solution(mesh):
    placed = (
        P("facet", None, "team", None),
        P(),
        P(),
        P("facet", None, None, None),
        P("facet", None, "team", None, None),
        P("facet", None, "team", None, None),
        P("facet", None, "team", None),
        P(),
    )
    return jax.shard_map(
        local,
        mesh=mesh,
        in_specs=placed,
        out_specs=P("facet", None, "team", "sub"),
        check_vma=False,
    )
```

```python
import functools
import math

import jax
import jax.numpy as jnp
import ml_dtypes
import numpy as np
from jax import lax
from jax.experimental import pallas as pl
from jax.experimental.pallas import tpu as pltpu
from jax.sharding import PartitionSpec as P

M = 128
LANES = 128
FINE = 16
HALF_BITS = 5
PIECES = 2
TWO_PI = 2.0 * math.pi
BF = jnp.bfloat16
F32 = jnp.float32
MESH = pl.DeviceIdType.MESH


def sincos(turns, period):
    shift = period.bit_length() - 3
    quad = (turns + (1 << (shift - 1))) >> shift
    t = (turns - (quad << shift)).astype(F32) * (TWO_PI / period)
    t2 = t * t
    s = t * (1.0 + t2 * (-1.0 / 6 + t2 * (1.0 / 120 + t2 * (-1.0 / 5040))))
    c = 1.0 + t2 * (-0.5 + t2 * (1.0 / 24 + t2 * (-1.0 / 720 + t2 * (1.0 / 40320))))
    odd = (quad & 1) != 0
    cos = jnp.where(odd, s, c)
    sin = jnp.where(odd, c, s)
    cos = jnp.where(((quad + 1) & 2) != 0, -cos, cos)
    sin = jnp.where((quad & 2) != 0, -sin, sin)
    return cos, sin


def mm(left, right):
    return jnp.dot(left, right, preferred_element_type=F32)


def mm_nt(left, right):
    return lax.dot_general(left, right, (((1,), (1,)), ((), ())), preferred_element_type=F32)


def cat(parts, axis):
    return jnp.concatenate(parts, axis)


def iota(shape, dim):
    return lax.broadcasted_iota(jnp.int32, shape, dim)


def body(dims, *refs):
    (sub_hbm, fac_hbm, cnt_hbm, rows_hbm, aterm_hbm, cells_hbm, obs_hbm, wt_hbm, kk_hbm, kt_hbm) = refs[:10]
    out = refs[10]
    (
        sub_off, fac_off, counts, rows, aterm, cells, observed, weights, kk, kt,
        spec_out, got1, slot_out, got_x, fold_out, got2,
        tw1, tw2, wt_near, wt_far, coarse, middle, col_w, row_w, row_c, row_s,
        sent, recv1, recv_x, recv2, in_sem, ready,
    ) = refs[11:]
    nf, nt, nb, length, size, rdev = dims
    rall = rdev * nt
    n = nf * nt
    slots = cells.shape[-1]
    period = 4 * size
    tiles = length // LANES
    my_f = lax.axis_index("facet")
    my_t = lax.axis_index("team")
    my_b = lax.axis_index("sub")
    me = my_f * nt + my_t
    other = 1 - my_b

    fetches = [
        pltpu.make_async_copy(sub_hbm, sub_off, in_sem.at[0]),
        pltpu.make_async_copy(rows_hbm, rows, in_sem.at[1]),
        pltpu.make_async_copy(fac_hbm, fac_off, in_sem.at[4]),
        pltpu.make_async_copy(cnt_hbm, counts, in_sem.at[2]),
        pltpu.make_async_copy(cells_hbm.at[0, my_b, 0], cells, in_sem.at[2]),
        pltpu.make_async_copy(obs_hbm.at[0, my_b, 0], observed, in_sem.at[2]),
        pltpu.make_async_copy(wt_hbm, weights, in_sem.at[2]),
        pltpu.make_async_copy(kt_hbm, kt, in_sem.at[0]),
        pltpu.make_async_copy(kk_hbm, kk, in_sem.at[1]),
        pltpu.make_async_copy(aterm_hbm.at[0, my_b], aterm, in_sem.at[3]),
    ]
    fetches[0].start()
    fetches[2].start()
    piece = length // PIECES
    for c in range(2):
        for q in range(PIECES):
            lanes = pl.ds(q * piece, piece)
            pltpu.make_async_copy(
                rows_hbm.at[0, c, :, lanes], rows.at[0, c, :, lanes], in_sem.at[1]
            ).start()
    for fetch in fetches[3:7]:
        fetch.start()

    barrier = pltpu.get_barrier_semaphore()
    nc = 2 - nf % 2
    ny = nf // nc
    rows_far = [(y + ny // 2) % ny for y in range(ny)]
    order = [y * nc + c for c in range(nc) for y in rows_far]
    first = order[:ny]
    second = order[ny:]
    local_k = list(range(nc))
    urgent = [k for k in order if k >= nc]
    my_c = lax.rem(my_f, nc)

    def facet_at(k):
        return lax.rem(my_f // nc + k // nc, ny) * nc + k % nc

    def greet(k, t, b):
        pl.semaphore_signal(
            barrier, inc=1, device_id={"facet": facet_at(k), "team": t, "sub": b}, device_id_type=MESH
        )

    def unless_self(k, act):
        if k < nc:
            pl.when(my_c != k)(act)
        else:
            act()

    def greet_team(t):
        for k in order:
            greet(k, t, my_b)

    for t in reversed(range(1, nt)):
        pl.when(my_t < t)(functools.partial(greet_team, t))
    pl.semaphore_signal(
        barrier, inc=1, device_id={"facet": my_f, "team": my_t, "sub": other}, device_id_type=MESH
    )
    for k in order:
        unless_self(k, functools.partial(greet, k, my_t, my_b))

    base_c, base_s = sincos(iota((M, LANES), 0) * iota((M, LANES), 1), length)
    lane_row = iota((1, LANES), 1)

    fetches[0].wait()
    fetches[2].wait()

    def column_weights(shift_v):
        pc, ps = sincos(lane_row * shift_v, length)
        c = (base_c * pc - base_s * ps).astype(BF)
        s = (base_s * pc + base_c * ps).astype(BF)
        return cat([cat([c, s], 1), cat([-s, c], 1)], 0)

    scale = 1.0 / math.sqrt(length)

    def prepare(k):
        shift_v = sub_off[1, facet_at(k) * nb + my_b]
        wt_near[k] = column_weights(shift_v)
        m_no = iota((tiles, M), 1)
        turns = iota((tiles, M), 0) * LANES * (m_no + shift_v) - m_no * fac_off[1, my_f]
        c, s = sincos(turns, length)
        tw1[k, 0] = c * scale
        tw1[k, 1] = s * scale

    for k in first:
        prepare(k)
    fetches[1].wait()
    for fetch in fetches[7:]:
        fetch.start()
    x = [
        cat([rows[0, c, :, k * LANES : (k + 1) * LANES].astype(F32) for k in range(tiles)], 0)
        for c in range(2)
    ]
    x = cat(x, 1).astype(BF)

    def spectrum(k):
        y = mm_nt(x, wt_near[k])
        acc = [None] * 4
        for j in range(tiles):
            yr = y[j * rdev : (j + 1) * rdev, :M]
            yi = y[j * rdev : (j + 1) * rdev, M:]
            c = tw1[k, 0, j : j + 1, :]
            s = tw1[k, 1, j : j + 1, :]
            q = 2 * (j % 2)
            add_re = yr * c + yi * s
            add_im = yi * c - yr * s
            acc[q] = add_re if acc[q] is None else acc[q] + add_re
            acc[q + 1] = add_im if acc[q + 1] is None else acc[q + 1] + add_im
        spec_out[k] = cat([acc[0] + acc[2], acc[1] + acc[3]], 1).astype(BF)

    for k in first:
        spectrum(k)
    for i in (3, 4, 5, 6):
        fetches[i].wait()
    live = iota((1, slots), 1) < counts[my_f, my_b, my_t]
    all_wt = weights[0, 0].astype(F32)
    own_wt = jnp.where(my_b == 0, all_wt[0:1, :], all_wt[1:2, :])
    own_wt = jnp.where(live, own_wt, 0.0)
    place = cells[...]
    packed = cat(
        [
            (place >> HALF_BITS).astype(F32), (place & ((1 << HALF_BITS) - 1)).astype(F32),
            observed[...].astype(F32), own_wt, own_wt,
        ],
        0,
    ).astype(BF)
    slot_out[...] = packed
    got_x[my_t] = packed

    pl.semaphore_wait(barrier, nf * (my_t + 1))

    def report(t):
        for k in order:
            pl.semaphore_signal(
                ready.at[my_t - 1], inc=1,
                device_id={"facet": facet_at(k), "team": t, "sub": my_b}, device_id_type=MESH,
            )


    def copy_x(t):
        return pltpu.make_async_remote_copy(
            src_ref=slot_out,
            dst_ref=got_x.at[my_t],
            send_sem=sent,
            recv_sem=recv_x.at[my_t],
            device_id={"facet": my_f, "team": t, "sub": my_b},
            device_id_type=MESH,
        )

    def copy1(k, t):
        return pltpu.make_async_remote_copy(
            src_ref=spec_out.at[k],
            dst_ref=got1.at[me],
            send_sem=sent,
            recv_sem=recv1,
            device_id={"facet": facet_at(k), "team": t, "sub": my_b},
            device_id_type=MESH,
        )

    def send_specs(ks, t):
        for k in ks:
            if k >= nc:
                copy1(k, t).start()
            else:
                there = jnp.logical_or(my_t != t, my_c != k)
                pl.when(there)(lambda: copy1(k, t).start())

    def send_slots(t):
        pl.when(my_t != t)(lambda: copy_x(t).start())

    send_specs(first, 0)
    send_slots(0)
    for t in range(nt - 1):
        pl.when(my_t > t)(functools.partial(report, t))
    for k in second:
        prepare(k)
        spectrum(k)
    send_specs(second, 0)
    got1[me] = spec_out[my_c]

    for i in (7, 8, 9):
        fetches[i].wait()
    mirror = size // 2
    shift_u = sub_off[0, my_f * nb + my_b]
    step = length // rall
    scale_g = 1.0 / math.sqrt(rall * nf)
    lane = iota((1, n * rdev), 1)
    col_a = jnp.zeros((1, n * rdev), jnp.int32)
    row2 = iota((nf * rdev, 1), 0)
    row_a = jnp.zeros((nf * rdev, 1), jnp.int32)
    for f in range(nf):
        col_a = jnp.where(lane // rall == f, fac_off[0, f], col_a)
        row_a = jnp.where(row2 // rdev == f, fac_off[0, f], row_a)
    p0 = iota((M, n * rdev), 0)
    gc, gs = sincos(p0 * col_a - (p0 + shift_u) * (lane % rall * step), length)
    gc = (gc * scale_g).astype(BF)
    gs = (gs * scale_g).astype(BF)
    a_mat = mm(kt[...], cat([cat([gc, gs], 1), cat([-gs, gc], 1)], 0)).astype(BF)
    p1 = iota((nf * rdev, M), 1)
    hc, hs = sincos(p1 * row_a - (p1 + shift_u) * ((row2 % rdev + my_t * rdev) * step), length)
    hc = (hc * scale_g).astype(BF)
    hs = (hs * scale_g).astype(BF)
    at = mm_nt(cat([cat([hc, -hs], 1), cat([hs, hc], 1)], 0), kt[...])
    ah = cat([at[: nf * rdev], -at[nf * rdev :]], 1).astype(BF)

    for t in range(1, nt):
        pl.when(my_t < t)(lambda: pl.semaphore_wait(ready.at[t - 1], nf))
        send_slots(t)
        send_specs(order, t)
    flip = (iota((mirror, mirror), 0) + iota((mirror, mirror), 1) == mirror - 1).astype(F32).astype(BF)
    low = mm(flip, aterm[:mirror, :])
    both = cat([aterm[mirror:, :].astype(F32), low], 0)
    amap = cat([both[:, mirror:], mm(both[:, :mirror].astype(BF), flip)], 1)
    amap = cat([amap, amap], 1)
    half = tiles // nb
    scale_b = 1.0 / (math.sqrt(M) * size)
    tile_no = iota((half, M), 0) + my_b * half
    for far in range(2):
        for a in range(nf):
            shift_v = sub_off[1, facet_at(a) * nb + (other if far else my_b)]
            if far:
                wt_far[a] = column_weights(shift_v)
            m_no = iota((half, M), 1)
            c, s = sincos((m_no + shift_v) * (tile_no * LANES) - m_no * fac_off[1, my_f], length)
            tw2[far, a, 0] = c * scale_b
            tw2[far, a, 1] = s * scale_b

    fine_no = iota((FINE, slots), 0)
    col_no = iota((mirror // FINE, slots), 0)
    for k in range(nt):
        src = lax.rem(my_t + k, nt)
        if k:
            pltpu.make_async_copy(got_x.at[src], got_x.at[src], recv_x.at[src]).wait()
        pos = got_x[src].astype(F32)[0:4, :].astype(jnp.int32)
        pos = (pos[0:2, :] << HALF_BITS) + pos[2:4, :]
        pos_x = pos[0:1, :]
        pos_y = pos[1:2, :]
        mid_c, mid_s = sincos((size - 1) * (pos_x + pos_y), 2 * period)
        middle[k, 0:1, :] = mid_c
        middle[k, 1:2, :] = mid_s
        for axis, place in enumerate((pos_x, pos_y)):
            lo_c, lo_s = sincos((2 * fine_no + 1) * place, 2 * period)
            hi_c, hi_s = sincos(2 * FINE * col_no * place, 2 * period)
            coarse[0] = hi_c
            coarse[1] = hi_s
            for q in range(mirror // FINE):
                c1 = coarse[0, q : q + 1, :]
                s1 = coarse[1, q : q + 1, :]
                c = c1 * lo_c - s1 * lo_s
                s = s1 * lo_c + c1 * lo_s
                rng = slice(q * FINE, (q + 1) * FINE)
                low = slice(mirror + q * FINE, mirror + (q + 1) * FINE)
                if axis == 0:
                    row_c[k, rng, :] = c
                    row_s[k, rng, :] = s
                    row_w[k, rng, :] = c.astype(BF)
                    row_w[k, low, :] = s.astype(BF)
                else:
                    col_w[k, rng, :] = c.astype(BF)
                    col_w[k, low, :] = s.astype(BF)
    done = got1.at[pl.ds(0, n - 1)]
    pltpu.make_async_copy(done, done, recv1).wait()
    got = got1[...].astype(F32).reshape(n * rdev, 2 * M)
    got = cat([got, cat([-got[:, M:], got[:, :M]], 1)], 0).astype(BF)
    full = mm(a_mat, got)
    image = mm(full.astype(BF), kk[...])
    image = amap * image
    re_p, re_n, im_p, im_n = (image[:, c * mirror : (c + 1) * mirror] for c in range(4))
    folded = cat(
        [cat([re_p + re_n, im_p - im_n], 1), cat([im_p + im_n, re_n - re_p], 1)], 0
    )
    a, b, c, d = (folded[q * mirror : (q + 1) * mirror] for q in range(4))
    folded = cat([a + b, a - b, c + d, c - d], 0).astype(BF)
    def degrid(k):
        src = lax.rem(my_t + k, nt)
        z = mm(folded, col_w[k])
        re_e, re_o, im_e, im_o = (z[q * mirror : (q + 1) * mirror] for q in range(4))
        rc = row_c[k]
        rs = row_s[k]
        mid_c = middle[k, 0:1, :]
        mid_s = middle[k, 1:2, :]
        sum_re = jnp.sum(rc * re_e + rs * im_o, 0, keepdims=True) * (1.0 / size)
        sum_im = jnp.sum(rc * im_e - rs * re_o, 0, keepdims=True) * (1.0 / size)
        pred_re = sum_re * mid_c + sum_im * mid_s
        pred_im = sum_im * mid_c - sum_re * mid_s
        info = got_x[src].astype(F32)
        res_re = info[6:7, :] * (info[4:5, :] - pred_re)
        res_im = info[6:7, :] * (info[5:6, :] - pred_im)
        turn_re = res_re * mid_c - res_im * mid_s
        turn_im = res_re * mid_s + res_im * mid_c
        turn_re = jnp.broadcast_to(turn_re.astype(BF), (size, slots))
        turn_im = jnp.broadcast_to(turn_im.astype(BF), (size, slots))
        rows_w = row_w[k]
        return cat([rows_w * turn_re, rows_w * turn_im], 0)

    left = [None] * nt
    prod = None
    for k in range(nt + 1):
        if k < nt:
            left[k] = degrid(k)
        if k:
            part = mm_nt(left[k - 1], col_w[k - 1])
            prod = part if prod is None else prod + part
    a, c, b, d = (prod[q * mirror : (q + 1) * mirror] for q in range(4))
    real = cat([a - d, a + d], 0)
    imag = cat([b + c, b - c], 0)
    cr, sr = real[:, :mirror], real[:, mirror:]
    ci, si = imag[:, :mirror], imag[:, mirror:]
    grid = cat([cr - si, cr + si, ci + sr, ci - sr], 1)
    v = (amap * grid).astype(BF)
    u = mm_nt(v, kk[...]).astype(BF)
    ur = u[:, :M]
    ui = u[:, M:]
    part = mm(ah, cat([u, cat([-ui, ur], 1)], 0))
    fold_out[...] = part.reshape(nf, rdev, 2 * M).astype(BF)


    def copy2(k, far):
        return pltpu.make_async_remote_copy(
            src_ref=fold_out.at[facet_at(k)],
            dst_ref=got2.at[far, my_f],
            send_sem=sent,
            recv_sem=recv2.at[min(k // nc, 1) + far],
            device_id={"facet": facet_at(k), "team": my_t, "sub": other if far else my_b},
            device_id_type=MESH,
        )

    for k in order:
        copy2(k, 1).start()
    for k in order:
        unless_self(k, lambda: copy2(k, 0).start())
    got2[0, my_f] = fold_out[my_f]

    def update(total, far, ks):
        for k in ks:
            g = got2[far, facet_at(k)].astype(F32)
            gr = g[:, :M]
            gi = g[:, M:]
            parts = []
            for j in range(half):
                c = tw2[far, k, 0, j : j + 1, :]
                s = tw2[far, k, 1, j : j + 1, :]
                parts.append(cat([gr * c - gi * s, gr * s + gi * c], 1))
            y = mm(cat(parts, 0).astype(BF), (wt_far if far else wt_near)[k])
            total = y if total is None else total + y
        return total

    def arrived(which, count):
        done = got1.at[pl.ds(0, count)]
        pltpu.make_async_copy(done, done, recv2.at[which]).wait()

    if nc > 1:
        arrived(0, nc - 1)
    total = update(None, 0, local_k)
    arrived(1, nf)
    total = update(total, 1, local_k)
    total = update(total, 0, urgent)
    if ny > 1:
        arrived(2, nf - nc)
    total = update(total, 1, urgent)
    for k in range(half):
        rng = slice(k * rdev, (k + 1) * rdev)
        lanes = slice(k * LANES, (k + 1) * LANES)
        out[0, 0, :, lanes] = total[rng, :LANES]
        out[0, 1, :, lanes] = total[rng, LANES:]
    for count in (n - 1, nt - 1, 2 * nf - 1):
        gone = got1.at[pl.ds(0, count)]
        pltpu.make_async_copy(gone, gone, sent).wait()


def tables(size):
    angle = (np.arange(M)[:, None] * np.arange(size)[None, :] % size) * (TWO_PI / size)
    kc = np.cos(angle) / math.sqrt(M)
    ks = np.sin(angle) / math.sqrt(M)
    half = size // 2
    order = np.concatenate([np.arange(half, size), np.arange(half - 1, -1, -1)])
    kc, ks = kc[:, order], ks[:, order]
    kt = np.concatenate([kc.T, ks.T], 1)
    kk = np.block([[kc, ks], [-ks, kc]])
    return [np.asarray(v, np.float32).astype(ml_dtypes.bfloat16) for v in (kk, kt)]


def local(facet_rows, sub_offsets, facet_offsets, aterm, cells, observed, weights, counts):
    nf = lax.axis_size("facet")
    nt = lax.axis_size("team")
    nb = lax.axis_size("sub")
    rdev, length = facet_rows.shape[2:]
    size = aterm.shape[-1]
    slots = cells.shape[-1]
    n = nf * nt
    tiles = length // LANES
    dims = (nf, nt, nb, length, size, rdev)
    consts = [jnp.asarray(v) for v in tables(size)]
    hbm = pl.BlockSpec(memory_space=pltpu.HBM)
    operands = [
        sub_offsets.T, facet_offsets.T, counts, facet_rows, aterm, cells, observed,
        weights.transpose(0, 2, 1, 3), *consts,
    ]
    dma = pltpu.SemaphoreType.DMA
    vmem = pltpu.VMEM
    return pl.pallas_call(
        functools.partial(body, dims),
        out_shape=pltpu.VMEM((1, 2, rdev, length // nb), F32),
        in_specs=[hbm] * 10,
        out_specs=pl.BlockSpec(memory_space=pltpu.VMEM),
        scratch_shapes=[
            *[pltpu.SMEM(v.shape, v.dtype) for v in operands[:3]],
            vmem(facet_rows.shape, BF),
            vmem((size, size), BF),
            vmem((2, slots), jnp.int32),
            vmem((2, slots), BF),
            *[vmem(v.shape, v.dtype) for v in operands[7:]],
            vmem((nf, rdev, 2 * M), BF),
            vmem((n, rdev, 2 * M), BF),
            vmem((8, slots), BF),
            vmem((nt, 8, slots), BF),
            vmem((nf, rdev, 2 * M), BF),
            vmem((nb, nf, rdev, 2 * M), BF),
            vmem((nf, 2, tiles, M), F32),
            vmem((nb, nf, 2, tiles // nb, M), F32),
            vmem((nf, 2 * M, 2 * LANES), BF),
            vmem((nf, 2 * M, 2 * LANES), BF),
            vmem((2, size // 2 // FINE, slots), F32),
            vmem((nt, 8, slots), F32),
            vmem((nt, size, slots), BF),
            vmem((nt, size, slots), BF),
            vmem((nt, size // 2, slots), F32),
            vmem((nt, size // 2, slots), F32),
            dma, dma, dma((nt,)), dma((3,)), dma((5,)), pltpu.SemaphoreType.REGULAR((max(nt - 1, 1),)),
        ],
        compiler_params=pltpu.CompilerParams(
            collective_id=0, has_side_effects=True
        ),
    )(*operands)


def solution(mesh):
    placed = (
        P("facet", None, "team", None),
        P(),
        P(),
        P("facet", None, None, None),
        P("facet", None, "team", None, None),
        P("facet", None, "team", None, None),
        P("facet", None, "team", None),
        P(),
    )
    return jax.shard_map(
        local,
        mesh=mesh,
        in_specs=placed,
        out_specs=P("facet", None, "team", "sub"),
        check_vma=False,
    )
```

```python
import functools
import math

import jax
import jax.numpy as jnp
import ml_dtypes
import numpy as np
from jax import lax
from jax.experimental import pallas as pl
from jax.experimental.pallas import tpu as pltpu
from jax.sharding import PartitionSpec as P

M = 128
LANES = 128
FINE = 16
HALF_BITS = 5
PIECES = 2
TWO_PI = 2.0 * math.pi
BF = jnp.bfloat16
F32 = jnp.float32
MESH = pl.DeviceIdType.MESH


def sincos(turns, period):
    shift = period.bit_length() - 3
    quad = (turns + (1 << (shift - 1))) >> shift
    t = (turns - (quad << shift)).astype(F32) * (TWO_PI / period)
    t2 = t * t
    s = t * (1.0 + t2 * (-1.0 / 6 + t2 * (1.0 / 120 + t2 * (-1.0 / 5040))))
    c = 1.0 + t2 * (-0.5 + t2 * (1.0 / 24 + t2 * (-1.0 / 720 + t2 * (1.0 / 40320))))
    odd = (quad & 1) != 0
    cos = jnp.where(odd, s, c)
    sin = jnp.where(odd, c, s)
    cos = jnp.where(((quad + 1) & 2) != 0, -cos, cos)
    sin = jnp.where((quad & 2) != 0, -sin, sin)
    return cos, sin


def mm(left, right):
    return jnp.dot(left, right, preferred_element_type=F32)


def mm_nt(left, right):
    return lax.dot_general(left, right, (((1,), (1,)), ((), ())), preferred_element_type=F32)


def cat(parts, axis):
    return jnp.concatenate(parts, axis)


def iota(shape, dim):
    return lax.broadcasted_iota(jnp.int32, shape, dim)


def body(dims, *refs):
    (sub_hbm, fac_hbm, cnt_hbm, rows_hbm, aterm_hbm, cells_hbm, obs_hbm, wt_hbm, kk_hbm, kt_hbm) = refs[:10]
    out = refs[10]
    (
        sub_off, fac_off, counts, rows, aterm, cells, observed, weights, kk, kt,
        spec_out, got1, slot_out, got_x, fold_out, got2,
        tw1, tw2, wt_near, wt_far, coarse, middle, col_w, row_w, row_c, row_s,
        sent, recv1, recv_x, recv2, in_sem, ready,
    ) = refs[11:]
    nf, nt, nb, length, size, rdev = dims
    rall = rdev * nt
    n = nf * nt
    slots = cells.shape[-1]
    period = 4 * size
    tiles = length // LANES
    my_f = lax.axis_index("facet")
    my_t = lax.axis_index("team")
    my_b = lax.axis_index("sub")
    me = my_f * nt + my_t
    other = 1 - my_b

    fetches = [
        pltpu.make_async_copy(sub_hbm, sub_off, in_sem.at[0]),
        pltpu.make_async_copy(rows_hbm, rows, in_sem.at[1]),
        pltpu.make_async_copy(fac_hbm, fac_off, in_sem.at[0]),
        pltpu.make_async_copy(cnt_hbm, counts, in_sem.at[2]),
        pltpu.make_async_copy(cells_hbm.at[0, my_b, 0], cells, in_sem.at[2]),
        pltpu.make_async_copy(obs_hbm.at[0, my_b, 0], observed, in_sem.at[2]),
        pltpu.make_async_copy(wt_hbm, weights, in_sem.at[2]),
        pltpu.make_async_copy(kt_hbm, kt, in_sem.at[0]),
        pltpu.make_async_copy(kk_hbm, kk, in_sem.at[0]),
        pltpu.make_async_copy(aterm_hbm.at[0, my_b], aterm, in_sem.at[0]),
    ]
    fetches[0].start()
    fetches[2].start()
    piece = length // PIECES
    for c in range(2):
        for q in range(PIECES):
            lanes = pl.ds(q * piece, piece)
            pltpu.make_async_copy(
                rows_hbm.at[0, c, :, lanes], rows.at[0, c, :, lanes], in_sem.at[1]
            ).start()
    for fetch in fetches[3:7]:
        fetch.start()

    barrier = pltpu.get_barrier_semaphore()
    nc = 2 - nf % 2
    ny = nf // nc
    rows_far = [(y + ny // 2) % ny for y in range(ny)]
    order = [y * nc + c for c in range(nc) for y in rows_far]
    first = order[:ny]
    second = order[ny:]
    local_k = list(range(nc))
    urgent = [k for k in order if k >= nc]
    my_c = lax.rem(my_f, nc)

    def facet_at(k):
        return lax.rem(my_f // nc + k // nc, ny) * nc + k % nc

    def greet(k, t, b):
        pl.semaphore_signal(
            barrier, inc=1, device_id={"facet": facet_at(k), "team": t, "sub": b}, device_id_type=MESH
        )

    def unless_self(k, act):
        if k < nc:
            pl.when(my_c != k)(act)
        else:
            act()

    def greet_team(t):
        for k in order:
            greet(k, t, my_b)

    for t in reversed(range(1, nt)):
        pl.when(my_t < t)(functools.partial(greet_team, t))
    pl.semaphore_signal(
        barrier, inc=1, device_id={"facet": my_f, "team": my_t, "sub": other}, device_id_type=MESH
    )
    for k in order:
        unless_self(k, functools.partial(greet, k, my_t, my_b))

    base_c, base_s = sincos(iota((M, LANES), 0) * iota((M, LANES), 1), length)
    lane_row = iota((1, LANES), 1)

    fetches[0].wait()
    fetches[2].wait()

    def column_weights(shift_v):
        pc, ps = sincos(lane_row * shift_v, length)
        c = (base_c * pc - base_s * ps).astype(BF)
        s = (base_s * pc + base_c * ps).astype(BF)
        return cat([cat([c, s], 1), cat([-s, c], 1)], 0)

    scale = 1.0 / math.sqrt(length)

    def prepare(k):
        shift_v = sub_off[1, facet_at(k) * nb + my_b]
        wt_near[k] = column_weights(shift_v)
        m_no = iota((tiles, M), 1)
        turns = iota((tiles, M), 0) * LANES * (m_no + shift_v) - m_no * fac_off[1, my_f]
        c, s = sincos(turns, length)
        tw1[k, 0] = c * scale
        tw1[k, 1] = s * scale

    for k in first:
        prepare(k)
    fetches[1].wait()
    for fetch in fetches[7:]:
        fetch.start()
    x = [
        cat([rows[0, c, :, k * LANES : (k + 1) * LANES].astype(F32) for k in range(tiles)], 0)
        for c in range(2)
    ]
    x = cat(x, 1).astype(BF)

    def spectrum(k):
        y = mm_nt(x, wt_near[k])
        acc = [None] * 4
        for j in range(tiles):
            yr = y[j * rdev : (j + 1) * rdev, :M]
            yi = y[j * rdev : (j + 1) * rdev, M:]
            c = tw1[k, 0, j : j + 1, :]
            s = tw1[k, 1, j : j + 1, :]
            q = 2 * (j % 2)
            add_re = yr * c + yi * s
            add_im = yi * c - yr * s
            acc[q] = add_re if acc[q] is None else acc[q] + add_re
            acc[q + 1] = add_im if acc[q + 1] is None else acc[q + 1] + add_im
        spec_out[k] = cat([acc[0] + acc[2], acc[1] + acc[3]], 1).astype(BF)

    for k in first:
        spectrum(k)
    for i in (3, 4, 5, 6):
        fetches[i].wait()
    live = iota((1, slots), 1) < counts[my_f, my_b, my_t]
    all_wt = weights[0, 0].astype(F32)
    own_wt = jnp.where(my_b == 0, all_wt[0:1, :], all_wt[1:2, :])
    own_wt = jnp.where(live, own_wt, 0.0)
    place = cells[...]
    packed = cat(
        [
            (place >> HALF_BITS).astype(F32), (place & ((1 << HALF_BITS) - 1)).astype(F32),
            observed[...].astype(F32), own_wt, own_wt,
        ],
        0,
    ).astype(BF)
    slot_out[...] = packed
    got_x[my_t] = packed

    pl.semaphore_wait(barrier, nf * (my_t + 1))

    def report(t):
        for k in order:
            pl.semaphore_signal(
                ready.at[my_t - 1], inc=1,
                device_id={"facet": facet_at(k), "team": t, "sub": my_b}, device_id_type=MESH,
            )


    def copy_x(t):
        return pltpu.make_async_remote_copy(
            src_ref=slot_out,
            dst_ref=got_x.at[my_t],
            send_sem=sent,
            recv_sem=recv_x.at[my_t],
            device_id={"facet": my_f, "team": t, "sub": my_b},
            device_id_type=MESH,
        )

    def copy1(k, t):
        return pltpu.make_async_remote_copy(
            src_ref=spec_out.at[k],
            dst_ref=got1.at[me],
            send_sem=sent,
            recv_sem=recv1,
            device_id={"facet": facet_at(k), "team": t, "sub": my_b},
            device_id_type=MESH,
        )

    def send_specs(ks, t):
        for k in ks:
            if k >= nc:
                copy1(k, t).start()
            else:
                there = jnp.logical_or(my_t != t, my_c != k)
                pl.when(there)(lambda: copy1(k, t).start())

    def send_slots(t):
        pl.when(my_t != t)(lambda: copy_x(t).start())

    send_specs(first, 0)
    send_slots(0)
    for t in range(nt - 1):
        pl.when(my_t > t)(functools.partial(report, t))
    for k in second:
        prepare(k)
        spectrum(k)
    send_specs(second, 0)
    got1[me] = spec_out[my_c]

    for i in (7, 8, 9):
        fetches[i].wait()
    mirror = size // 2
    shift_u = sub_off[0, my_f * nb + my_b]
    step = length // rall
    scale_g = 1.0 / math.sqrt(rall * nf)
    lane = iota((1, n * rdev), 1)
    col_a = jnp.zeros((1, n * rdev), jnp.int32)
    row2 = iota((nf * rdev, 1), 0)
    row_a = jnp.zeros((nf * rdev, 1), jnp.int32)
    for f in range(nf):
        col_a = jnp.where(lane // rall == f, fac_off[0, f], col_a)
        row_a = jnp.where(row2 // rdev == f, fac_off[0, f], row_a)
    p0 = iota((M, n * rdev), 0)
    gc, gs = sincos(p0 * col_a - (p0 + shift_u) * (lane % rall * step), length)
    gc = (gc * scale_g).astype(BF)
    gs = (gs * scale_g).astype(BF)
    a_mat = mm(kt[...], cat([cat([gc, gs], 1), cat([-gs, gc], 1)], 0)).astype(BF)
    p1 = iota((nf * rdev, M), 1)
    hc, hs = sincos(p1 * row_a - (p1 + shift_u) * ((row2 % rdev + my_t * rdev) * step), length)
    hc = (hc * scale_g).astype(BF)
    hs = (hs * scale_g).astype(BF)
    at = mm_nt(cat([cat([hc, -hs], 1), cat([hs, hc], 1)], 0), kt[...])
    ah = cat([at[: nf * rdev], -at[nf * rdev :]], 1).astype(BF)

    for t in range(1, nt):
        pl.when(my_t < t)(lambda: pl.semaphore_wait(ready.at[t - 1], nf))
        send_slots(t)
        send_specs(order, t)
    flip = (iota((mirror, mirror), 0) + iota((mirror, mirror), 1) == mirror - 1).astype(F32).astype(BF)
    low = mm(flip, aterm[:mirror, :])
    both = cat([aterm[mirror:, :].astype(F32), low], 0)
    amap = cat([both[:, mirror:], mm(both[:, :mirror].astype(BF), flip)], 1)
    amap = cat([amap, amap], 1)
    half = tiles // nb
    scale_b = 1.0 / (math.sqrt(M) * size)
    tile_no = iota((half, M), 0) + my_b * half
    for far in range(2):
        for a in range(nf):
            shift_v = sub_off[1, facet_at(a) * nb + (other if far else my_b)]
            if far:
                wt_far[a] = column_weights(shift_v)
            m_no = iota((half, M), 1)
            c, s = sincos((m_no + shift_v) * (tile_no * LANES) - m_no * fac_off[1, my_f], length)
            tw2[far, a, 0] = c * scale_b
            tw2[far, a, 1] = s * scale_b

    fine_no = iota((FINE, slots), 0)
    col_no = iota((mirror // FINE, slots), 0)
    for k in range(nt):
        src = lax.rem(my_t + k, nt)
        if k:
            pltpu.make_async_copy(got_x.at[src], got_x.at[src], recv_x.at[src]).wait()
        pos = got_x[src].astype(F32)[0:4, :].astype(jnp.int32)
        pos = (pos[0:2, :] << HALF_BITS) + pos[2:4, :]
        pos_x = pos[0:1, :]
        pos_y = pos[1:2, :]
        mid_c, mid_s = sincos((size - 1) * (pos_x + pos_y), 2 * period)
        middle[k, 0:1, :] = mid_c
        middle[k, 1:2, :] = mid_s
        for axis, place in enumerate((pos_x, pos_y)):
            lo_c, lo_s = sincos((2 * fine_no + 1) * place, 2 * period)
            hi_c, hi_s = sincos(2 * FINE * col_no * place, 2 * period)
            coarse[0] = hi_c
            coarse[1] = hi_s
            for q in range(mirror // FINE):
                c1 = coarse[0, q : q + 1, :]
                s1 = coarse[1, q : q + 1, :]
                c = c1 * lo_c - s1 * lo_s
                s = s1 * lo_c + c1 * lo_s
                rng = slice(q * FINE, (q + 1) * FINE)
                low = slice(mirror + q * FINE, mirror + (q + 1) * FINE)
                if axis == 0:
                    row_c[k, rng, :] = c
                    row_s[k, rng, :] = s
                    row_w[k, rng, :] = c.astype(BF)
                    row_w[k, low, :] = s.astype(BF)
                else:
                    col_w[k, rng, :] = c.astype(BF)
                    col_w[k, low, :] = s.astype(BF)
    done = got1.at[pl.ds(0, n - 1)]
    pltpu.make_async_copy(done, done, recv1).wait()
    got = got1[...].astype(F32).reshape(n * rdev, 2 * M)
    got = cat([got, cat([-got[:, M:], got[:, :M]], 1)], 0).astype(BF)
    full = mm(a_mat, got)
    image = mm(full.astype(BF), kk[...])
    image = amap * image
    re_p, re_n, im_p, im_n = (image[:, c * mirror : (c + 1) * mirror] for c in range(4))
    folded = cat(
        [cat([re_p + re_n, im_p - im_n], 1), cat([im_p + im_n, re_n - re_p], 1)], 0
    )
    a, b, c, d = (folded[q * mirror : (q + 1) * mirror] for q in range(4))
    folded = cat([a + b, a - b, c + d, c - d], 0).astype(BF)
    def degrid(k):
        src = lax.rem(my_t + k, nt)
        z = mm(folded, col_w[k])
        re_e, re_o, im_e, im_o = (z[q * mirror : (q + 1) * mirror] for q in range(4))
        rc = row_c[k]
        rs = row_s[k]
        mid_c = middle[k, 0:1, :]
        mid_s = middle[k, 1:2, :]
        sum_re = jnp.sum(rc * re_e + rs * im_o, 0, keepdims=True) * (1.0 / size)
        sum_im = jnp.sum(rc * im_e - rs * re_o, 0, keepdims=True) * (1.0 / size)
        pred_re = sum_re * mid_c + sum_im * mid_s
        pred_im = sum_im * mid_c - sum_re * mid_s
        info = got_x[src].astype(F32)
        res_re = info[6:7, :] * (info[4:5, :] - pred_re)
        res_im = info[6:7, :] * (info[5:6, :] - pred_im)
        turn_re = res_re * mid_c - res_im * mid_s
        turn_im = res_re * mid_s + res_im * mid_c
        turn_re = jnp.broadcast_to(turn_re.astype(BF), (size, slots))
        turn_im = jnp.broadcast_to(turn_im.astype(BF), (size, slots))
        rows_w = row_w[k]
        return cat([rows_w * turn_re, rows_w * turn_im], 0)

    left = [None] * nt
    prod = None
    for k in range(nt):
        left[k] = degrid(k)
    prod = mm_nt(cat(left, 1), cat([col_w[k] for k in range(nt)], 1))
    a, c, b, d = (prod[q * mirror : (q + 1) * mirror] for q in range(4))
    real = cat([a - d, a + d], 0)
    imag = cat([b + c, b - c], 0)
    cr, sr = real[:, :mirror], real[:, mirror:]
    ci, si = imag[:, :mirror], imag[:, mirror:]
    grid = cat([cr - si, cr + si, ci + sr, ci - sr], 1)
    v = (amap * grid).astype(BF)
    u = mm_nt(v, kk[...]).astype(BF)
    ur = u[:, :M]
    ui = u[:, M:]
    part = mm(ah, cat([u, cat([-ui, ur], 1)], 0))
    fold_out[...] = part.reshape(nf, rdev, 2 * M).astype(BF)


    def copy2(k, far):
        return pltpu.make_async_remote_copy(
            src_ref=fold_out.at[facet_at(k)],
            dst_ref=got2.at[far, my_f],
            send_sem=sent,
            recv_sem=recv2.at[min(k // nc, 1) + far],
            device_id={"facet": facet_at(k), "team": my_t, "sub": other if far else my_b},
            device_id_type=MESH,
        )

    for k in order:
        copy2(k, 1).start()
    for k in order:
        unless_self(k, lambda: copy2(k, 0).start())
    got2[0, my_f] = fold_out[my_f]

    def update(total, far, ks):
        for k in ks:
            g = got2[far, facet_at(k)].astype(F32)
            gr = g[:, :M]
            gi = g[:, M:]
            parts = []
            for j in range(half):
                c = tw2[far, k, 0, j : j + 1, :]
                s = tw2[far, k, 1, j : j + 1, :]
                parts.append(cat([gr * c - gi * s, gr * s + gi * c], 1))
            y = mm(cat(parts, 0).astype(BF), (wt_far if far else wt_near)[k])
            total = y if total is None else total + y
        return total

    def arrived(which, count):
        done = got1.at[pl.ds(0, count)]
        pltpu.make_async_copy(done, done, recv2.at[which]).wait()

    if nc > 1:
        arrived(0, nc - 1)
    total = update(None, 0, local_k)
    arrived(1, nf)
    total = update(total, 1, local_k)
    total = update(total, 0, urgent)
    if ny > 1:
        arrived(2, nf - nc)
    total = update(total, 1, urgent)
    for k in range(half):
        rng = slice(k * rdev, (k + 1) * rdev)
        lanes = slice(k * LANES, (k + 1) * LANES)
        out[0, 0, :, lanes] = total[rng, :LANES]
        out[0, 1, :, lanes] = total[rng, LANES:]
    for count in (n - 1, nt - 1, 2 * nf - 1):
        gone = got1.at[pl.ds(0, count)]
        pltpu.make_async_copy(gone, gone, sent).wait()


def tables(size):
    angle = (np.arange(M)[:, None] * np.arange(size)[None, :] % size) * (TWO_PI / size)
    kc = np.cos(angle) / math.sqrt(M)
    ks = np.sin(angle) / math.sqrt(M)
    half = size // 2
    order = np.concatenate([np.arange(half, size), np.arange(half - 1, -1, -1)])
    kc, ks = kc[:, order], ks[:, order]
    kt = np.concatenate([kc.T, ks.T], 1)
    kk = np.block([[kc, ks], [-ks, kc]])
    return [np.asarray(v, np.float32).astype(ml_dtypes.bfloat16) for v in (kk, kt)]


def local(facet_rows, sub_offsets, facet_offsets, aterm, cells, observed, weights, counts):
    nf = lax.axis_size("facet")
    nt = lax.axis_size("team")
    nb = lax.axis_size("sub")
    rdev, length = facet_rows.shape[2:]
    size = aterm.shape[-1]
    slots = cells.shape[-1]
    n = nf * nt
    tiles = length // LANES
    dims = (nf, nt, nb, length, size, rdev)
    consts = [jnp.asarray(v) for v in tables(size)]
    hbm = pl.BlockSpec(memory_space=pltpu.HBM)
    operands = [
        sub_offsets.T, facet_offsets.T, counts, facet_rows, aterm, cells, observed,
        weights.transpose(0, 2, 1, 3), *consts,
    ]
    dma = pltpu.SemaphoreType.DMA
    vmem = pltpu.VMEM
    return pl.pallas_call(
        functools.partial(body, dims),
        out_shape=pltpu.VMEM((1, 2, rdev, length // nb), F32),
        in_specs=[hbm] * 10,
        out_specs=pl.BlockSpec(memory_space=pltpu.VMEM),
        scratch_shapes=[
            *[pltpu.SMEM(v.shape, v.dtype) for v in operands[:3]],
            vmem(facet_rows.shape, BF),
            vmem((size, size), BF),
            vmem((2, slots), jnp.int32),
            vmem((2, slots), BF),
            *[vmem(v.shape, v.dtype) for v in operands[7:]],
            vmem((nf, rdev, 2 * M), BF),
            vmem((n, rdev, 2 * M), BF),
            vmem((8, slots), BF),
            vmem((nt, 8, slots), BF),
            vmem((nf, rdev, 2 * M), BF),
            vmem((nb, nf, rdev, 2 * M), BF),
            vmem((nf, 2, tiles, M), F32),
            vmem((nb, nf, 2, tiles // nb, M), F32),
            vmem((nf, 2 * M, 2 * LANES), BF),
            vmem((nf, 2 * M, 2 * LANES), BF),
            vmem((2, size // 2 // FINE, slots), F32),
            vmem((nt, 8, slots), F32),
            vmem((nt, size, slots), BF),
            vmem((nt, size, slots), BF),
            vmem((nt, size // 2, slots), F32),
            vmem((nt, size // 2, slots), F32),
            dma, dma, dma((nt,)), dma((3,)), dma((3,)), pltpu.SemaphoreType.REGULAR((max(nt - 1, 1),)),
        ],
        compiler_params=pltpu.CompilerParams(
            collective_id=0, has_side_effects=True
        ),
    )(*operands)


def solution(mesh):
    placed = (
        P("facet", None, "team", None),
        P(),
        P(),
        P("facet", None, None, None),
        P("facet", None, "team", None, None),
        P("facet", None, "team", None, None),
        P("facet", None, "team", None),
        P(),
    )
    return jax.shard_map(
        local,
        mesh=mesh,
        in_specs=placed,
        out_specs=P("facet", None, "team", "sub"),
        check_vma=False,
    )
```

```python
import functools
import math

import jax
import jax.numpy as jnp
import ml_dtypes
import numpy as np
from jax import lax
from jax.experimental import pallas as pl
from jax.experimental.pallas import tpu as pltpu
from jax.sharding import PartitionSpec as P

M = 128
LANES = 128
FINE = 16
HALF_BITS = 5
PIECES = 2
TWO_PI = 2.0 * math.pi
BF = jnp.bfloat16
F32 = jnp.float32
MESH = pl.DeviceIdType.MESH


def sincos(turns, period):
    shift = period.bit_length() - 3
    quad = (turns + (1 << (shift - 1))) >> shift
    t = (turns - (quad << shift)).astype(F32) * (TWO_PI / period)
    t2 = t * t
    s = t * (1.0 + t2 * (-1.0 / 6 + t2 * (1.0 / 120 + t2 * (-1.0 / 5040))))
    c = 1.0 + t2 * (-0.5 + t2 * (1.0 / 24 + t2 * (-1.0 / 720 + t2 * (1.0 / 40320))))
    odd = (quad & 1) != 0
    cos = jnp.where(odd, s, c)
    sin = jnp.where(odd, c, s)
    cos = jnp.where(((quad + 1) & 2) != 0, -cos, cos)
    sin = jnp.where((quad & 2) != 0, -sin, sin)
    return cos, sin


def mm(left, right):
    return jnp.dot(left, right, preferred_element_type=F32)


def mm_nt(left, right):
    return lax.dot_general(left, right, (((1,), (1,)), ((), ())), preferred_element_type=F32)


def cat(parts, axis):
    return jnp.concatenate(parts, axis)


def iota(shape, dim):
    return lax.broadcasted_iota(jnp.int32, shape, dim)


def body(dims, *refs):
    (sub_hbm, fac_hbm, cnt_hbm, rows_hbm, aterm_hbm, cells_hbm, obs_hbm, wt_hbm, kk_hbm, kt_hbm) = refs[:10]
    out = refs[10]
    (
        sub_off, fac_off, counts, rows, aterm, cells, observed, weights, kk, kt,
        spec_out, got1, slot_out, got_x, fold_out, got2,
        tw1, tw2, wt_near, wt_far, coarse, middle, col_w, row_w, row_c, row_s,
        sent, recv1, recv_x, recv2, in_sem, ready,
    ) = refs[11:]
    nf, nt, nb, length, size, rdev = dims
    rall = rdev * nt
    n = nf * nt
    slots = cells.shape[-1]
    period = 4 * size
    tiles = length // LANES
    my_f = lax.axis_index("facet")
    my_t = lax.axis_index("team")
    my_b = lax.axis_index("sub")
    me = my_f * nt + my_t
    other = 1 - my_b

    fetches = [
        pltpu.make_async_copy(sub_hbm, sub_off, in_sem.at[0]),
        pltpu.make_async_copy(rows_hbm, rows, in_sem.at[1]),
        pltpu.make_async_copy(fac_hbm, fac_off, in_sem.at[0]),
        pltpu.make_async_copy(cnt_hbm, counts, in_sem.at[2]),
        pltpu.make_async_copy(cells_hbm.at[0, my_b, 0], cells, in_sem.at[2]),
        pltpu.make_async_copy(obs_hbm.at[0, my_b, 0], observed, in_sem.at[2]),
        pltpu.make_async_copy(wt_hbm, weights, in_sem.at[2]),
        pltpu.make_async_copy(kt_hbm, kt, in_sem.at[0]),
        pltpu.make_async_copy(kk_hbm, kk, in_sem.at[0]),
        pltpu.make_async_copy(aterm_hbm.at[0, my_b], aterm, in_sem.at[0]),
    ]
    fetches[0].start()
    fetches[2].start()
    piece = length // PIECES
    for c in range(2):
        for q in range(PIECES):
            lanes = pl.ds(q * piece, piece)
            pltpu.make_async_copy(
                rows_hbm.at[0, c, :, lanes], rows.at[0, c, :, lanes], in_sem.at[1]
            ).start()
    for fetch in fetches[3:7]:
        fetch.start()

    barrier = pltpu.get_barrier_semaphore()
    nc = 2 - nf % 2
    ny = nf // nc
    rows_far = [(y + ny // 2) % ny for y in range(ny)]
    order = [y * nc + c for c in range(nc) for y in rows_far]
    first = order[:ny]
    second = order[ny:]
    local_k = list(range(nc))
    urgent = [k for k in order if k >= nc]
    my_c = lax.rem(my_f, nc)

    def facet_at(k):
        return lax.rem(my_f // nc + k // nc, ny) * nc + k % nc

    def greet(k, t, b):
        pl.semaphore_signal(
            barrier, inc=1, device_id={"facet": facet_at(k), "team": t, "sub": b}, device_id_type=MESH
        )

    def unless_self(k, act):
        if k < nc:
            pl.when(my_c != k)(act)
        else:
            act()

    def greet_team(t):
        for k in order:
            greet(k, t, my_b)

    for t in reversed(range(1, nt)):
        pl.when(my_t < t)(functools.partial(greet_team, t))
    pl.semaphore_signal(
        barrier, inc=1, device_id={"facet": my_f, "team": my_t, "sub": other}, device_id_type=MESH
    )
    for k in order:
        unless_self(k, functools.partial(greet, k, my_t, my_b))

    base_c, base_s = sincos(iota((M, LANES), 0) * iota((M, LANES), 1), length)
    lane_row = iota((1, LANES), 1)

    fetches[0].wait()
    fetches[2].wait()

    def column_weights(shift_v):
        pc, ps = sincos(lane_row * shift_v, length)
        c = (base_c * pc - base_s * ps).astype(BF)
        s = (base_s * pc + base_c * ps).astype(BF)
        return cat([cat([c, s], 1), cat([-s, c], 1)], 0)

    scale = 1.0 / math.sqrt(length)

    def prepare(k):
        shift_v = sub_off[1, facet_at(k) * nb + my_b]
        wt_near[k] = column_weights(shift_v)
        m_no = iota((tiles, M), 1)
        turns = iota((tiles, M), 0) * LANES * (m_no + shift_v) - m_no * fac_off[1, my_f]
        c, s = sincos(turns, length)
        tw1[k, 0] = c * scale
        tw1[k, 1] = s * scale

    for k in first:
        prepare(k)
    fetches[1].wait()
    for fetch in fetches[7:]:
        fetch.start()
    x = [
        cat([rows[0, c, :, k * LANES : (k + 1) * LANES].astype(F32) for k in range(tiles)], 0)
        for c in range(2)
    ]
    x = cat(x, 1).astype(BF)

    def spectrum(k):
        y = mm_nt(x, wt_near[k])
        acc = [None] * 4
        for j in range(tiles):
            yr = y[j * rdev : (j + 1) * rdev, :M]
            yi = y[j * rdev : (j + 1) * rdev, M:]
            c = tw1[k, 0, j : j + 1, :]
            s = tw1[k, 1, j : j + 1, :]
            q = 2 * (j % 2)
            add_re = yr * c + yi * s
            add_im = yi * c - yr * s
            acc[q] = add_re if acc[q] is None else acc[q] + add_re
            acc[q + 1] = add_im if acc[q + 1] is None else acc[q + 1] + add_im
        spec_out[k] = cat([acc[0] + acc[2], acc[1] + acc[3]], 1).astype(BF)

    for k in first:
        spectrum(k)
    for i in (3, 4, 5, 6):
        fetches[i].wait()
    live = iota((1, slots), 1) < counts[my_f, my_b, my_t]
    all_wt = weights[0, 0].astype(F32)
    own_wt = jnp.where(my_b == 0, all_wt[0:1, :], all_wt[1:2, :])
    own_wt = jnp.where(live, own_wt, 0.0)
    place = cells[...]
    packed = cat(
        [
            (place >> HALF_BITS).astype(F32), (place & ((1 << HALF_BITS) - 1)).astype(F32),
            observed[...].astype(F32), own_wt, own_wt,
        ],
        0,
    ).astype(BF)
    slot_out[...] = packed
    got_x[my_t] = packed

    pl.semaphore_wait(barrier, nf * (my_t + 1))

    def report(t):
        for k in order:
            pl.semaphore_signal(
                ready.at[my_t - 1], inc=1,
                device_id={"facet": facet_at(k), "team": t, "sub": my_b}, device_id_type=MESH,
            )


    def copy_x(t):
        return pltpu.make_async_remote_copy(
            src_ref=slot_out,
            dst_ref=got_x.at[my_t],
            send_sem=sent,
            recv_sem=recv_x.at[lax.rem(my_t - t + nt, nt) - 1],
            device_id={"facet": my_f, "team": t, "sub": my_b},
            device_id_type=MESH,
        )

    def copy1(k, t):
        return pltpu.make_async_remote_copy(
            src_ref=spec_out.at[k],
            dst_ref=got1.at[me],
            send_sem=sent,
            recv_sem=recv1,
            device_id={"facet": facet_at(k), "team": t, "sub": my_b},
            device_id_type=MESH,
        )

    def send_specs(ks, t):
        for k in ks:
            if k >= nc:
                copy1(k, t).start()
            else:
                there = jnp.logical_or(my_t != t, my_c != k)
                pl.when(there)(lambda: copy1(k, t).start())

    def send_slots(t):
        pl.when(my_t != t)(lambda: copy_x(t).start())

    send_specs(first, 0)
    send_slots(0)
    for t in range(nt - 1):
        pl.when(my_t > t)(functools.partial(report, t))
    for k in second:
        prepare(k)
        spectrum(k)
    send_specs(second, 0)
    got1[me] = spec_out[my_c]

    for i in (7, 8, 9):
        fetches[i].wait()
    mirror = size // 2
    shift_u = sub_off[0, my_f * nb + my_b]
    step = length // rall
    scale_g = 1.0 / math.sqrt(rall * nf)
    lane = iota((1, n * rdev), 1)
    col_a = jnp.zeros((1, n * rdev), jnp.int32)
    row2 = iota((nf * rdev, 1), 0)
    row_a = jnp.zeros((nf * rdev, 1), jnp.int32)
    for f in range(nf):
        col_a = jnp.where(lane // rall == f, fac_off[0, f], col_a)
        row_a = jnp.where(row2 // rdev == f, fac_off[0, f], row_a)
    p0 = iota((M, n * rdev), 0)
    gc, gs = sincos(p0 * col_a - (p0 + shift_u) * (lane % rall * step), length)
    gc = (gc * scale_g).astype(BF)
    gs = (gs * scale_g).astype(BF)
    a_mat = mm(kt[...], cat([cat([gc, gs], 1), cat([-gs, gc], 1)], 0)).astype(BF)
    p1 = iota((nf * rdev, M), 1)
    hc, hs = sincos(p1 * row_a - (p1 + shift_u) * ((row2 % rdev + my_t * rdev) * step), length)
    hc = (hc * scale_g).astype(BF)
    hs = (hs * scale_g).astype(BF)
    at = mm_nt(cat([cat([hc, -hs], 1), cat([hs, hc], 1)], 0), kt[...])
    ah = cat([at[: nf * rdev], -at[nf * rdev :]], 1).astype(BF)

    for t in range(1, nt):
        pl.when(my_t < t)(lambda: pl.semaphore_wait(ready.at[t - 1], nf))
        send_slots(t)
        send_specs(order, t)
    flip = (iota((mirror, mirror), 0) + iota((mirror, mirror), 1) == mirror - 1).astype(F32).astype(BF)
    low = mm(flip, aterm[:mirror, :])
    both = cat([aterm[mirror:, :].astype(F32), low], 0)
    amap = cat([both[:, mirror:], mm(both[:, :mirror].astype(BF), flip)], 1)
    amap = cat([amap, amap], 1)
    half = tiles // nb
    scale_b = 1.0 / (math.sqrt(M) * size)
    tile_no = iota((half, M), 0) + my_b * half
    for far in range(2):
        for a in range(nf):
            shift_v = sub_off[1, facet_at(a) * nb + (other if far else my_b)]
            if far:
                wt_far[a] = column_weights(shift_v)
            m_no = iota((half, M), 1)
            c, s = sincos((m_no + shift_v) * (tile_no * LANES) - m_no * fac_off[1, my_f], length)
            tw2[far, a, 0] = c * scale_b
            tw2[far, a, 1] = s * scale_b

    fine_no = iota((FINE, slots), 0)
    col_no = iota((mirror // FINE, slots), 0)
    for k in range(nt):
        src = lax.rem(my_t + k, nt)
        if k:
            pltpu.make_async_copy(got_x.at[src], got_x.at[src], recv_x.at[k - 1]).wait()
        pos = got_x[src].astype(F32)[0:4, :].astype(jnp.int32)
        pos = (pos[0:2, :] << HALF_BITS) + pos[2:4, :]
        pos_x = pos[0:1, :]
        pos_y = pos[1:2, :]
        mid_c, mid_s = sincos((size - 1) * (pos_x + pos_y), 2 * period)
        middle[k, 0:1, :] = mid_c
        middle[k, 1:2, :] = mid_s
        for axis, place in enumerate((pos_x, pos_y)):
            lo_c, lo_s = sincos((2 * fine_no + 1) * place, 2 * period)
            hi_c, hi_s = sincos(2 * FINE * col_no * place, 2 * period)
            coarse[0] = hi_c
            coarse[1] = hi_s
            for q in range(mirror // FINE):
                c1 = coarse[0, q : q + 1, :]
                s1 = coarse[1, q : q + 1, :]
                c = c1 * lo_c - s1 * lo_s
                s = s1 * lo_c + c1 * lo_s
                rng = slice(q * FINE, (q + 1) * FINE)
                low = slice(mirror + q * FINE, mirror + (q + 1) * FINE)
                if axis == 0:
                    row_c[k, rng, :] = c
                    row_s[k, rng, :] = s
                    row_w[k, rng, :] = c.astype(BF)
                    row_w[k, low, :] = s.astype(BF)
                else:
                    col_w[k, rng, :] = c.astype(BF)
                    col_w[k, low, :] = s.astype(BF)
    done = got1.at[pl.ds(0, n - 1)]
    pltpu.make_async_copy(done, done, recv1).wait()
    got = got1[...].astype(F32).reshape(n * rdev, 2 * M)
    got = cat([got, cat([-got[:, M:], got[:, :M]], 1)], 0).astype(BF)
    full = mm(a_mat, got)
    image = mm(full.astype(BF), kk[...])
    image = amap * image
    re_p, re_n, im_p, im_n = (image[:, c * mirror : (c + 1) * mirror] for c in range(4))
    folded = cat(
        [cat([re_p + re_n, im_p - im_n], 1), cat([im_p + im_n, re_n - re_p], 1)], 0
    )
    a, b, c, d = (folded[q * mirror : (q + 1) * mirror] for q in range(4))
    folded = cat([a + b, a - b, c + d, c - d], 0).astype(BF)
    def degrid(k):
        src = lax.rem(my_t + k, nt)
        z = mm(folded, col_w[k])
        re_e, re_o, im_e, im_o = (z[q * mirror : (q + 1) * mirror] for q in range(4))
        rc = row_c[k]
        rs = row_s[k]
        mid_c = middle[k, 0:1, :]
        mid_s = middle[k, 1:2, :]
        sum_re = jnp.sum(rc * re_e + rs * im_o, 0, keepdims=True) * (1.0 / size)
        sum_im = jnp.sum(rc * im_e - rs * re_o, 0, keepdims=True) * (1.0 / size)
        pred_re = sum_re * mid_c + sum_im * mid_s
        pred_im = sum_im * mid_c - sum_re * mid_s
        info = got_x[src].astype(F32)
        res_re = info[6:7, :] * (info[4:5, :] - pred_re)
        res_im = info[6:7, :] * (info[5:6, :] - pred_im)
        turn_re = res_re * mid_c - res_im * mid_s
        turn_im = res_re * mid_s + res_im * mid_c
        turn_re = jnp.broadcast_to(turn_re.astype(BF), (size, slots))
        turn_im = jnp.broadcast_to(turn_im.astype(BF), (size, slots))
        rows_w = row_w[k]
        return cat([rows_w * turn_re, rows_w * turn_im], 0)

    left = [None] * nt
    prod = None
    for k in range(nt):
        left[k] = degrid(k)
    prod = mm_nt(cat(left, 1), cat([col_w[k] for k in range(nt)], 1))
    a, c, b, d = (prod[q * mirror : (q + 1) * mirror] for q in range(4))
    real = cat([a - d, a + d], 0)
    imag = cat([b + c, b - c], 0)
    cr, sr = real[:, :mirror], real[:, mirror:]
    ci, si = imag[:, :mirror], imag[:, mirror:]
    grid = cat([cr - si, cr + si, ci + sr, ci - sr], 1)
    v = (amap * grid).astype(BF)
    u = mm_nt(v, kk[...]).astype(BF)
    ur = u[:, :M]
    ui = u[:, M:]
    part = mm(ah, cat([u, cat([-ui, ur], 1)], 0))
    fold_out[...] = part.reshape(nf, rdev, 2 * M).astype(BF)


    def copy2(k, far):
        return pltpu.make_async_remote_copy(
            src_ref=fold_out.at[facet_at(k)],
            dst_ref=got2.at[far, my_f],
            send_sem=sent,
            recv_sem=recv2.at[2 + my_c if far and k >= nc else min(k // nc, 1) + far],
            device_id={"facet": facet_at(k), "team": my_t, "sub": other if far else my_b},
            device_id_type=MESH,
        )

    for k in order:
        copy2(k, 1).start()
    for k in order:
        unless_self(k, lambda: copy2(k, 0).start())
    got2[0, my_f] = fold_out[my_f]

    def update(total, far, ks):
        for k in ks:
            g = got2[far, facet_at(k)].astype(F32)
            gr = g[:, :M]
            gi = g[:, M:]
            parts = []
            for j in range(half):
                c = tw2[far, k, 0, j : j + 1, :]
                s = tw2[far, k, 1, j : j + 1, :]
                parts.append(cat([gr * c - gi * s, gr * s + gi * c], 1))
            y = mm(cat(parts, 0).astype(BF), (wt_far if far else wt_near)[k])
            total = y if total is None else total + y
        return total

    def arrived(which, count):
        done = got1.at[pl.ds(0, count)]
        pltpu.make_async_copy(done, done, recv2.at[which]).wait()

    if nc > 1:
        arrived(0, nc - 1)
    total = update(None, 0, local_k)
    arrived(1, nf)
    total = update(total, 1, local_k)
    total = update(total, 0, urgent)
    if ny > 1:
        for c in reversed(range(nc)):
            arrived(2 + c, ny - 1)
            total = update(total, 1, [k for k in urgent if k % nc == c])
    for k in range(half):
        rng = slice(k * rdev, (k + 1) * rdev)
        lanes = slice(k * LANES, (k + 1) * LANES)
        out[0, 0, :, lanes] = total[rng, :LANES]
        out[0, 1, :, lanes] = total[rng, LANES:]
    for count in (n - 1, nt - 1, 2 * nf - 1):
        gone = got1.at[pl.ds(0, count)]
        pltpu.make_async_copy(gone, gone, sent).wait()


def tables(size):
    angle = (np.arange(M)[:, None] * np.arange(size)[None, :] % size) * (TWO_PI / size)
    kc = np.cos(angle) / math.sqrt(M)
    ks = np.sin(angle) / math.sqrt(M)
    half = size // 2
    order = np.concatenate([np.arange(half, size), np.arange(half - 1, -1, -1)])
    kc, ks = kc[:, order], ks[:, order]
    kt = np.concatenate([kc.T, ks.T], 1)
    kk = np.block([[kc, ks], [-ks, kc]])
    return [np.asarray(v, np.float32).astype(ml_dtypes.bfloat16) for v in (kk, kt)]


def local(facet_rows, sub_offsets, facet_offsets, aterm, cells, observed, weights, counts):
    nf = lax.axis_size("facet")
    nt = lax.axis_size("team")
    nb = lax.axis_size("sub")
    rdev, length = facet_rows.shape[2:]
    size = aterm.shape[-1]
    slots = cells.shape[-1]
    n = nf * nt
    tiles = length // LANES
    nc = 2 - nf % 2
    dims = (nf, nt, nb, length, size, rdev)
    consts = [jnp.asarray(v) for v in tables(size)]
    hbm = pl.BlockSpec(memory_space=pltpu.HBM)
    operands = [
        sub_offsets.T, facet_offsets.T, counts, facet_rows, aterm, cells, observed,
        weights.transpose(0, 2, 1, 3), *consts,
    ]
    dma = pltpu.SemaphoreType.DMA
    vmem = pltpu.VMEM
    return pl.pallas_call(
        functools.partial(body, dims),
        out_shape=pltpu.VMEM((1, 2, rdev, length // nb), F32),
        in_specs=[hbm] * 10,
        out_specs=pl.BlockSpec(memory_space=pltpu.VMEM),
        scratch_shapes=[
            *[pltpu.SMEM(v.shape, v.dtype) for v in operands[:3]],
            vmem(facet_rows.shape, BF),
            vmem((size, size), BF),
            vmem((2, slots), jnp.int32),
            vmem((2, slots), BF),
            *[vmem(v.shape, v.dtype) for v in operands[7:]],
            vmem((nf, rdev, 2 * M), BF),
            vmem((n, rdev, 2 * M), BF),
            vmem((8, slots), BF),
            vmem((nt, 8, slots), BF),
            vmem((nf, rdev, 2 * M), BF),
            vmem((nb, nf, rdev, 2 * M), BF),
            vmem((nf, 2, tiles, M), F32),
            vmem((nb, nf, 2, tiles // nb, M), F32),
            vmem((nf, 2 * M, 2 * LANES), BF),
            vmem((nf, 2 * M, 2 * LANES), BF),
            vmem((2, size // 2 // FINE, slots), F32),
            vmem((nt, 8, slots), F32),
            vmem((nt, size, slots), BF),
            vmem((nt, size, slots), BF),
            vmem((nt, size // 2, slots), F32),
            vmem((nt, size // 2, slots), F32),
            dma, dma, dma((max(nt - 1, 1),)), dma((2 + nc,)), dma((3,)), pltpu.SemaphoreType.REGULAR((max(nt - 1, 1),)),
        ],
        compiler_params=pltpu.CompilerParams(
            collective_id=0, has_side_effects=True
        ),
    )(*operands)


def solution(mesh):
    placed = (
        P("facet", None, "team", None),
        P(),
        P(),
        P("facet", None, None, None),
        P("facet", None, "team", None, None),
        P("facet", None, "team", None, None),
        P("facet", None, "team", None),
        P(),
    )
    return jax.shard_map(
        local,
        mesh=mesh,
        in_specs=placed,
        out_specs=P("facet", None, "team", "sub"),
        check_vma=False,
    )
```

```python
import functools
import math

import jax
import jax.numpy as jnp
import ml_dtypes
import numpy as np
from jax import lax
from jax.experimental import pallas as pl
from jax.experimental.pallas import tpu as pltpu
from jax.sharding import PartitionSpec as P

M = 128
LANES = 128
FINE = 16
HALF_BITS = 5
PIECES = 1
TWO_PI = 2.0 * math.pi
BF = jnp.bfloat16
F32 = jnp.float32
MESH = pl.DeviceIdType.MESH


def sincos(turns, period):
    shift = period.bit_length() - 3
    quad = (turns + (1 << (shift - 1))) >> shift
    t = (turns - (quad << shift)).astype(F32) * (TWO_PI / period)
    t2 = t * t
    s = t * (1.0 + t2 * (-1.0 / 6 + t2 * (1.0 / 120 + t2 * (-1.0 / 5040))))
    c = 1.0 + t2 * (-0.5 + t2 * (1.0 / 24 + t2 * (-1.0 / 720 + t2 * (1.0 / 40320))))
    odd = (quad & 1) != 0
    cos = jnp.where(odd, s, c)
    sin = jnp.where(odd, c, s)
    cos = jnp.where(((quad + 1) & 2) != 0, -cos, cos)
    sin = jnp.where((quad & 2) != 0, -sin, sin)
    return cos, sin


def mm(left, right):
    return jnp.dot(left, right, preferred_element_type=F32)


def mm_nt(left, right):
    return lax.dot_general(left, right, (((1,), (1,)), ((), ())), preferred_element_type=F32)


def cat(parts, axis):
    return jnp.concatenate(parts, axis)


def iota(shape, dim):
    return lax.broadcasted_iota(jnp.int32, shape, dim)


def body(dims, *refs):
    (sub_hbm, fac_hbm, cnt_hbm, rows_hbm, aterm_hbm, cells_hbm, obs_hbm, wt_hbm, kk_hbm, kt_hbm) = refs[:10]
    out = refs[10]
    (
        sub_off, fac_off, counts, rows, aterm, cells, observed, weights, kk, kt,
        spec_out, got1, slot_out, got_x, fold_out, got2,
        tw1, tw2, wt_near, wt_far, coarse, middle, col_w, row_w, row_c, row_s,
        sent, recv1, recv_x, recv2, in_sem, ready,
    ) = refs[11:]
    nf, nt, nb, length, size, rdev = dims
    rall = rdev * nt
    n = nf * nt
    slots = cells.shape[-1]
    period = 4 * size
    tiles = length // LANES
    my_f = lax.axis_index("facet")
    my_t = lax.axis_index("team")
    my_b = lax.axis_index("sub")
    me = my_f * nt + my_t
    other = 1 - my_b

    fetches = [
        pltpu.make_async_copy(sub_hbm, sub_off, in_sem.at[0]),
        pltpu.make_async_copy(rows_hbm, rows, in_sem.at[1]),
        pltpu.make_async_copy(fac_hbm, fac_off, in_sem.at[0]),
        pltpu.make_async_copy(cnt_hbm, counts, in_sem.at[2]),
        pltpu.make_async_copy(cells_hbm.at[0, my_b, 0], cells, in_sem.at[2]),
        pltpu.make_async_copy(obs_hbm.at[0, my_b, 0], observed, in_sem.at[2]),
        pltpu.make_async_copy(wt_hbm, weights, in_sem.at[2]),
        pltpu.make_async_copy(kt_hbm, kt, in_sem.at[0]),
        pltpu.make_async_copy(kk_hbm, kk, in_sem.at[0]),
        pltpu.make_async_copy(aterm_hbm.at[0, my_b], aterm, in_sem.at[0]),
    ]
    fetches[0].start()
    fetches[2].start()
    piece = length // PIECES
    for c in range(2):
        for q in range(PIECES):
            lanes = pl.ds(q * piece, piece)
            pltpu.make_async_copy(
                rows_hbm.at[0, c, :, lanes], rows.at[0, c, :, lanes], in_sem.at[1]
            ).start()
    for fetch in fetches[3:7]:
        fetch.start()

    barrier = pltpu.get_barrier_semaphore()
    nc = 2 - nf % 2
    ny = nf // nc
    rows_far = [(y + ny // 2) % ny for y in range(ny)]
    order = [y * nc + c for c in range(nc) for y in rows_far]
    first = order[:ny]
    second = order[ny:]
    local_k = list(range(nc))
    urgent = [k for k in order if k >= nc]
    my_c = lax.rem(my_f, nc)

    def facet_at(k):
        return lax.rem(my_f // nc + k // nc, ny) * nc + k % nc

    def greet(k, t, b):
        pl.semaphore_signal(
            barrier, inc=1, device_id={"facet": facet_at(k), "team": t, "sub": b}, device_id_type=MESH
        )

    def unless_self(k, act):
        if k < nc:
            pl.when(my_c != k)(act)
        else:
            act()

    def greet_team(t):
        for k in order:
            greet(k, t, my_b)

    for t in reversed(range(1, nt)):
        pl.when(my_t < t)(functools.partial(greet_team, t))
    pl.semaphore_signal(
        barrier, inc=1, device_id={"facet": my_f, "team": my_t, "sub": other}, device_id_type=MESH
    )
    for k in order:
        unless_self(k, functools.partial(greet, k, my_t, my_b))

    base_c, base_s = sincos(iota((M, LANES), 0) * iota((M, LANES), 1), length)
    lane_row = iota((1, LANES), 1)

    fetches[0].wait()
    fetches[2].wait()

    def column_weights(shift_v):
        pc, ps = sincos(lane_row * shift_v, length)
        c = (base_c * pc - base_s * ps).astype(BF)
        s = (base_s * pc + base_c * ps).astype(BF)
        return cat([cat([c, s], 1), cat([-s, c], 1)], 0)

    scale = 1.0 / math.sqrt(length)

    def prepare(k):
        shift_v = sub_off[1, facet_at(k) * nb + my_b]
        wt_near[k] = column_weights(shift_v)
        m_no = iota((tiles, M), 1)
        turns = iota((tiles, M), 0) * LANES * (m_no + shift_v) - m_no * fac_off[1, my_f]
        c, s = sincos(turns, length)
        tw1[k, 0] = c * scale
        tw1[k, 1] = s * scale

    for k in first:
        prepare(k)
    fetches[1].wait()
    for fetch in fetches[7:]:
        fetch.start()
    x = [
        cat([rows[0, c, :, k * LANES : (k + 1) * LANES].astype(F32) for k in range(tiles)], 0)
        for c in range(2)
    ]
    x = cat(x, 1).astype(BF)

    def spectrum(k):
        y = mm_nt(x, wt_near[k])
        acc = [None] * 4
        for j in range(tiles):
            yr = y[j * rdev : (j + 1) * rdev, :M]
            yi = y[j * rdev : (j + 1) * rdev, M:]
            c = tw1[k, 0, j : j + 1, :]
            s = tw1[k, 1, j : j + 1, :]
            q = 2 * (j % 2)
            add_re = yr * c + yi * s
            add_im = yi * c - yr * s
            acc[q] = add_re if acc[q] is None else acc[q] + add_re
            acc[q + 1] = add_im if acc[q + 1] is None else acc[q + 1] + add_im
        spec_out[k] = cat([acc[0] + acc[2], acc[1] + acc[3]], 1).astype(BF)

    for k in first:
        spectrum(k)
    for i in (3, 4, 5, 6):
        fetches[i].wait()
    live = iota((1, slots), 1) < counts[my_f, my_b, my_t]
    all_wt = weights[0, 0].astype(F32)
    own_wt = jnp.where(my_b == 0, all_wt[0:1, :], all_wt[1:2, :])
    own_wt = jnp.where(live, own_wt, 0.0)
    place = cells[...]
    packed = cat(
        [
            (place >> HALF_BITS).astype(F32), (place & ((1 << HALF_BITS) - 1)).astype(F32),
            observed[...].astype(F32), own_wt, own_wt,
        ],
        0,
    ).astype(BF)
    slot_out[...] = packed
    got_x[my_t] = packed

    pl.semaphore_wait(barrier, nf * (my_t + 1))

    def report(t):
        for k in order:
            pl.semaphore_signal(
                ready.at[my_t - 1], inc=1,
                device_id={"facet": facet_at(k), "team": t, "sub": my_b}, device_id_type=MESH,
            )


    def copy_x(t):
        return pltpu.make_async_remote_copy(
            src_ref=slot_out,
            dst_ref=got_x.at[my_t],
            send_sem=sent,
            recv_sem=recv_x.at[lax.rem(my_t - t + nt, nt) - 1],
            device_id={"facet": my_f, "team": t, "sub": my_b},
            device_id_type=MESH,
        )

    def copy1(k, t):
        return pltpu.make_async_remote_copy(
            src_ref=spec_out.at[k],
            dst_ref=got1.at[me],
            send_sem=sent,
            recv_sem=recv1,
            device_id={"facet": facet_at(k), "team": t, "sub": my_b},
            device_id_type=MESH,
        )

    def send_specs(ks, t):
        for k in ks:
            if k >= nc:
                copy1(k, t).start()
            else:
                there = jnp.logical_or(my_t != t, my_c != k)
                pl.when(there)(lambda: copy1(k, t).start())

    def send_slots(t):
        pl.when(my_t != t)(lambda: copy_x(t).start())

    send_specs(first, 0)
    send_slots(0)
    for t in range(nt - 1):
        pl.when(my_t > t)(functools.partial(report, t))
    for k in second:
        prepare(k)
        spectrum(k)
    send_specs(second, 0)
    got1[me] = spec_out[my_c]

    for i in (7, 8, 9):
        fetches[i].wait()
    mirror = size // 2
    shift_u = sub_off[0, my_f * nb + my_b]
    step = length // rall
    scale_g = 1.0 / math.sqrt(rall * nf)
    lane = iota((1, n * rdev), 1)
    col_a = jnp.zeros((1, n * rdev), jnp.int32)
    row2 = iota((nf * rdev, 1), 0)
    row_a = jnp.zeros((nf * rdev, 1), jnp.int32)
    for f in range(nf):
        col_a = jnp.where(lane // rall == f, fac_off[0, f], col_a)
        row_a = jnp.where(row2 // rdev == f, fac_off[0, f], row_a)
    p0 = iota((M, n * rdev), 0)
    gc, gs = sincos(p0 * col_a - (p0 + shift_u) * (lane % rall * step), length)
    gc = (gc * scale_g).astype(BF)
    gs = (gs * scale_g).astype(BF)
    a_mat = mm(kt[...], cat([cat([gc, gs], 1), cat([-gs, gc], 1)], 0)).astype(BF)
    p1 = iota((nf * rdev, M), 1)
    hc, hs = sincos(p1 * row_a - (p1 + shift_u) * ((row2 % rdev + my_t * rdev) * step), length)
    hc = (hc * scale_g).astype(BF)
    hs = (hs * scale_g).astype(BF)
    at = mm_nt(cat([cat([hc, -hs], 1), cat([hs, hc], 1)], 0), kt[...])
    ah = cat([at[: nf * rdev], -at[nf * rdev :]], 1).astype(BF)

    for t in range(1, nt):
        pl.when(my_t < t)(lambda: pl.semaphore_wait(ready.at[t - 1], nf))
        send_slots(t)
        send_specs(order, t)
    flip = (iota((mirror, mirror), 0) + iota((mirror, mirror), 1) == mirror - 1).astype(F32).astype(BF)
    low = mm(flip, aterm[:mirror, :])
    both = cat([aterm[mirror:, :].astype(F32), low], 0)
    amap = cat([both[:, mirror:], mm(both[:, :mirror].astype(BF), flip)], 1)
    amap = cat([amap, amap], 1)
    half = tiles // nb
    scale_b = 1.0 / (math.sqrt(M) * size)
    tile_no = iota((half, M), 0) + my_b * half
    for far in range(2):
        for a in range(nf):
            shift_v = sub_off[1, facet_at(a) * nb + (other if far else my_b)]
            if far:
                wt_far[a] = column_weights(shift_v)
            m_no = iota((half, M), 1)
            c, s = sincos((m_no + shift_v) * (tile_no * LANES) - m_no * fac_off[1, my_f], length)
            tw2[far, a, 0] = c * scale_b
            tw2[far, a, 1] = s * scale_b

    fine_no = iota((FINE, slots), 0)
    col_no = iota((mirror // FINE, slots), 0)
    for k in range(nt):
        src = lax.rem(my_t + k, nt)
        if k:
            pltpu.make_async_copy(got_x.at[src], got_x.at[src], recv_x.at[k - 1]).wait()
        pos = got_x[src].astype(F32)[0:4, :].astype(jnp.int32)
        pos = (pos[0:2, :] << HALF_BITS) + pos[2:4, :]
        pos_x = pos[0:1, :]
        pos_y = pos[1:2, :]
        mid_c, mid_s = sincos((size - 1) * (pos_x + pos_y), 2 * period)
        middle[k, 0:1, :] = mid_c
        middle[k, 1:2, :] = mid_s
        for axis, place in enumerate((pos_x, pos_y)):
            lo_c, lo_s = sincos((2 * fine_no + 1) * place, 2 * period)
            hi_c, hi_s = sincos(2 * FINE * col_no * place, 2 * period)
            coarse[0] = hi_c
            coarse[1] = hi_s
            for q in range(mirror // FINE):
                c1 = coarse[0, q : q + 1, :]
                s1 = coarse[1, q : q + 1, :]
                c = c1 * lo_c - s1 * lo_s
                s = s1 * lo_c + c1 * lo_s
                rng = slice(q * FINE, (q + 1) * FINE)
                low = slice(mirror + q * FINE, mirror + (q + 1) * FINE)
                if axis == 0:
                    row_c[k, rng, :] = c
                    row_s[k, rng, :] = s
                    row_w[k, rng, :] = c.astype(BF)
                    row_w[k, low, :] = s.astype(BF)
                else:
                    col_w[k, rng, :] = c.astype(BF)
                    col_w[k, low, :] = s.astype(BF)
    done = got1.at[pl.ds(0, n - 1)]
    pltpu.make_async_copy(done, done, recv1).wait()
    got = got1[...].astype(F32).reshape(n * rdev, 2 * M)
    got = cat([got, cat([-got[:, M:], got[:, :M]], 1)], 0).astype(BF)
    full = mm(a_mat, got)
    image = mm(full.astype(BF), kk[...])
    image = amap * image
    re_p, re_n, im_p, im_n = (image[:, c * mirror : (c + 1) * mirror] for c in range(4))
    folded = cat(
        [cat([re_p + re_n, im_p - im_n], 1), cat([im_p + im_n, re_n - re_p], 1)], 0
    )
    a, b, c, d = (folded[q * mirror : (q + 1) * mirror] for q in range(4))
    folded = cat([a + b, a - b, c + d, c - d], 0).astype(BF)
    def degrid(k):
        src = lax.rem(my_t + k, nt)
        z = mm(folded, col_w[k])
        re_e, re_o, im_e, im_o = (z[q * mirror : (q + 1) * mirror] for q in range(4))
        rc = row_c[k]
        rs = row_s[k]
        mid_c = middle[k, 0:1, :]
        mid_s = middle[k, 1:2, :]
        sum_re = jnp.sum(rc * re_e + rs * im_o, 0, keepdims=True) * (1.0 / size)
        sum_im = jnp.sum(rc * im_e - rs * re_o, 0, keepdims=True) * (1.0 / size)
        pred_re = sum_re * mid_c + sum_im * mid_s
        pred_im = sum_im * mid_c - sum_re * mid_s
        info = got_x[src].astype(F32)
        res_re = info[6:7, :] * (info[4:5, :] - pred_re)
        res_im = info[6:7, :] * (info[5:6, :] - pred_im)
        turn_re = res_re * mid_c - res_im * mid_s
        turn_im = res_re * mid_s + res_im * mid_c
        turn_re = jnp.broadcast_to(turn_re.astype(BF), (size, slots))
        turn_im = jnp.broadcast_to(turn_im.astype(BF), (size, slots))
        rows_w = row_w[k]
        return cat([rows_w * turn_re, rows_w * turn_im], 0)

    left = [None] * nt
    prod = None
    for k in range(nt):
        left[k] = degrid(k)
    prod = mm_nt(cat(left, 1), cat([col_w[k] for k in range(nt)], 1))
    a, c, b, d = (prod[q * mirror : (q + 1) * mirror] for q in range(4))
    real = cat([a - d, a + d], 0)
    imag = cat([b + c, b - c], 0)
    cr, sr = real[:, :mirror], real[:, mirror:]
    ci, si = imag[:, :mirror], imag[:, mirror:]
    grid = cat([cr - si, cr + si, ci + sr, ci - sr], 1)
    v = (amap * grid).astype(BF)
    u = mm_nt(v, kk[...]).astype(BF)
    ur = u[:, :M]
    ui = u[:, M:]
    part = mm(ah, cat([u, cat([-ui, ur], 1)], 0))
    fold_out[...] = part.reshape(nf, rdev, 2 * M).astype(BF)


    def copy2(k, far):
        return pltpu.make_async_remote_copy(
            src_ref=fold_out.at[facet_at(k)],
            dst_ref=got2.at[far, my_f],
            send_sem=sent,
            recv_sem=recv2.at[2 + my_c if far and k >= nc else min(k // nc, 1) + far],
            device_id={"facet": facet_at(k), "team": my_t, "sub": other if far else my_b},
            device_id_type=MESH,
        )

    for k in order:
        copy2(k, 1).start()
    for k in order:
        unless_self(k, lambda: copy2(k, 0).start())
    got2[0, my_f] = fold_out[my_f]

    def update(total, far, ks):
        for k in ks:
            g = got2[far, facet_at(k)].astype(F32)
            gr = g[:, :M]
            gi = g[:, M:]
            parts = []
            for j in range(half):
                c = tw2[far, k, 0, j : j + 1, :]
                s = tw2[far, k, 1, j : j + 1, :]
                parts.append(cat([gr * c - gi * s, gr * s + gi * c], 1))
            y = mm(cat(parts, 0).astype(BF), (wt_far if far else wt_near)[k])
            total = y if total is None else total + y
        return total

    def arrived(which, count):
        done = got1.at[pl.ds(0, count)]
        pltpu.make_async_copy(done, done, recv2.at[which]).wait()

    if nc > 1:
        arrived(0, nc - 1)
    total = update(None, 0, local_k)
    arrived(1, nf)
    total = update(total, 1, local_k)
    total = update(total, 0, urgent)
    if ny > 1:
        for c in reversed(range(nc)):
            arrived(2 + c, ny - 1)
            total = update(total, 1, [k for k in urgent if k % nc == c])
    for k in range(half):
        rng = slice(k * rdev, (k + 1) * rdev)
        lanes = slice(k * LANES, (k + 1) * LANES)
        out[0, 0, :, lanes] = total[rng, :LANES]
        out[0, 1, :, lanes] = total[rng, LANES:]
    for count in (n - 1, nt - 1, 2 * nf - 1):
        gone = got1.at[pl.ds(0, count)]
        pltpu.make_async_copy(gone, gone, sent).wait()


def tables(size):
    angle = (np.arange(M)[:, None] * np.arange(size)[None, :] % size) * (TWO_PI / size)
    kc = np.cos(angle) / math.sqrt(M)
    ks = np.sin(angle) / math.sqrt(M)
    half = size // 2
    order = np.concatenate([np.arange(half, size), np.arange(half - 1, -1, -1)])
    kc, ks = kc[:, order], ks[:, order]
    kt = np.concatenate([kc.T, ks.T], 1)
    kk = np.block([[kc, ks], [-ks, kc]])
    return [np.asarray(v, np.float32).astype(ml_dtypes.bfloat16) for v in (kk, kt)]


def local(facet_rows, sub_offsets, facet_offsets, aterm, cells, observed, weights, counts):
    nf = lax.axis_size("facet")
    nt = lax.axis_size("team")
    nb = lax.axis_size("sub")
    rdev, length = facet_rows.shape[2:]
    size = aterm.shape[-1]
    slots = cells.shape[-1]
    n = nf * nt
    tiles = length // LANES
    nc = 2 - nf % 2
    dims = (nf, nt, nb, length, size, rdev)
    consts = [jnp.asarray(v) for v in tables(size)]
    hbm = pl.BlockSpec(memory_space=pltpu.HBM)
    operands = [
        sub_offsets.T, facet_offsets.T, counts, facet_rows, aterm, cells, observed,
        weights.transpose(0, 2, 1, 3), *consts,
    ]
    dma = pltpu.SemaphoreType.DMA
    vmem = pltpu.VMEM
    return pl.pallas_call(
        functools.partial(body, dims),
        out_shape=pltpu.VMEM((1, 2, rdev, length // nb), F32),
        in_specs=[hbm] * 10,
        out_specs=pl.BlockSpec(memory_space=pltpu.VMEM),
        scratch_shapes=[
            *[pltpu.SMEM(v.shape, v.dtype) for v in operands[:3]],
            vmem(facet_rows.shape, BF),
            vmem((size, size), BF),
            vmem((2, slots), jnp.int32),
            vmem((2, slots), BF),
            *[vmem(v.shape, v.dtype) for v in operands[7:]],
            vmem((nf, rdev, 2 * M), BF),
            vmem((n, rdev, 2 * M), BF),
            vmem((8, slots), BF),
            vmem((nt, 8, slots), BF),
            vmem((nf, rdev, 2 * M), BF),
            vmem((nb, nf, rdev, 2 * M), BF),
            vmem((nf, 2, tiles, M), F32),
            vmem((nb, nf, 2, tiles // nb, M), F32),
            vmem((nf, 2 * M, 2 * LANES), BF),
            vmem((nf, 2 * M, 2 * LANES), BF),
            vmem((2, size // 2 // FINE, slots), F32),
            vmem((nt, 8, slots), F32),
            vmem((nt, size, slots), BF),
            vmem((nt, size, slots), BF),
            vmem((nt, size // 2, slots), F32),
            vmem((nt, size // 2, slots), F32),
            dma, dma, dma((max(nt - 1, 1),)), dma((2 + nc,)), dma((3,)), pltpu.SemaphoreType.REGULAR((max(nt - 1, 1),)),
        ],
        compiler_params=pltpu.CompilerParams(
            collective_id=0, has_side_effects=True
        ),
    )(*operands)


def solution(mesh):
    placed = (
        P("facet", None, "team", None),
        P(),
        P(),
        P("facet", None, None, None),
        P("facet", None, "team", None, None),
        P("facet", None, "team", None, None),
        P("facet", None, "team", None),
        P(),
    )
    return jax.shard_map(
        local,
        mesh=mesh,
        in_specs=placed,
        out_specs=P("facet", None, "team", "sub"),
        check_vma=False,
    )
```
